32 devices in a mesh: dp: 8 (over z, y), tensor: 4 (over x, core).
Axes of the slice: x: 2, y: 2, z: 4, core: 2. Of those that a mesh axis runs over, the one named last changes fastest.
Arguments:
- inputs: bfloat16 [26656, 768], P('dp'), may hold values from -6 to 6
- cotangent: bfloat16 [26656, 768], P('dp'), may hold values from -6 to 6
- master_inward: float32 [3, 768, 768], P(None, 'dp', 'tensor'), may hold values from -0.28867513 to 0.28867513
- first_inward: float32 [3, 768, 768], P(None, 'dp', 'tensor'), may hold values from -512 to 512
- second_inward: float32 [3, 768, 768], P(None, 'dp', 'tensor'), may hold values from 3332 to 53312
- master_outward: float32 [768, 768], P('tensor', 'dp'), may hold values from -0.8164966 to 0.8164966
- first_outward: float32 [768, 768], P('tensor', 'dp'), may hold values from -320 to 320
- second_outward: float32 [768, 768], P('tensor', 'dp'), may hold values from 1332.8 to 21324.8
- master_widening: float32 [768, 3072], P('dp', 'tensor'), may hold values from -0.28867513 to 0.28867513
- first_widening: float32 [768, 3072], P('dp', 'tensor'), may hold values from -320 to 320
- second_widening: float32 [768, 3072], P('dp', 'tensor'), may hold values from 1332.8 to 21324.8
- master_narrowing: float32 [3072, 768], P('tensor', 'dp'), may hold values from -0.14433757 to 0.14433757
- first_narrowing: float32 [3072, 768], P('tensor', 'dp'), may hold values from -640 to 640
- second_narrowing: float32 [3072, 768], P('tensor', 'dp'), may hold values from 5331.2 to 85299.2
- master_scaling: float32 [768], P('dp'), may hold values from 0.5 to 1.5
- first_scaling: float32 [768], P('dp'), may hold values from -1024 to 1024
- second_scaling: float32 [768], P('dp'), may hold values from 13328 to 213248
Outputs:
- output: bfloat16 [26656, 768], P(('dp', 'tensor'))
- input_grad: bfloat16 [26656, 768], P('dp')
- moment_inward: float32 [3, 768, 768], P(None, 'dp', 'tensor')
- square_inward: float32 [3, 768, 768], P(None, 'dp', 'tensor')
- weight_inward: float32 [3, 768, 768], P(None, 'dp', 'tensor')
- bfloat_inward: bfloat16 [3, 768, 768], P(None, 'dp', 'tensor')
- moment_outward: float32 [768, 768], P('tensor', 'dp')
- square_outward: float32 [768, 768], P('tensor', 'dp')
- weight_outward: float32 [768, 768], P('tensor', 'dp')
- bfloat_outward: bfloat16 [768, 768], P('tensor', 'dp')
- moment_widening: float32 [768, 3072], P('dp', 'tensor')
- square_widening: float32 [768, 3072], P('dp', 'tensor')
- weight_widening: float32 [768, 3072], P('dp', 'tensor')
- bfloat_widening: bfloat16 [768, 3072], P('dp', 'tensor')
- moment_narrowing: float32 [3072, 768], P('tensor', 'dp')
- square_narrowing: float32 [3072, 768], P('tensor', 'dp')
- weight_narrowing: float32 [3072, 768], P('tensor', 'dp')
- bfloat_narrowing: bfloat16 [3072, 768], P('tensor', 'dp')
- moment_scaling: float32 [768], P('dp')
- square_scaling: float32 [768], P('dp')
- weight_scaling: float32 [768], P('dp')
- bfloat_scaling: bfloat16 [768], P('dp')
- trust_norms: float32 [5, 2], replicated
The draws below stay inside these ranges and needn't reach their ends.
All inputs are finite; a program needn't handle non-finite values.
Results may differ from the reference program's by a relative error of at most 0.012.
The reference program's roundings to bfloat16 on the way count: a program that leaves them out, or rounds other values in their place, can miss the bound.
Values may be sent and summed in bfloat16 or wider, within the bound.
A program may use at most 192 MiB of HBM per device.

```python
import math
import jax
import jax.numpy as jnp
from jax import lax

D = 768
HEADS = 12
HEAD_DIM = 64
FF = 3072
SEQ = 196
IMG_DEV = 17
STEP = 5
TOKENS = 26656
N_DP = 8


def rising(key, shape, dim, fan):
    base = jnp.clip(jax.random.normal(key, shape, jnp.float32), -6.0, 6.0)
    spread = math.log(3.0) / 2.0
    place = lax.broadcasted_iota(jnp.float32, shape, dim) / shape[dim]
    return base * jnp.exp(spread * (place - 0.5)) / math.sqrt(fan)


def draw_master_inward(key, part):
    return rising(key, (3, D, D), 1, D)


def draw_master_outward(key, part):
    return rising(key, (D, D), 1, D // 8)


def draw_master_widening(key, part):
    return rising(key, (D, FF), 0, D)


def draw_master_narrowing(key, part):
    return rising(key, (FF, D), 1, FF)


def with_spikes(values, rng, source, target, shards_of, factor):
    def block_of(axis_at):
        return (jnp.arange(values.shape[axis_at]) // (values.shape[axis_at] // shards_of)).reshape((-1,) + (1,) * (values.ndim - 1 - axis_at))

    first = jax.random.permutation(rng, shards_of)[block_of(target)]
    other_side = (block_of(target) + shards_of // 2) % shards_of
    return jnp.where((block_of(source) == first) | (block_of(source) == other_side), factor * values, values)


def levels(stream_key, dims, pieces, least, largest):
    loudness = 1.0
    for axis_at, blocks in pieces:
        draws = jax.random.uniform(jax.random.fold_in(jax.random.fold_in(stream_key, 6), axis_at), (blocks,), jnp.float32, least / len(pieces), largest / len(pieces))
        loudness = loudness * jnp.repeat(jnp.exp(draws), dims[axis_at] // blocks).reshape((-1,) + (1,) * (len(dims) - 1 - axis_at))
    return loudness


def gaussian(stream_key, dims, deviation, limit, split=(), dtype=jnp.bfloat16):
    entries = deviation * jax.random.normal(stream_key, dims, jnp.float32)
    if split:
        entries = entries * levels(stream_key, dims, split, -0.22, 0.18)
    return jnp.clip(entries, -limit, limit).astype(dtype)


def bell_draw_with(stream_key, extent, scale, reach, pieces, heavy, held_as=jnp.bfloat16):
    entries = scale * jax.random.normal(stream_key, extent, jnp.float32)
    if pieces:
        entries = entries * levels(stream_key, extent, pieces, -0.22, 0.18)
    return jnp.clip(with_spikes(entries, jax.random.fold_in(stream_key, 3), *heavy), -reach, reach).astype(held_as)


def setup_inputs(seed: int = 0) -> dict:
    seeds = jax.random.split(jax.random.key(seed), 18)
    inputs = bell_draw_with(seeds[0], (TOKENS, D), 1.0, 6.0, ((0, 8),), (0, 1, 8, 2.0))
    cotangent = bell_draw_with(seeds[1], (TOKENS, D), 1.0, 6.0, ((0, 8),), (0, 1, 8, 2.0))
    master_inward = draw_master_inward(jax.random.fold_in(seeds[17], 71), 0)
    first_inward = gaussian(seeds[3], (3, D, D), (0.5 * TOKENS ** 0.5), 512.0, ((1, 8), (2, 4)), jnp.float32)
    second_inward = jnp.clip(jnp.exp(math.log(53312.0) - 2.7725887 * jax.random.uniform(seeds[4], (3, D, D), jnp.float32) ** levels(seeds[4], (3, D, D), ((1, 8), (2, 4)), -0.2, 0.2)), 3332.0, 53312.0)
    master_outward = draw_master_outward(jax.random.fold_in(seeds[17], 71), 0)
    first_outward = gaussian(seeds[6], (D, D), (0.32 * TOKENS ** 0.5), 320.0, ((0, 4), (1, 8)), jnp.float32)
    second_outward = jnp.clip(jnp.exp(math.log(21324.8) - 2.7725887 * jax.random.uniform(seeds[7], (D, D), jnp.float32) ** levels(seeds[7], (D, D), ((0, 4), (1, 8)), -0.2, 0.2)), 1332.8, 21324.8)
    master_widening = draw_master_widening(jax.random.fold_in(seeds[17], 71), 0)
    first_widening = gaussian(seeds[9], (D, FF), (0.32 * TOKENS ** 0.5), 320.0, ((0, 8), (1, 4)), jnp.float32)
    second_widening = jnp.clip(jnp.exp(math.log(21324.8) - 2.7725887 * jax.random.uniform(seeds[10], (D, FF), jnp.float32) ** levels(seeds[10], (D, FF), ((0, 8), (1, 4)), -0.2, 0.2)), 1332.8, 21324.8)
    master_narrowing = draw_master_narrowing(jax.random.fold_in(seeds[17], 71), 0)
    first_narrowing = gaussian(seeds[12], (FF, D), (0.63 * TOKENS ** 0.5), 640.0, ((0, 4), (1, 8)), jnp.float32)
    second_narrowing = jnp.clip(jnp.exp(math.log(85299.2) - 2.7725887 * jax.random.uniform(seeds[13], (FF, D), jnp.float32) ** levels(seeds[13], (FF, D), ((0, 4), (1, 8)), -0.2, 0.2)), 5331.2, 85299.2)
    master_scaling = jnp.clip(1.0 + 0.1 * jax.random.normal(seeds[14], (D,), jnp.float32), 0.5, 1.5)
    first_scaling = gaussian(seeds[15], (D,), (TOKENS ** 0.5), 1024.0, ((0, 8),), jnp.float32)
    second_scaling = jnp.clip(jnp.exp(math.log(213248.0) - 2.7725887 * jax.random.uniform(seeds[16], (D,), jnp.float32) ** levels(seeds[16], (D,), ((0, 8),), -0.2, 0.2)), 13328.0, 213248.0)
    return dict(inputs=inputs, cotangent=cotangent, master_inward=master_inward, first_inward=first_inward, second_inward=second_inward, master_outward=master_outward, first_outward=first_outward, second_outward=second_outward, master_widening=master_widening, first_widening=first_widening, second_widening=second_widening, master_narrowing=master_narrowing, first_narrowing=first_narrowing, second_narrowing=second_narrowing, master_scaling=master_scaling, first_scaling=first_scaling, second_scaling=second_scaling)


@jax.custom_vjp
def low(v):
    return lax.optimization_barrier(v.astype(jnp.bfloat16)).astype(jnp.float32)

@jax.custom_vjp
def low_back(v):
    return v

def low_keep(v):
    return (low(v), None)

def low_pass(kept, grad):
    return (grad,)

def back_keep(v):
    return (v, None)

def back_low(kept, grad):
    return (low(grad),)
low.defvjp(low_keep, low_pass)
low_back.defvjp(back_keep, back_low)
norm_eps = 1e-06
beta_one = 0.5
beta_two = 0.5
lamb_eps = 1e-06
weight_decay = 0.01
learn_rate = 0.5
highest = lax.Precision.HIGHEST

def working(master):
    return lax.optimization_barrier(master.astype(jnp.bfloat16)).astype(jnp.float32)

def attend_block(parts):
    query_rows, key_rows, value_rows = parts
    scores = low_back(jnp.einsum('bqhd,bkhd->bhqk', query_rows, key_rows, precision=highest) * HEAD_DIM ** (-0.5))
    probs = low(jax.nn.softmax(scores, axis=-1))
    return jnp.einsum('bhqk,bkhd->bqhd', probs, value_rows, precision=highest)

def forward(floats_in, scaling, inward, outward, widening, narrowing):
    centred = floats_in - lax.optimization_barrier(jnp.mean(floats_in, axis=1, keepdims=True))
    inv_std = lax.rsqrt(lax.optimization_barrier(jnp.mean(centred * centred, axis=1, keepdims=True)) + norm_eps)
    normed = low(centred * inv_std * scaling)
    projected = low(low_back(jnp.einsum('rd,tde->tre', normed, inward, precision=highest)))
    blocks = projected.reshape(3, N_DP, IMG_DEV, SEQ, HEADS, HEAD_DIM)
    attended = lax.map(jax.checkpoint(attend_block), (blocks[0], blocks[1], blocks[2]))
    attended = low(low_back(attended.reshape(TOKENS, HEADS * HEAD_DIM)))
    upper = low_back(jnp.dot(normed, widening, precision=highest))
    hidden = low(jax.nn.gelu(upper, approximate=True))
    branches = jnp.dot(attended, outward, precision=highest) + jnp.dot(hidden, narrowing, precision=highest)
    return floats_in + branches

def lamb_parts(master, first, second, grad):
    moment = beta_one * first + (1.0 - beta_one) * grad
    square = beta_two * second + (1.0 - beta_two) * grad * grad
    update = moment / (1.0 - beta_one ** STEP) / (jnp.sqrt(square / (1.0 - beta_two ** STEP)) + lamb_eps) + weight_decay * master
    weight_norm = jnp.sqrt(jnp.sum(master * master))
    update_norm = jnp.sqrt(jnp.sum(update * update))
    fresh = master - learn_rate * (weight_norm / update_norm) * update
    return (moment, square, fresh, fresh.astype(jnp.bfloat16), jnp.stack([weight_norm, update_norm]))

def reference(inputs, cotangent, master_inward, first_inward, second_inward, master_outward, first_outward, second_outward, master_widening, first_widening, second_widening, master_narrowing, first_narrowing, second_narrowing, master_scaling, first_scaling, second_scaling):
    floats_in = inputs.astype(jnp.float32)
    work_in = working(master_inward)
    work_out = working(master_outward)
    work_wide = working(master_widening)
    work_narrow = working(master_narrowing)
    work_scale = working(master_scaling)

    def whole(a_in, a_scale, a_inward, a_outward, a_wide, a_narrow):
        return forward(a_in, a_scale, a_inward, a_outward, a_wide, a_narrow)
    result, pull = jax.vjp(whole, floats_in, work_scale, work_in, work_out, work_wide, work_narrow)
    grads = pull(cotangent.astype(jnp.float32))
    output = result.astype(jnp.bfloat16)
    input_grad = grads[0].astype(jnp.bfloat16)
    part_in = lamb_parts(master_inward, first_inward, second_inward, grads[2])
    part_out = lamb_parts(master_outward, first_outward, second_outward, grads[3])
    part_wide = lamb_parts(master_widening, first_widening, second_widening, grads[4])
    part_narrow = lamb_parts(master_narrowing, first_narrowing, second_narrowing, grads[5])
    part_scale = lamb_parts(master_scaling, first_scaling, second_scaling, grads[1])
    trust_norms = jnp.stack([part_in[4], part_out[4], part_wide[4], part_narrow[4], part_scale[4]])
    return (output, input_grad, part_in[0], part_in[1], part_in[2], part_in[3], part_out[0], part_out[1], part_out[2], part_out[3], part_wide[0], part_wide[1], part_wide[2], part_wide[3], part_narrow[0], part_narrow[1], part_narrow[2], part_narrow[3], part_scale[0], part_scale[1], part_scale[2], part_scale[3], trust_norms)
```

```python
import functools

import jax
import jax.numpy as jnp
from jax import lax
from jax.experimental import pallas as pl
from jax.experimental.pallas import tpu as pltpu
from jax.sharding import PartitionSpec as P

MESH = pl.DeviceIdType.MESH
PAIR = 2

HEAD_DIM = 64
SEQ = 196
STEP = 5


norm_eps = 1e-06
beta_one = 0.5
beta_two = 0.5
lamb_eps = 1e-06
weight_decay = 0.01
learn_rate = 0.5


def lamb_parts(master, first, second, grad):
    moment = beta_one * first + (1.0 - beta_one) * grad
    square = beta_two * second + (1.0 - beta_two) * grad * grad
    update = (
        moment / (1.0 - beta_one**STEP) / (jnp.sqrt(square / (1.0 - beta_two**STEP)) + lamb_eps)
        + weight_decay * master
    )
    return (moment, square, update)


def greet(place, line, up, down, other):
    barrier = pltpu.get_barrier_semaphore()
    pl.semaphore_signal(barrier, inc=1, device_id=other, device_id_type=MESH)

    @pl.when(place < line - 1)
    def _():
        pl.semaphore_signal(barrier, inc=1, device_id=up, device_id_type=MESH)

    @pl.when(place > 0)
    def _():
        pl.semaphore_signal(barrier, inc=1, device_id=down, device_id_type=MESH)

    pl.semaphore_wait(barrier, 1 + jnp.minimum(place, 1) + jnp.minimum(line - 1 - place, 1))


def gather_kernel(line, own_ref, all_ref, own_sem, up_sem, down_sem, pair_sem, recv_sem):
    me = lax.axis_index("dp")
    place, side = me // PAIR, me % PAIR
    up, down, other = {"dp": me + PAIR}, {"dp": me - PAIR}, {"dp": me + 1 - 2 * side}
    has_up, has_down = place < line - 1, place > 0
    greet(place, line, up, down, other)

    def move(step, source, block, sems, peer):
        return pltpu.make_async_remote_copy(
            src_ref=source,
            dst_ref=all_ref.at[block],
            send_sem=sems.at[step],
            recv_sem=recv_sem.at[block],
            device_id=peer,
            device_id_type=MESH,
        )

    def held(block):
        return all_ref.at[block]

    def arrived(block, peer):
        move(0, held(block), block, pair_sem, peer).wait_recv()

    own = pltpu.make_async_copy(own_ref, all_ref.at[me], own_sem)

    @pl.when(has_up)
    def _():
        move(place, own_ref, me, up_sem, up).start()

    @pl.when(has_down)
    def _():
        move(place, own_ref, me, down_sem, down).start()

    move(place, own_ref, me, pair_sem, other).start()
    own.start()

    @pl.loop(1, line)
    def _(step):
        low, high = place - step, place + step

        @pl.when(low >= 0)
        def _():
            block = low * PAIR + side
            arrived(block, other)

            @pl.when(has_up)
            def _():
                move(low, held(block), block, up_sem, up).start()

            move(low, held(block), block, pair_sem, other).start()

        @pl.when(high < line)
        def _():
            block = high * PAIR + side
            arrived(block, other)

            @pl.when(has_down)
            def _():
                move(high, held(block), block, down_sem, down).start()

            move(high, held(block), block, pair_sem, other).start()

    own.wait()

    @pl.loop(0, line)
    def _(spot):
        block = spot * PAIR + side
        arrived(spot * PAIR + 1 - side, other)
        move(spot, held(block), block, pair_sem, other).wait_send()

        @pl.when(jnp.logical_and(has_up, spot <= place))
        def _():
            move(spot, held(block), block, up_sem, up).wait_send()

        @pl.when(jnp.logical_and(has_down, spot >= place))
        def _():
            move(spot, held(block), block, down_sem, down).wait_send()


def gather_blocks(own):
    rows, width = own.shape
    devices = lax.axis_size("dp")
    line = devices // PAIR
    return pl.pallas_call(
        functools.partial(gather_kernel, line),
        out_shape=jax.ShapeDtypeStruct((devices, rows, width), own.dtype),
        in_specs=[pl.BlockSpec(memory_space=pltpu.VMEM)],
        out_specs=pl.BlockSpec(memory_space=pl.ANY),
        scratch_shapes=[
            pltpu.SemaphoreType.DMA,
            pltpu.SemaphoreType.DMA((line,)),
            pltpu.SemaphoreType.DMA((line,)),
            pltpu.SemaphoreType.DMA((line,)),
            pltpu.SemaphoreType.DMA((devices,)),
        ],
        compiler_params=pltpu.CompilerParams(collective_id=0, has_side_effects=True),
        cost_estimate=pl.CostEstimate(flops=0, bytes_accessed=100_000_000, transcendentals=0),
        name="gather_blocks",
    )(own)


def reduce_kernel(
    line, own_ref, sum_ref, pair_in, up_in, down_in, up_out, down_out,
    pair_send, pair_recv, up_send, up_recv, down_send, down_recv,
):
    me = lax.axis_index("dp")
    place, side = me // PAIR, me % PAIR
    up, down, other = {"dp": me + PAIR}, {"dp": me - PAIR}, {"dp": me + 1 - 2 * side}
    has_up, has_down = place < line - 1, place > 0
    greet(place, line, up, down, other)

    def pair_move(spot):
        return pltpu.make_async_remote_copy(
            src_ref=own_ref.at[spot * PAIR + 1 - side],
            dst_ref=pair_in.at[spot],
            send_sem=pair_send.at[spot],
            recv_sem=pair_recv.at[spot],
            device_id=other,
            device_id_type=MESH,
        )

    def line_move(spot, source, target, sends, recvs, peer):
        return pltpu.make_async_remote_copy(
            src_ref=source.at[spot],
            dst_ref=target.at[spot],
            send_sem=sends.at[spot],
            recv_sem=recvs.at[spot],
            device_id=peer,
            device_id_type=MESH,
        )

    def up_move(spot):
        return line_move(spot, up_out, up_in, up_send, up_recv, up)

    def down_move(spot):
        return line_move(spot, down_out, down_in, down_send, down_recv, down)

    @pl.loop(0, line)
    def _(turn):
        far = line - 1 - turn

        @pl.when(place + far < line)
        def _():
            pair_move(place + far).start()

        @pl.when(jnp.logical_and(place - far >= 0, far > 0))
        def _():
            pair_move(place - far).start()

    def both(spot):
        return own_ref[spot * PAIR + side].astype(jnp.float32) + pair_in[spot].astype(jnp.float32)

    @pl.loop(0, line - 1)
    def _(turn):
        far = line - 1 - turn

        @pl.when(place + far < line)
        def _():
            spot = place + far
            pair_move(spot).wait_recv()

            @pl.when(has_down)
            def _():
                up_move(spot).wait_recv()
                up_out[spot] = (both(spot) + up_in[spot].astype(jnp.float32)).astype(jnp.bfloat16)

            @pl.when(jnp.logical_not(has_down))
            def _():
                up_out[spot] = both(spot).astype(jnp.bfloat16)

            up_move(spot).start()

        @pl.when(place - far >= 0)
        def _():
            spot = place - far
            pair_move(spot).wait_recv()

            @pl.when(has_up)
            def _():
                down_move(spot).wait_recv()
                down_out[spot] = (both(spot) + down_in[spot].astype(jnp.float32)).astype(
                    jnp.bfloat16
                )

            @pl.when(jnp.logical_not(has_up))
            def _():
                down_out[spot] = both(spot).astype(jnp.bfloat16)

            down_move(spot).start()

    pair_move(place).wait_recv()
    sum_ref[...] = both(place)

    @pl.when(has_down)
    def _():
        up_move(place).wait_recv()
        sum_ref[...] += up_in[place].astype(jnp.float32)

    @pl.when(has_up)
    def _():
        down_move(place).wait_recv()
        sum_ref[...] += down_in[place].astype(jnp.float32)

    @pl.loop(0, line)
    def _(spot):
        pair_move(spot).wait_send()

        @pl.when(spot > place)
        def _():
            up_move(spot).wait_send()

        @pl.when(spot < place)
        def _():
            down_move(spot).wait_send()


def reduce_blocks(own):
    devices, rows, width = own.shape
    line = devices // PAIR
    buffer = pltpu.VMEM((line, rows, width), own.dtype)
    return pl.pallas_call(
        functools.partial(reduce_kernel, line),
        out_shape=jax.ShapeDtypeStruct((rows, width), jnp.float32),
        in_specs=[pl.BlockSpec(memory_space=pltpu.VMEM)],
        out_specs=pl.BlockSpec(memory_space=pltpu.VMEM),
        scratch_shapes=[buffer] * 5 + [pltpu.SemaphoreType.DMA((line,))] * 6,
        compiler_params=pltpu.CompilerParams(
            collective_id=1, has_side_effects=True, vmem_limit_bytes=40 * 2**20
        ),
        cost_estimate=pl.CostEstimate(flops=0, bytes_accessed=100_000_000, transcendentals=0),
        name="reduce_blocks",
    )(own)


def total_kernel(
    devices, ranks, own_ref, sum_ref, rank_in, dp_out, dp_in,
    rank_send, rank_recv, dp_send, dp_recv,
):
    me, rank = lax.axis_index("dp"), lax.axis_index("tensor")
    barrier = pltpu.get_barrier_semaphore()
    for shift in range(1, ranks):
        peer = {"tensor": lax.rem(rank + shift, ranks)}
        pl.semaphore_signal(barrier, inc=1, device_id=peer, device_id_type=MESH)
    for shift in range(1, devices):
        peer = {"dp": lax.rem(me + shift, devices)}
        pl.semaphore_signal(barrier, inc=1, device_id=peer, device_id_type=MESH)
    pl.semaphore_wait(barrier, ranks - 1 + devices - 1)

    def rank_move(shift):
        return pltpu.make_async_remote_copy(
            src_ref=own_ref,
            dst_ref=rank_in.at[rank],
            send_sem=rank_send.at[shift],
            recv_sem=rank_recv.at[rank],
            device_id={"tensor": lax.rem(rank + shift, ranks)},
            device_id_type=MESH,
        )

    def rank_arrival(source):
        return pltpu.make_async_remote_copy(
            src_ref=own_ref,
            dst_ref=rank_in.at[source],
            send_sem=rank_send.at[0],
            recv_sem=rank_recv.at[source],
            device_id={"tensor": lax.rem(rank + 1, ranks)},
            device_id_type=MESH,
        )

    def dp_move(shift):
        return pltpu.make_async_remote_copy(
            src_ref=dp_out,
            dst_ref=dp_in.at[me],
            send_sem=dp_send.at[shift],
            recv_sem=dp_recv.at[me],
            device_id={"dp": lax.rem(me + shift, devices)},
            device_id_type=MESH,
        )

    def dp_arrival(source):
        return pltpu.make_async_remote_copy(
            src_ref=dp_out,
            dst_ref=dp_in.at[source],
            send_sem=dp_send.at[0],
            recv_sem=dp_recv.at[source],
            device_id={"dp": lax.rem(me + 1, devices)},
            device_id_type=MESH,
        )

    for shift in range(1, ranks):
        rank_move(shift).start()
    rank_in[rank] = own_ref[...]
    for shift in range(1, ranks):
        rank_arrival(lax.rem(rank + shift, ranks)).wait_recv()
    part = rank_in[0]
    for spot in range(1, ranks):
        part = part + rank_in[spot]
    dp_out[...] = part
    for shift in range(1, devices):
        dp_move(shift).start()
    dp_in[me] = part
    for shift in range(1, devices):
        dp_arrival(lax.rem(me + shift, devices)).wait_recv()
    whole = dp_in[0]
    for spot in range(1, devices):
        whole = whole + dp_in[spot]
    sum_ref[...] = whole
    for shift in range(1, ranks):
        rank_move(shift).wait_send()
    for shift in range(1, devices):
        dp_move(shift).wait_send()


def total_of(own, collective_id):
    devices, ranks = lax.axis_size("dp"), lax.axis_size("tensor")
    return pl.pallas_call(
        functools.partial(total_kernel, devices, ranks),
        out_shape=jax.ShapeDtypeStruct(own.shape, own.dtype),
        in_specs=[pl.BlockSpec(memory_space=pltpu.VMEM)],
        out_specs=pl.BlockSpec(memory_space=pltpu.VMEM),
        scratch_shapes=[
            pltpu.VMEM((ranks,) + own.shape, own.dtype),
            pltpu.VMEM(own.shape, own.dtype),
            pltpu.VMEM((devices,) + own.shape, own.dtype),
            pltpu.SemaphoreType.DMA((ranks,)),
            pltpu.SemaphoreType.DMA((ranks,)),
            pltpu.SemaphoreType.DMA((devices,)),
            pltpu.SemaphoreType.DMA((devices,)),
        ],
        compiler_params=pltpu.CompilerParams(
            collective_id=collective_id, has_side_effects=True
        ),
        cost_estimate=pl.CostEstimate(flops=0, bytes_accessed=20_000_000, transcendentals=0),
        name="total_" + str(collective_id),
    )(own)


def gelu_tanh(values):
    return jax.nn.gelu(values, approximate=True)


def local(
    inputs,
    cotangent,
    master_inward,
    first_inward,
    second_inward,
    master_outward,
    first_outward,
    second_outward,
    master_widening,
    first_widening,
    second_widening,
    master_narrowing,
    first_narrowing,
    second_narrowing,
    master_scaling,
    first_scaling,
    second_scaling,
):
    depth = master_widening.shape[0]
    hidden_here = master_widening.shape[1]
    head_cols = master_inward.shape[2]
    model = inputs.shape[1]
    cuts = (hidden_here, 2 * hidden_here, 2 * hidden_here + 3 * head_cols)
    width = cuts[2] + head_cols
    gain_cols = 128 + (-width) % 128
    shard = jnp.concatenate(
        [
            master_widening,
            master_narrowing.T,
            jnp.transpose(master_inward, (1, 0, 2)).reshape(depth, 3 * head_cols),
            master_outward.T,
            jnp.broadcast_to(master_scaling[:, None], (depth, gain_cols)),
        ],
        axis=1,
    ).astype(jnp.bfloat16)
    copies = gather_blocks(shard).reshape(model, width + gain_cols)
    widening = copies[:, : cuts[0]]
    narrowing_t = copies[:, cuts[0] : cuts[1]]
    inward = copies[:, cuts[1] : cuts[2]]
    outward_t = copies[:, cuts[2] : width]
    scaling = copies[:, width]
    floats_in = inputs.astype(jnp.float32)
    rows_here = floats_in.shape[0]
    images = rows_here // SEQ
    heads_here = head_cols // HEAD_DIM
    factor = HEAD_DIM ** (-0.5)
    centred = floats_in - jnp.mean(floats_in, axis=1, keepdims=True)
    inv_std = lax.rsqrt(jnp.mean(centred * centred, axis=1, keepdims=True) + norm_eps)
    unit_rows = centred * inv_std
    gain_rows = scaling.astype(jnp.float32)
    normed = (unit_rows * gain_rows).astype(jnp.bfloat16)
    projected = jnp.dot(normed, inward, preferred_element_type=jnp.float32).astype(jnp.bfloat16)
    query_rows, key_rows, value_rows = (
        projected[:, i * head_cols : (i + 1) * head_cols].reshape(
            images, SEQ, heads_here, HEAD_DIM
        )
        for i in range(3)
    )
    scores = (
        jnp.einsum("bqhd,bkhd->bhqk", query_rows, key_rows, preferred_element_type=jnp.float32)
        * factor
    )
    peak = jnp.max(scores, axis=-1, keepdims=True)
    log_total = peak + jnp.log(jnp.sum(jnp.exp(scores - peak), axis=-1, keepdims=True))
    probs_low = jnp.exp(scores - log_total).astype(jnp.bfloat16)
    attended = jnp.einsum(
        "bhqk,bkhd->bqhd", probs_low, value_rows, preferred_element_type=jnp.float32
    )
    attended = attended.astype(jnp.bfloat16).reshape(rows_here, heads_here * HEAD_DIM)
    upper = jnp.dot(normed, widening, preferred_element_type=jnp.float32)
    hidden = gelu_tanh(upper).astype(jnp.bfloat16)
    partial_sum = jnp.einsum(
        "re,de->rd", attended, outward_t, preferred_element_type=jnp.float32
    ) + jnp.einsum("rf,df->rd", hidden, narrowing_t, preferred_element_type=jnp.float32)
    share = rows_here // lax.axis_size("tensor")
    start = lax.axis_index("tensor") * share
    total = lax.psum_scatter(
        partial_sum.astype(jnp.bfloat16), "tensor", scatter_dimension=0, tiled=True
    )
    inputs_mine = lax.dynamic_slice_in_dim(inputs, start, share, 0).astype(jnp.float32)
    output = (inputs_mine + total.astype(jnp.float32)).astype(jnp.bfloat16)
    d_attended = jnp.dot(cotangent, outward_t, preferred_element_type=jnp.float32).astype(
        jnp.bfloat16
    )
    d_hidden = jnp.dot(cotangent, narrowing_t, preferred_element_type=jnp.float32)
    gelu_value, gelu_pull = jax.vjp(gelu_tanh, upper)
    d_upper = gelu_pull(d_hidden)[0].astype(jnp.bfloat16)
    back_sum = jnp.einsum("rf,df->rd", d_upper, widening, preferred_element_type=jnp.float32)
    d_att_blocks = d_attended.reshape(images, SEQ, heads_here, HEAD_DIM)
    rescored = (
        jnp.einsum("bqhd,bkhd->bhqk", query_rows, key_rows, preferred_element_type=jnp.float32)
        * factor
    )
    probs_full = jnp.exp(rescored - log_total)
    probs_again = probs_full.astype(jnp.bfloat16)
    d_probs = jnp.einsum(
        "bqhd,bkhd->bhqk", d_att_blocks, value_rows, preferred_element_type=jnp.float32
    )
    d_value = jnp.einsum(
        "bhqk,bqhd->bkhd", probs_again, d_att_blocks, preferred_element_type=jnp.float32
    ).astype(jnp.bfloat16)
    inner = jnp.sum(probs_full * d_probs, axis=-1, keepdims=True)
    d_scores = (probs_full * (d_probs - inner)).astype(jnp.bfloat16)
    d_query = (
        jnp.einsum("bhqk,bkhd->bqhd", d_scores, key_rows, preferred_element_type=jnp.float32)
        * factor
    ).astype(jnp.bfloat16)
    d_key = (
        jnp.einsum("bhqk,bqhd->bkhd", d_scores, query_rows, preferred_element_type=jnp.float32)
        * factor
    ).astype(jnp.bfloat16)
    d_projected = jnp.concatenate(
        [d.reshape(rows_here, head_cols) for d in (d_query, d_key, d_value)], axis=1
    )
    back_sum = back_sum + jnp.einsum(
        "re,de->rd", d_projected, inward, preferred_element_type=jnp.float32
    )
    d_normed = lax.psum_scatter(
        back_sum.astype(jnp.bfloat16), "tensor", scatter_dimension=0, tiled=True
    ).astype(jnp.float32)

    def weight_grad(rows, columns):
        return jnp.einsum("rd,rf->df", rows, columns, preferred_element_type=jnp.float32)

    grads = jnp.concatenate(
        [
            weight_grad(normed, d_upper).astype(jnp.bfloat16),
            weight_grad(cotangent, hidden).astype(jnp.bfloat16),
            weight_grad(normed, d_projected).astype(jnp.bfloat16),
            weight_grad(cotangent, attended).astype(jnp.bfloat16),
        ],
        axis=1,
    )
    centred_mine = inputs_mine - jnp.mean(inputs_mine, axis=1, keepdims=True)
    inv_mine = lax.rsqrt(jnp.mean(centred_mine * centred_mine, axis=1, keepdims=True) + norm_eps)
    unit_mine = centred_mine * inv_mine
    grad_scaling = jnp.sum(d_normed * unit_mine, axis=0)
    d_unit = d_normed * gain_rows
    d_floats = inv_mine * (
        d_unit
        - jnp.mean(d_unit, axis=1, keepdims=True)
        - unit_mine * jnp.mean(d_unit * unit_mine, axis=1, keepdims=True)
    )
    cotangent_mine = lax.dynamic_slice_in_dim(cotangent, start, share, 0).astype(jnp.float32)
    input_grad = lax.all_gather(
        (cotangent_mine + d_floats).astype(jnp.bfloat16), "tensor", axis=0, tiled=True
    )
    grad_scaling = total_of(grad_scaling.reshape(-1, 128), 2).reshape(-1)
    grad_scaling = lax.dynamic_slice_in_dim(
        grad_scaling, lax.axis_index("dp") * depth, depth, 0
    )
    summed = reduce_blocks(grads.reshape(lax.axis_size("dp"), depth, width))
    grad_widening = summed[:, : cuts[0]]
    grad_narrowing = summed[:, cuts[0] : cuts[1]].T
    grad_inward = jnp.transpose(
        summed[:, cuts[1] : cuts[2]].reshape(depth, 3, head_cols), (1, 0, 2)
    )
    grad_outward = summed[:, cuts[2] :].T
    part_in = lamb_parts(master_inward, first_inward, second_inward, grad_inward)
    part_out = lamb_parts(master_outward, first_outward, second_outward, grad_outward)
    part_wide = lamb_parts(master_widening, first_widening, second_widening, grad_widening)
    part_narrow = lamb_parts(master_narrowing, first_narrowing, second_narrowing, grad_narrowing)
    part_scale = lamb_parts(master_scaling, first_scaling, second_scaling, grad_scaling)
    replicas = 1.0 / lax.axis_size("tensor")
    local_sums = jnp.stack(
        [
            jnp.stack([jnp.sum(master_inward * master_inward), jnp.sum(part_in[2] * part_in[2])]),
            jnp.stack(
                [jnp.sum(master_outward * master_outward), jnp.sum(part_out[2] * part_out[2])]
            ),
            jnp.stack(
                [jnp.sum(master_widening * master_widening), jnp.sum(part_wide[2] * part_wide[2])]
            ),
            jnp.stack(
                [
                    jnp.sum(master_narrowing * master_narrowing),
                    jnp.sum(part_narrow[2] * part_narrow[2]),
                ]
            ),
            jnp.stack(
                [jnp.sum(master_scaling * master_scaling), jnp.sum(part_scale[2] * part_scale[2])]
            )
            * replicas,
        ]
    )
    packed = jnp.zeros((8, 128), jnp.float32).at[:5, :2].set(local_sums)
    trust_norms = jnp.sqrt(total_of(packed, 3)[:5, :2])
    fresh_in = master_inward - learn_rate * (trust_norms[0, 0] / trust_norms[0, 1]) * part_in[2]
    fresh_out = master_outward - learn_rate * (trust_norms[1, 0] / trust_norms[1, 1]) * part_out[2]
    fresh_wide = (
        master_widening - learn_rate * (trust_norms[2, 0] / trust_norms[2, 1]) * part_wide[2]
    )
    fresh_narrow = (
        master_narrowing - learn_rate * (trust_norms[3, 0] / trust_norms[3, 1]) * part_narrow[2]
    )
    fresh_scale = (
        master_scaling - learn_rate * (trust_norms[4, 0] / trust_norms[4, 1]) * part_scale[2]
    )
    return (
        output,
        input_grad,
        part_in[0],
        part_in[1],
        fresh_in,
        fresh_in.astype(jnp.bfloat16),
        part_out[0],
        part_out[1],
        fresh_out,
        fresh_out.astype(jnp.bfloat16),
        part_wide[0],
        part_wide[1],
        fresh_wide,
        fresh_wide.astype(jnp.bfloat16),
        part_narrow[0],
        part_narrow[1],
        fresh_narrow,
        fresh_narrow.astype(jnp.bfloat16),
        part_scale[0],
        part_scale[1],
        fresh_scale,
        fresh_scale.astype(jnp.bfloat16),
        trust_norms,
    )


def solution(mesh):
    in_specs = (
        P("dp", None),
        P("dp", None),
        P(None, "dp", "tensor"),
        P(None, "dp", "tensor"),
        P(None, "dp", "tensor"),
        P("tensor", "dp"),
        P("tensor", "dp"),
        P("tensor", "dp"),
        P("dp", "tensor"),
        P("dp", "tensor"),
        P("dp", "tensor"),
        P("tensor", "dp"),
        P("tensor", "dp"),
        P("tensor", "dp"),
        P("dp"),
        P("dp"),
        P("dp"),
    )
    out_specs = (
        P(("dp", "tensor"), None),
        P("dp", None),
        P(None, "dp", "tensor"),
        P(None, "dp", "tensor"),
        P(None, "dp", "tensor"),
        P(None, "dp", "tensor"),
        P("tensor", "dp"),
        P("tensor", "dp"),
        P("tensor", "dp"),
        P("tensor", "dp"),
        P("dp", "tensor"),
        P("dp", "tensor"),
        P("dp", "tensor"),
        P("dp", "tensor"),
        P("tensor", "dp"),
        P("tensor", "dp"),
        P("tensor", "dp"),
        P("tensor", "dp"),
        P("dp"),
        P("dp"),
        P("dp"),
        P("dp"),
        P(),
    )
    return jax.shard_map(local, mesh=mesh, in_specs=in_specs, out_specs=out_specs, check_vma=False)
```

```python
import functools

import jax
import jax.numpy as jnp
from jax import lax
from jax.experimental import pallas as pl
from jax.experimental.pallas import tpu as pltpu
from jax.sharding import PartitionSpec as P

MESH = pl.DeviceIdType.MESH
PAIR = 2

HEAD_DIM = 64
SEQ = 196
STEP = 5


norm_eps = 1e-06
beta_one = 0.5
beta_two = 0.5
lamb_eps = 1e-06
weight_decay = 0.01
learn_rate = 0.5


def lamb_parts(master, first, second, grad):
    moment = beta_one * first + (1.0 - beta_one) * grad
    square = beta_two * second + (1.0 - beta_two) * grad * grad
    update = (
        moment / (1.0 - beta_one**STEP) / (jnp.sqrt(square / (1.0 - beta_two**STEP)) + lamb_eps)
        + weight_decay * master
    )
    return (moment, square, update)


def greet(place, line, up, down, other):
    barrier = pltpu.get_barrier_semaphore()
    pl.semaphore_signal(barrier, inc=1, device_id=other, device_id_type=MESH)

    @pl.when(place < line - 1)
    def _():
        pl.semaphore_signal(barrier, inc=1, device_id=up, device_id_type=MESH)

    @pl.when(place > 0)
    def _():
        pl.semaphore_signal(barrier, inc=1, device_id=down, device_id_type=MESH)

    pl.semaphore_wait(barrier, 1 + jnp.minimum(place, 1) + jnp.minimum(line - 1 - place, 1))


def gather_kernel(line, own_ref, all_ref, own_sem, up_sem, down_sem, pair_sem, recv_sem):
    me = lax.axis_index("dp")
    place, side = me // PAIR, me % PAIR
    up, down, other = {"dp": me + PAIR}, {"dp": me - PAIR}, {"dp": me + 1 - 2 * side}
    has_up, has_down = place < line - 1, place > 0
    greet(place, line, up, down, other)

    def move(step, source, block, sems, peer):
        return pltpu.make_async_remote_copy(
            src_ref=source,
            dst_ref=all_ref.at[block],
            send_sem=sems.at[step],
            recv_sem=recv_sem.at[block],
            device_id=peer,
            device_id_type=MESH,
        )

    def held(block):
        return all_ref.at[block]

    def arrived(block, peer):
        move(0, held(block), block, pair_sem, peer).wait_recv()

    own = pltpu.make_async_copy(own_ref, all_ref.at[me], own_sem)

    @pl.when(has_up)
    def _():
        move(place, own_ref, me, up_sem, up).start()

    @pl.when(has_down)
    def _():
        move(place, own_ref, me, down_sem, down).start()

    move(place, own_ref, me, pair_sem, other).start()
    own.start()

    @pl.loop(1, line)
    def _(step):
        low, high = place - step, place + step

        @pl.when(low >= 0)
        def _():
            block = low * PAIR + side
            arrived(block, other)

            @pl.when(has_up)
            def _():
                move(low, held(block), block, up_sem, up).start()

            move(low, held(block), block, pair_sem, other).start()

        @pl.when(high < line)
        def _():
            block = high * PAIR + side
            arrived(block, other)

            @pl.when(has_down)
            def _():
                move(high, held(block), block, down_sem, down).start()

            move(high, held(block), block, pair_sem, other).start()

    own.wait()

    @pl.loop(0, line)
    def _(spot):
        block = spot * PAIR + side
        arrived(spot * PAIR + 1 - side, other)
        move(spot, held(block), block, pair_sem, other).wait_send()

        @pl.when(jnp.logical_and(has_up, spot <= place))
        def _():
            move(spot, held(block), block, up_sem, up).wait_send()

        @pl.when(jnp.logical_and(has_down, spot >= place))
        def _():
            move(spot, held(block), block, down_sem, down).wait_send()


def gather_blocks(own):
    rows, width = own.shape
    devices = lax.axis_size("dp")
    line = devices // PAIR
    return pl.pallas_call(
        functools.partial(gather_kernel, line),
        out_shape=jax.ShapeDtypeStruct((devices, rows, width), own.dtype),
        in_specs=[pl.BlockSpec(memory_space=pltpu.VMEM)],
        out_specs=pl.BlockSpec(memory_space=pl.ANY),
        scratch_shapes=[
            pltpu.SemaphoreType.DMA,
            pltpu.SemaphoreType.DMA((line,)),
            pltpu.SemaphoreType.DMA((line,)),
            pltpu.SemaphoreType.DMA((line,)),
            pltpu.SemaphoreType.DMA((devices,)),
        ],
        compiler_params=pltpu.CompilerParams(collective_id=0, has_side_effects=True),
        cost_estimate=pl.CostEstimate(flops=0, bytes_accessed=100_000_000, transcendentals=0),
        name="gather_blocks",
    )(own)


def reduce_kernel(
    line, own_ref, sum_ref, pair_in, up_in, down_in, up_out, down_out,
    pair_send, pair_recv, up_send, up_recv, down_send, down_recv,
):
    me = lax.axis_index("dp")
    place, side = me // PAIR, me % PAIR
    up, down, other = {"dp": me + PAIR}, {"dp": me - PAIR}, {"dp": me + 1 - 2 * side}
    has_up, has_down = place < line - 1, place > 0
    greet(place, line, up, down, other)

    def pair_move(spot):
        return pltpu.make_async_remote_copy(
            src_ref=own_ref.at[spot * PAIR + 1 - side],
            dst_ref=pair_in.at[spot],
            send_sem=pair_send.at[spot],
            recv_sem=pair_recv.at[spot],
            device_id=other,
            device_id_type=MESH,
        )

    def line_move(spot, source, target, sends, recvs, peer):
        return pltpu.make_async_remote_copy(
            src_ref=source.at[spot],
            dst_ref=target.at[spot],
            send_sem=sends.at[spot],
            recv_sem=recvs.at[spot],
            device_id=peer,
            device_id_type=MESH,
        )

    def up_move(spot):
        return line_move(spot, up_out, up_in, up_send, up_recv, up)

    def down_move(spot):
        return line_move(spot, down_out, down_in, down_send, down_recv, down)

    @pl.loop(0, line)
    def _(turn):
        far = line - 1 - turn

        @pl.when(place + far < line)
        def _():
            pair_move(place + far).start()

        @pl.when(jnp.logical_and(place - far >= 0, far > 0))
        def _():
            pair_move(place - far).start()

    def both(spot):
        return own_ref[spot * PAIR + side].astype(jnp.float32) + pair_in[spot].astype(jnp.float32)

    @pl.loop(0, line - 1)
    def _(turn):
        far = line - 1 - turn

        @pl.when(place + far < line)
        def _():
            spot = place + far
            pair_move(spot).wait_recv()

            @pl.when(has_down)
            def _():
                up_move(spot).wait_recv()
                up_out[spot] = (both(spot) + up_in[spot].astype(jnp.float32)).astype(jnp.bfloat16)

            @pl.when(jnp.logical_not(has_down))
            def _():
                up_out[spot] = both(spot).astype(jnp.bfloat16)

            up_move(spot).start()

        @pl.when(place - far >= 0)
        def _():
            spot = place - far
            pair_move(spot).wait_recv()

            @pl.when(has_up)
            def _():
                down_move(spot).wait_recv()
                down_out[spot] = (both(spot) + down_in[spot].astype(jnp.float32)).astype(
                    jnp.bfloat16
                )

            @pl.when(jnp.logical_not(has_up))
            def _():
                down_out[spot] = both(spot).astype(jnp.bfloat16)

            down_move(spot).start()

    pair_move(place).wait_recv()
    sum_ref[...] = both(place)

    @pl.when(has_down)
    def _():
        up_move(place).wait_recv()
        sum_ref[...] += up_in[place].astype(jnp.float32)

    @pl.when(has_up)
    def _():
        down_move(place).wait_recv()
        sum_ref[...] += down_in[place].astype(jnp.float32)

    @pl.loop(0, line)
    def _(spot):
        pair_move(spot).wait_send()

        @pl.when(spot > place)
        def _():
            up_move(spot).wait_send()

        @pl.when(spot < place)
        def _():
            down_move(spot).wait_send()


def reduce_blocks(own):
    devices, rows, width = own.shape
    line = devices // PAIR
    buffer = pltpu.VMEM((line, rows, width), own.dtype)
    return pl.pallas_call(
        functools.partial(reduce_kernel, line),
        out_shape=jax.ShapeDtypeStruct((rows, width), jnp.float32),
        in_specs=[pl.BlockSpec(memory_space=pltpu.VMEM)],
        out_specs=pl.BlockSpec(memory_space=pltpu.VMEM),
        scratch_shapes=[buffer] * 5 + [pltpu.SemaphoreType.DMA((line,))] * 6,
        compiler_params=pltpu.CompilerParams(
            collective_id=1, has_side_effects=True, vmem_limit_bytes=40 * 2**20
        ),
        cost_estimate=pl.CostEstimate(flops=0, bytes_accessed=100_000_000, transcendentals=0),
        name="reduce_blocks",
    )(own)


def total_kernel(
    devices, ranks, own_ref, sum_ref, rank_in, dp_out, dp_in,
    rank_send, rank_recv, dp_send, dp_recv,
):
    me, rank = lax.axis_index("dp"), lax.axis_index("tensor")
    barrier = pltpu.get_barrier_semaphore()
    for shift in range(1, ranks):
        peer = {"tensor": lax.rem(rank + shift, ranks)}
        pl.semaphore_signal(barrier, inc=1, device_id=peer, device_id_type=MESH)
    for shift in range(1, devices):
        peer = {"dp": lax.rem(me + shift, devices)}
        pl.semaphore_signal(barrier, inc=1, device_id=peer, device_id_type=MESH)
    pl.semaphore_wait(barrier, ranks - 1 + devices - 1)

    def rank_move(shift):
        return pltpu.make_async_remote_copy(
            src_ref=own_ref,
            dst_ref=rank_in.at[rank],
            send_sem=rank_send.at[shift],
            recv_sem=rank_recv.at[rank],
            device_id={"tensor": lax.rem(rank + shift, ranks)},
            device_id_type=MESH,
        )

    def rank_arrival(source):
        return pltpu.make_async_remote_copy(
            src_ref=own_ref,
            dst_ref=rank_in.at[source],
            send_sem=rank_send.at[0],
            recv_sem=rank_recv.at[source],
            device_id={"tensor": lax.rem(rank + 1, ranks)},
            device_id_type=MESH,
        )

    def dp_move(shift):
        return pltpu.make_async_remote_copy(
            src_ref=dp_out,
            dst_ref=dp_in.at[me],
            send_sem=dp_send.at[shift],
            recv_sem=dp_recv.at[me],
            device_id={"dp": lax.rem(me + shift, devices)},
            device_id_type=MESH,
        )

    def dp_arrival(source):
        return pltpu.make_async_remote_copy(
            src_ref=dp_out,
            dst_ref=dp_in.at[source],
            send_sem=dp_send.at[0],
            recv_sem=dp_recv.at[source],
            device_id={"dp": lax.rem(me + 1, devices)},
            device_id_type=MESH,
        )

    for shift in range(1, ranks):
        rank_move(shift).start()
    rank_in[rank] = own_ref[...]
    for shift in range(1, ranks):
        rank_arrival(lax.rem(rank + shift, ranks)).wait_recv()
    part = rank_in[0]
    for spot in range(1, ranks):
        part = part + rank_in[spot]
    dp_out[...] = part
    for shift in range(1, devices):
        dp_move(shift).start()
    dp_in[me] = part
    for shift in range(1, devices):
        dp_arrival(lax.rem(me + shift, devices)).wait_recv()
    whole = dp_in[0]
    for spot in range(1, devices):
        whole = whole + dp_in[spot]
    sum_ref[...] = whole
    for shift in range(1, ranks):
        rank_move(shift).wait_send()
    for shift in range(1, devices):
        dp_move(shift).wait_send()


def total_of(own, collective_id):
    devices, ranks = lax.axis_size("dp"), lax.axis_size("tensor")
    return pl.pallas_call(
        functools.partial(total_kernel, devices, ranks),
        out_shape=jax.ShapeDtypeStruct(own.shape, own.dtype),
        in_specs=[pl.BlockSpec(memory_space=pltpu.VMEM)],
        out_specs=pl.BlockSpec(memory_space=pltpu.VMEM),
        scratch_shapes=[
            pltpu.VMEM((ranks,) + own.shape, own.dtype),
            pltpu.VMEM(own.shape, own.dtype),
            pltpu.VMEM((devices,) + own.shape, own.dtype),
            pltpu.SemaphoreType.DMA((ranks,)),
            pltpu.SemaphoreType.DMA((ranks,)),
            pltpu.SemaphoreType.DMA((devices,)),
            pltpu.SemaphoreType.DMA((devices,)),
        ],
        compiler_params=pltpu.CompilerParams(
            collective_id=collective_id, has_side_effects=True
        ),
        cost_estimate=pl.CostEstimate(flops=0, bytes_accessed=20_000_000, transcendentals=0),
        name="total_" + str(collective_id),
    )(own)


def image_kernel(
    images, cuts, x_ref, c_ref, x_old_ref, c_old_ref, w1_ref, w2_ref, gain_ref,
    out_ref, grad_in_ref, g1_ref, g2_ref, g_gain_ref,
    acc1, acc2, qkv, back_cols, front_cols, partial, pair_in, chip_sum, line_in, total,
    s1, r1, s2, r2, s3, r3,
):
    step = pl.program_id(0)
    rank = lax.axis_index("tensor")
    core = rank % 2
    sibling = {"tensor": rank + 1 - 2 * core}
    across = {"tensor": lax.rem(rank + 2, 4)}
    width, head_cols = cuts
    heads = head_cols // HEAD_DIM
    rows, model = x_ref.shape[1], x_ref.shape[2]
    half = model // 2
    f32, b16 = jnp.float32, jnp.bfloat16

    @pl.when(step == 0)
    def _():
        barrier = pltpu.get_barrier_semaphore()
        pl.semaphore_signal(barrier, inc=1, device_id=sibling, device_id_type=MESH)
        pl.semaphore_signal(barrier, inc=1, device_id=across, device_id_type=MESH)
        pl.semaphore_wait(barrier, 2)
        acc1[...] = jnp.zeros_like(acc1)
        acc2[...] = jnp.zeros_like(acc2)
        g_gain_ref[...] = jnp.zeros_like(g_gain_ref)

    def move(source, target, sends, recvs, slot, peer):
        return pltpu.make_async_remote_copy(
            src_ref=source,
            dst_ref=target,
            send_sem=sends.at[slot],
            recv_sem=recvs.at[slot],
            device_id=peer,
            device_id_type=MESH,
        )

    def first(slot):
        return move(partial.at[slot, 1 - core], pair_in.at[slot], s1, r1, slot, sibling)

    def second(slot):
        return move(chip_sum.at[slot], line_in.at[slot], s2, r2, slot, across)

    def third(slot):
        return move(total.at[slot, core], total.at[slot, core], s3, r3, slot, sibling)

    def normalised(values):
        floats = values.astype(f32)
        centred = floats - jnp.mean(floats, axis=1, keepdims=True)
        inv_std = lax.rsqrt(jnp.mean(centred * centred, axis=1, keepdims=True) + norm_eps)
        return floats, centred * inv_std, inv_std

    gain = gain_ref[...].astype(f32)

    @pl.when(step >= 3)
    def _():
        slot = (step - 3) % 2
        third(slot).wait()
        floats, unit, inv_std = normalised(x_old_ref[0])
        sums = jnp.concatenate([total[slot, 0, 0], total[slot, 1, 0]], axis=1).astype(f32)
        out_ref[0] = (floats + sums).astype(b16)
        d_normed = jnp.concatenate([total[slot, 0, 1], total[slot, 1, 1]], axis=1).astype(f32)
        weighted = d_normed * unit
        g_gain_ref[...] += jnp.sum(weighted, axis=0, keepdims=True)
        d_unit = d_normed * gain
        d_floats = inv_std * (
            d_unit
            - jnp.mean(d_unit, axis=1, keepdims=True)
            - unit * jnp.mean(weighted * gain, axis=1, keepdims=True)
        )
        grad_in_ref[0] = (c_old_ref[0].astype(f32) + d_floats).astype(b16)

    @pl.when(jnp.logical_and(step >= 2, step < images + 2))
    def _():
        slot = (step - 2) % 2
        second(slot).wait()
        total[slot, core] = (chip_sum[slot].astype(f32) + line_in[slot].astype(f32)).astype(b16)
        third(slot).start()

    @pl.when(jnp.logical_and(step >= 1, step < images + 1))
    def _():
        slot = (step - 1) % 2
        first(slot).wait()
        chip_sum[slot] = (partial[slot, core].astype(f32) + pair_in[slot].astype(f32)).astype(b16)
        second(slot).start()

    @pl.when(step < images)
    def _():
        slot = step % 2
        _floats, unit, _inv = normalised(x_ref[0])
        normed = (unit * gain).astype(b16)
        cot = c_ref[0]

        def mm(a, b):
            return jnp.dot(a, b, preferred_element_type=f32)

        def mm_nt(a, b):
            return lax.dot_general(a, b, (((1,), (1,)), ((), ())), preferred_element_type=f32)

        def mm_tn(a, b):
            return lax.dot_general(a, b, (((0,), (0,)), ((), ())), preferred_element_type=f32)

        qkv[:, : 3 * head_cols] = mm(normed, w1_ref[:, width:]).astype(b16)
        qkv[:, 3 * head_cols :] = mm(cot, w2_ref[:, width:]).astype(b16)
        keys_wide = pl.cdiv(rows, 128) * 128
        filler = jnp.zeros((keys_wide - rows, HEAD_DIM), b16)
        real = lax.broadcasted_iota(jnp.int32, (rows, keys_wide), 1) < SEQ
        for head in range(heads):
            def part(kind):
                at = kind * head_cols + head * HEAD_DIM
                return qkv[:, at : at + HEAD_DIM]

            query = part(0) * jnp.asarray(HEAD_DIM ** (-0.5), b16)
            key = jnp.concatenate([part(1), filler], axis=0)
            value = jnp.concatenate([part(2), filler], axis=0)
            d_att = part(3)
            scores = jnp.where(real, mm_nt(query, key), -1e30)
            powers = jnp.exp(scores - jnp.max(scores, axis=1, keepdims=True))
            probs = powers * (1.0 / jnp.sum(powers, axis=1, keepdims=True))
            probs_low = probs.astype(b16)
            spot = head * HEAD_DIM
            front_cols[:, width + spot : width + spot + HEAD_DIM] = mm(probs_low, value).astype(b16)
            d_probs = mm_nt(d_att, value)
            d_value = mm_tn(probs_low, d_att)[:rows].astype(b16)
            inner = jnp.sum(probs * d_probs, axis=1, keepdims=True)
            d_scores = (probs * (d_probs - inner)).astype(b16)
            d_query = (mm(d_scores, key) * (HEAD_DIM ** (-0.5))).astype(b16)
            d_key = mm_tn(d_scores, query)[:rows].astype(b16)
            for kind, value_of in ((0, d_query), (1, d_key), (2, d_value)):
                at = width + kind * head_cols + spot
                back_cols[:, at : at + HEAD_DIM] = value_of

        upper = mm(normed, w1_ref[:, :width])
        d_hidden = mm(cot, w2_ref[:, :width])
        scale = (2.0 / 3.141592653589793) ** 0.5
        square = upper * upper
        bend = jnp.tanh(scale * upper * (1.0 + 0.044715 * square))
        step_up = 0.5 * (1.0 + bend)
        front_cols[:, :width] = (upper * step_up).astype(b16)
        slope = step_up + (0.5 * scale) * upper * (1.0 - bend * bend) * (
            1.0 + (3.0 * 0.044715) * square
        )
        back_cols[:, :width] = (d_hidden * slope).astype(b16)

        out_part = mm_nt(front_cols[...], w2_ref[...]).astype(b16)
        partial[slot, 0, 0] = out_part[:, :half]
        partial[slot, 1, 0] = out_part[:, half:]
        back_part = mm_nt(back_cols[...], w1_ref[...]).astype(b16)
        partial[slot, 0, 1] = back_part[:, :half]
        partial[slot, 1, 1] = back_part[:, half:]
        first(slot).start()
        acc1[...] += mm_tn(normed, back_cols[...])
        acc2[...] += mm_tn(cot, front_cols[...])

    @pl.when(step == images - 1)
    def _():
        g1_ref[...] = acc1[...].astype(b16)
        g2_ref[...] = acc2[...].astype(b16)


def image_block(inputs, cotangent, w1, w2, gain, width, head_cols):
    images, rows, model = inputs.shape
    half = model // 2
    now = lambda i: (jnp.minimum(i, images - 1), 0, 0)
    old = lambda i: (jnp.maximum(i - 3, 0), 0, 0)
    fixed = lambda i: (0, 0)
    block = (1, rows, model)

    def whole(shape):
        return pl.BlockSpec(shape, fixed, pipeline_mode=pl.Buffered(1))

    bf = jnp.bfloat16
    return pl.pallas_call(
        functools.partial(image_kernel, images, (width, head_cols)),
        grid=(images + 3,),
        out_shape=(
            jax.ShapeDtypeStruct(inputs.shape, bf),
            jax.ShapeDtypeStruct(inputs.shape, bf),
            jax.ShapeDtypeStruct(w1.shape, bf),
            jax.ShapeDtypeStruct(w2.shape, bf),
            jax.ShapeDtypeStruct((1, model), jnp.float32),
        ),
        in_specs=[
            pl.BlockSpec(block, now),
            pl.BlockSpec(block, now),
            pl.BlockSpec(block, old),
            pl.BlockSpec(block, old),
            whole(w1.shape),
            whole(w2.shape),
            whole((1, model)),
        ],
        out_specs=[
            pl.BlockSpec(block, old),
            pl.BlockSpec(block, old),
            whole(w1.shape),
            whole(w2.shape),
            whole((1, model)),
        ],
        scratch_shapes=[
            pltpu.VMEM(w1.shape, jnp.float32),
            pltpu.VMEM(w2.shape, jnp.float32),
            pltpu.VMEM((rows, 4 * head_cols), bf),
            pltpu.VMEM((rows, w1.shape[1]), bf),
            pltpu.VMEM((rows, w2.shape[1]), bf),
            pltpu.VMEM((2, 2, 2, rows, half), bf),
            pltpu.VMEM((2, 2, rows, half), bf),
            pltpu.VMEM((2, 2, rows, half), bf),
            pltpu.VMEM((2, 2, rows, half), bf),
            pltpu.VMEM((2, 2, 2, rows, half), bf),
        ]
        + [pltpu.SemaphoreType.DMA((2,))] * 6,
        compiler_params=pltpu.CompilerParams(
            collective_id=4,
            has_side_effects=True,
            vmem_limit_bytes=60 * 2**20,
            dimension_semantics=("arbitrary",),
        ),
        name="image_block",
    )(inputs, cotangent, inputs, cotangent, w1, w2, gain)


def local(
    inputs,
    cotangent,
    master_inward,
    first_inward,
    second_inward,
    master_outward,
    first_outward,
    second_outward,
    master_widening,
    first_widening,
    second_widening,
    master_narrowing,
    first_narrowing,
    second_narrowing,
    master_scaling,
    first_scaling,
    second_scaling,
):
    depth = master_widening.shape[0]
    hidden_here = master_widening.shape[1]
    head_cols = master_inward.shape[2]
    model = inputs.shape[1]
    cuts = (hidden_here, hidden_here + 3 * head_cols, 2 * hidden_here + 3 * head_cols)
    width = cuts[2] + head_cols
    gain_cols = 128 + (-width) % 128
    shard = jnp.concatenate(
        [
            master_widening,
            jnp.transpose(master_inward, (1, 0, 2)).reshape(depth, 3 * head_cols),
            master_narrowing.T,
            master_outward.T,
            jnp.broadcast_to(master_scaling[:, None], (depth, gain_cols)),
        ],
        axis=1,
    ).astype(jnp.bfloat16)
    copies = gather_blocks(shard).reshape(model, width + gain_cols)
    wide_cut = hidden_here + 3 * head_cols
    rows_here = inputs.shape[0]
    images = rows_here // SEQ
    padded = -(-SEQ // 16) * 16

    def by_image(values):
        return jnp.pad(
            values.reshape(images, SEQ, model), ((0, 0), (0, padded - SEQ), (0, 0))
        )

    summed_out, input_grad, grads_one, grads_two, grad_scaling = image_block(
        by_image(inputs),
        by_image(cotangent),
        copies[:, :wide_cut],
        copies[:, wide_cut:width],
        copies[:, width].reshape(1, model),
        hidden_here,
        head_cols,
    )
    share = rows_here // lax.axis_size("tensor")
    start = lax.axis_index("tensor") * share
    output = lax.dynamic_slice_in_dim(
        summed_out[:, :SEQ].reshape(rows_here, model), start, share, 0
    )
    input_grad = input_grad[:, :SEQ].reshape(rows_here, model)
    grads = jnp.concatenate([grads_one, grads_two], axis=1)
    grad_scaling = grad_scaling * (1.0 / lax.axis_size("tensor"))
    grad_scaling = total_of(grad_scaling.reshape(-1, 128), 2).reshape(-1)
    grad_scaling = lax.dynamic_slice_in_dim(
        grad_scaling, lax.axis_index("dp") * depth, depth, 0
    )
    summed = reduce_blocks(grads.reshape(lax.axis_size("dp"), depth, width))
    grad_widening = summed[:, : cuts[0]]
    grad_inward = jnp.transpose(
        summed[:, cuts[0] : cuts[1]].reshape(depth, 3, head_cols), (1, 0, 2)
    )
    grad_narrowing = summed[:, cuts[1] : cuts[2]].T
    grad_outward = summed[:, cuts[2] :].T
    part_in = lamb_parts(master_inward, first_inward, second_inward, grad_inward)
    part_out = lamb_parts(master_outward, first_outward, second_outward, grad_outward)
    part_wide = lamb_parts(master_widening, first_widening, second_widening, grad_widening)
    part_narrow = lamb_parts(master_narrowing, first_narrowing, second_narrowing, grad_narrowing)
    part_scale = lamb_parts(master_scaling, first_scaling, second_scaling, grad_scaling)
    replicas = 1.0 / lax.axis_size("tensor")
    local_sums = jnp.stack(
        [
            jnp.stack([jnp.sum(master_inward * master_inward), jnp.sum(part_in[2] * part_in[2])]),
            jnp.stack(
                [jnp.sum(master_outward * master_outward), jnp.sum(part_out[2] * part_out[2])]
            ),
            jnp.stack(
                [jnp.sum(master_widening * master_widening), jnp.sum(part_wide[2] * part_wide[2])]
            ),
            jnp.stack(
                [
                    jnp.sum(master_narrowing * master_narrowing),
                    jnp.sum(part_narrow[2] * part_narrow[2]),
                ]
            ),
            jnp.stack(
                [jnp.sum(master_scaling * master_scaling), jnp.sum(part_scale[2] * part_scale[2])]
            )
            * replicas,
        ]
    )
    packed = jnp.zeros((8, 128), jnp.float32).at[:5, :2].set(local_sums)
    trust_norms = jnp.sqrt(total_of(packed, 3)[:5, :2])
    fresh_in = master_inward - learn_rate * (trust_norms[0, 0] / trust_norms[0, 1]) * part_in[2]
    fresh_out = master_outward - learn_rate * (trust_norms[1, 0] / trust_norms[1, 1]) * part_out[2]
    fresh_wide = (
        master_widening - learn_rate * (trust_norms[2, 0] / trust_norms[2, 1]) * part_wide[2]
    )
    fresh_narrow = (
        master_narrowing - learn_rate * (trust_norms[3, 0] / trust_norms[3, 1]) * part_narrow[2]
    )
    fresh_scale = (
        master_scaling - learn_rate * (trust_norms[4, 0] / trust_norms[4, 1]) * part_scale[2]
    )
    return (
        output,
        input_grad,
        part_in[0],
        part_in[1],
        fresh_in,
        fresh_in.astype(jnp.bfloat16),
        part_out[0],
        part_out[1],
        fresh_out,
        fresh_out.astype(jnp.bfloat16),
        part_wide[0],
        part_wide[1],
        fresh_wide,
        fresh_wide.astype(jnp.bfloat16),
        part_narrow[0],
        part_narrow[1],
        fresh_narrow,
        fresh_narrow.astype(jnp.bfloat16),
        part_scale[0],
        part_scale[1],
        fresh_scale,
        fresh_scale.astype(jnp.bfloat16),
        trust_norms,
    )


def solution(mesh):
    in_specs = (
        P("dp", None),
        P("dp", None),
        P(None, "dp", "tensor"),
        P(None, "dp", "tensor"),
        P(None, "dp", "tensor"),
        P("tensor", "dp"),
        P("tensor", "dp"),
        P("tensor", "dp"),
        P("dp", "tensor"),
        P("dp", "tensor"),
        P("dp", "tensor"),
        P("tensor", "dp"),
        P("tensor", "dp"),
        P("tensor", "dp"),
        P("dp"),
        P("dp"),
        P("dp"),
    )
    out_specs = (
        P(("dp", "tensor"), None),
        P("dp", None),
        P(None, "dp", "tensor"),
        P(None, "dp", "tensor"),
        P(None, "dp", "tensor"),
        P(None, "dp", "tensor"),
        P("tensor", "dp"),
        P("tensor", "dp"),
        P("tensor", "dp"),
        P("tensor", "dp"),
        P("dp", "tensor"),
        P("dp", "tensor"),
        P("dp", "tensor"),
        P("dp", "tensor"),
        P("tensor", "dp"),
        P("tensor", "dp"),
        P("tensor", "dp"),
        P("tensor", "dp"),
        P("dp"),
        P("dp"),
        P("dp"),
        P("dp"),
        P(),
    )
    return jax.shard_map(local, mesh=mesh, in_specs=in_specs, out_specs=out_specs, check_vma=False)
```

```python
import functools

import jax
import jax.numpy as jnp
from jax import lax
from jax.experimental import pallas as pl
from jax.experimental.pallas import tpu as pltpu
from jax.sharding import PartitionSpec as P

MESH = pl.DeviceIdType.MESH
PAIR = 2

HEAD_DIM = 64
SEQ = 196
STEP = 5


norm_eps = 1e-06
beta_one = 0.5
beta_two = 0.5
lamb_eps = 1e-06
weight_decay = 0.01
learn_rate = 0.5


def lamb_parts(master, first, second, grad):
    moment = beta_one * first + (1.0 - beta_one) * grad
    square = beta_two * second + (1.0 - beta_two) * grad * grad
    update = (
        moment / (1.0 - beta_one**STEP) / (jnp.sqrt(square / (1.0 - beta_two**STEP)) + lamb_eps)
        + weight_decay * master
    )
    return (moment, square, update)


def greet(place, line, up, down, other):
    barrier = pltpu.get_barrier_semaphore()
    pl.semaphore_signal(barrier, inc=1, device_id=other, device_id_type=MESH)

    @pl.when(place < line - 1)
    def _():
        pl.semaphore_signal(barrier, inc=1, device_id=up, device_id_type=MESH)

    @pl.when(place > 0)
    def _():
        pl.semaphore_signal(barrier, inc=1, device_id=down, device_id_type=MESH)

    pl.semaphore_wait(barrier, 1 + jnp.minimum(place, 1) + jnp.minimum(line - 1 - place, 1))


def gather_kernel(line, own_ref, all_ref, own_sem, up_sem, down_sem, pair_sem, recv_sem):
    me = lax.axis_index("dp")
    place, side = me // PAIR, me % PAIR
    up, down, other = {"dp": me + PAIR}, {"dp": me - PAIR}, {"dp": me + 1 - 2 * side}
    has_up, has_down = place < line - 1, place > 0
    greet(place, line, up, down, other)

    def move(step, source, block, sems, peer):
        return pltpu.make_async_remote_copy(
            src_ref=source,
            dst_ref=all_ref.at[block],
            send_sem=sems.at[step],
            recv_sem=recv_sem.at[block],
            device_id=peer,
            device_id_type=MESH,
        )

    def held(block):
        return all_ref.at[block]

    def arrived(block, peer):
        move(0, held(block), block, pair_sem, peer).wait_recv()

    own = pltpu.make_async_copy(own_ref, all_ref.at[me], own_sem)

    @pl.when(has_up)
    def _():
        move(place, own_ref, me, up_sem, up).start()

    @pl.when(has_down)
    def _():
        move(place, own_ref, me, down_sem, down).start()

    move(place, own_ref, me, pair_sem, other).start()
    own.start()

    @pl.loop(1, line)
    def _(step):
        low, high = place - step, place + step

        @pl.when(low >= 0)
        def _():
            block = low * PAIR + side
            arrived(block, other)

            @pl.when(has_up)
            def _():
                move(low, held(block), block, up_sem, up).start()

            move(low, held(block), block, pair_sem, other).start()

        @pl.when(high < line)
        def _():
            block = high * PAIR + side
            arrived(block, other)

            @pl.when(has_down)
            def _():
                move(high, held(block), block, down_sem, down).start()

            move(high, held(block), block, pair_sem, other).start()

    own.wait()

    @pl.loop(0, line)
    def _(spot):
        block = spot * PAIR + side
        arrived(spot * PAIR + 1 - side, other)
        move(spot, held(block), block, pair_sem, other).wait_send()

        @pl.when(jnp.logical_and(has_up, spot <= place))
        def _():
            move(spot, held(block), block, up_sem, up).wait_send()

        @pl.when(jnp.logical_and(has_down, spot >= place))
        def _():
            move(spot, held(block), block, down_sem, down).wait_send()


def gather_blocks(own):
    rows, width = own.shape
    devices = lax.axis_size("dp")
    line = devices // PAIR
    return pl.pallas_call(
        functools.partial(gather_kernel, line),
        out_shape=jax.ShapeDtypeStruct((devices, rows, width), own.dtype),
        in_specs=[pl.BlockSpec(memory_space=pltpu.VMEM)],
        out_specs=pl.BlockSpec(memory_space=pl.ANY),
        scratch_shapes=[
            pltpu.SemaphoreType.DMA,
            pltpu.SemaphoreType.DMA((line,)),
            pltpu.SemaphoreType.DMA((line,)),
            pltpu.SemaphoreType.DMA((line,)),
            pltpu.SemaphoreType.DMA((devices,)),
        ],
        compiler_params=pltpu.CompilerParams(collective_id=0, has_side_effects=True),
        cost_estimate=pl.CostEstimate(flops=0, bytes_accessed=100_000_000, transcendentals=0),
        name="gather_blocks",
    )(own)


def reduce_kernel(
    line, own_ref, sum_ref, pair_in, up_in, down_in, up_out, down_out,
    pair_send, pair_recv, up_send, up_recv, down_send, down_recv,
):
    me = lax.axis_index("dp")
    place, side = me // PAIR, me % PAIR
    up, down, other = {"dp": me + PAIR}, {"dp": me - PAIR}, {"dp": me + 1 - 2 * side}
    has_up, has_down = place < line - 1, place > 0
    greet(place, line, up, down, other)

    def pair_move(spot):
        return pltpu.make_async_remote_copy(
            src_ref=own_ref.at[spot * PAIR + 1 - side],
            dst_ref=pair_in.at[spot],
            send_sem=pair_send.at[spot],
            recv_sem=pair_recv.at[spot],
            device_id=other,
            device_id_type=MESH,
        )

    def line_move(spot, source, target, sends, recvs, peer):
        return pltpu.make_async_remote_copy(
            src_ref=source.at[spot],
            dst_ref=target.at[spot],
            send_sem=sends.at[spot],
            recv_sem=recvs.at[spot],
            device_id=peer,
            device_id_type=MESH,
        )

    def up_move(spot):
        return line_move(spot, up_out, up_in, up_send, up_recv, up)

    def down_move(spot):
        return line_move(spot, down_out, down_in, down_send, down_recv, down)

    @pl.loop(0, line)
    def _(turn):
        far = line - 1 - turn

        @pl.when(place + far < line)
        def _():
            pair_move(place + far).start()

        @pl.when(jnp.logical_and(place - far >= 0, far > 0))
        def _():
            pair_move(place - far).start()

    def both(spot):
        return own_ref[spot * PAIR + side].astype(jnp.float32) + pair_in[spot].astype(jnp.float32)

    @pl.loop(0, line - 1)
    def _(turn):
        far = line - 1 - turn

        @pl.when(place + far < line)
        def _():
            spot = place + far
            pair_move(spot).wait_recv()

            @pl.when(has_down)
            def _():
                up_move(spot).wait_recv()
                up_out[spot] = (both(spot) + up_in[spot].astype(jnp.float32)).astype(jnp.bfloat16)

            @pl.when(jnp.logical_not(has_down))
            def _():
                up_out[spot] = both(spot).astype(jnp.bfloat16)

            up_move(spot).start()

        @pl.when(place - far >= 0)
        def _():
            spot = place - far
            pair_move(spot).wait_recv()

            @pl.when(has_up)
            def _():
                down_move(spot).wait_recv()
                down_out[spot] = (both(spot) + down_in[spot].astype(jnp.float32)).astype(
                    jnp.bfloat16
                )

            @pl.when(jnp.logical_not(has_up))
            def _():
                down_out[spot] = both(spot).astype(jnp.bfloat16)

            down_move(spot).start()

    pair_move(place).wait_recv()
    sum_ref[...] = both(place)

    @pl.when(has_down)
    def _():
        up_move(place).wait_recv()
        sum_ref[...] += up_in[place].astype(jnp.float32)

    @pl.when(has_up)
    def _():
        down_move(place).wait_recv()
        sum_ref[...] += down_in[place].astype(jnp.float32)

    @pl.loop(0, line)
    def _(spot):
        pair_move(spot).wait_send()

        @pl.when(spot > place)
        def _():
            up_move(spot).wait_send()

        @pl.when(spot < place)
        def _():
            down_move(spot).wait_send()


def reduce_blocks(own):
    devices, rows, width = own.shape
    line = devices // PAIR
    buffer = pltpu.VMEM((line, rows, width), own.dtype)
    return pl.pallas_call(
        functools.partial(reduce_kernel, line),
        out_shape=jax.ShapeDtypeStruct((rows, width), jnp.float32),
        in_specs=[pl.BlockSpec(memory_space=pltpu.VMEM)],
        out_specs=pl.BlockSpec(memory_space=pltpu.VMEM),
        scratch_shapes=[buffer] * 5 + [pltpu.SemaphoreType.DMA((line,))] * 6,
        compiler_params=pltpu.CompilerParams(
            collective_id=1, has_side_effects=True, vmem_limit_bytes=40 * 2**20
        ),
        cost_estimate=pl.CostEstimate(flops=0, bytes_accessed=100_000_000, transcendentals=0),
        name="reduce_blocks",
    )(own)


def total_kernel(
    devices, ranks, own_ref, sum_ref, rank_in, dp_out, dp_in,
    rank_send, rank_recv, dp_send, dp_recv,
):
    me, rank = lax.axis_index("dp"), lax.axis_index("tensor")
    barrier = pltpu.get_barrier_semaphore()
    for shift in range(1, ranks):
        peer = {"tensor": lax.rem(rank + shift, ranks)}
        pl.semaphore_signal(barrier, inc=1, device_id=peer, device_id_type=MESH)
    for shift in range(1, devices):
        peer = {"dp": lax.rem(me + shift, devices)}
        pl.semaphore_signal(barrier, inc=1, device_id=peer, device_id_type=MESH)
    pl.semaphore_wait(barrier, ranks - 1 + devices - 1)

    def rank_move(shift):
        return pltpu.make_async_remote_copy(
            src_ref=own_ref,
            dst_ref=rank_in.at[rank],
            send_sem=rank_send.at[shift],
            recv_sem=rank_recv.at[rank],
            device_id={"tensor": lax.rem(rank + shift, ranks)},
            device_id_type=MESH,
        )

    def rank_arrival(source):
        return pltpu.make_async_remote_copy(
            src_ref=own_ref,
            dst_ref=rank_in.at[source],
            send_sem=rank_send.at[0],
            recv_sem=rank_recv.at[source],
            device_id={"tensor": lax.rem(rank + 1, ranks)},
            device_id_type=MESH,
        )

    def dp_move(shift):
        return pltpu.make_async_remote_copy(
            src_ref=dp_out,
            dst_ref=dp_in.at[me],
            send_sem=dp_send.at[shift],
            recv_sem=dp_recv.at[me],
            device_id={"dp": lax.rem(me + shift, devices)},
            device_id_type=MESH,
        )

    def dp_arrival(source):
        return pltpu.make_async_remote_copy(
            src_ref=dp_out,
            dst_ref=dp_in.at[source],
            send_sem=dp_send.at[0],
            recv_sem=dp_recv.at[source],
            device_id={"dp": lax.rem(me + 1, devices)},
            device_id_type=MESH,
        )

    for shift in range(1, ranks):
        rank_move(shift).start()
    rank_in[rank] = own_ref[...]
    for shift in range(1, ranks):
        rank_arrival(lax.rem(rank + shift, ranks)).wait_recv()
    part = rank_in[0]
    for spot in range(1, ranks):
        part = part + rank_in[spot]
    dp_out[...] = part
    for shift in range(1, devices):
        dp_move(shift).start()
    dp_in[me] = part
    for shift in range(1, devices):
        dp_arrival(lax.rem(me + shift, devices)).wait_recv()
    whole = dp_in[0]
    for spot in range(1, devices):
        whole = whole + dp_in[spot]
    sum_ref[...] = whole
    for shift in range(1, ranks):
        rank_move(shift).wait_send()
    for shift in range(1, devices):
        dp_move(shift).wait_send()


def total_of(own, collective_id):
    devices, ranks = lax.axis_size("dp"), lax.axis_size("tensor")
    return pl.pallas_call(
        functools.partial(total_kernel, devices, ranks),
        out_shape=jax.ShapeDtypeStruct(own.shape, own.dtype),
        in_specs=[pl.BlockSpec(memory_space=pltpu.VMEM)],
        out_specs=pl.BlockSpec(memory_space=pltpu.VMEM),
        scratch_shapes=[
            pltpu.VMEM((ranks,) + own.shape, own.dtype),
            pltpu.VMEM(own.shape, own.dtype),
            pltpu.VMEM((devices,) + own.shape, own.dtype),
            pltpu.SemaphoreType.DMA((ranks,)),
            pltpu.SemaphoreType.DMA((ranks,)),
            pltpu.SemaphoreType.DMA((devices,)),
            pltpu.SemaphoreType.DMA((devices,)),
        ],
        compiler_params=pltpu.CompilerParams(
            collective_id=collective_id, has_side_effects=True
        ),
        cost_estimate=pl.CostEstimate(flops=0, bytes_accessed=20_000_000, transcendentals=0),
        name="total_" + str(collective_id),
    )(own)


WINDOW = 224


def image_kernel(
    images, cuts, x_hbm, c_hbm, tail_ref, w_ref,
    out_ref, grad_in_ref, g_ref,
    acc1, acc2, gain_row, g_gain, windows, kept, qkv, back_cols, front_cols,
    partial, pair_in, chip_sum, line_in, total,
    in_sem, s1, r1, s2, r2, s3, r3,
):
    step = pl.program_id(0)
    rank = lax.axis_index("tensor")
    core = rank % 2
    sibling = {"tensor": rank + 1 - 2 * core}
    across = {"tensor": lax.rem(rank + 2, 4)}
    width, head_cols = cuts
    heads = head_cols // HEAD_DIM
    rows, model = kept.shape[2], kept.shape[3]
    half = model // 2
    f32, b16 = jnp.float32, jnp.bfloat16
    back_width, front_width = back_cols.shape[1], front_cols.shape[1]
    last_window = images * SEQ // 16 * 16 - WINDOW

    def window_start(image):
        return pl.multiple_of(jnp.minimum(image * SEQ // 16 * 16, last_window), 16)

    def fetches(image, slot):
        return [
            pltpu.make_async_copy(
                source.at[pl.ds(window_start(image), WINDOW)],
                windows.at[slot, kind, pl.ds(0, WINDOW)],
                in_sem.at[slot, kind],
            )
            for kind, source in ((0, x_hbm), (1, c_hbm))
        ]

    def one_hot(shape, row_is):
        at = [lax.broadcasted_iota(jnp.int32, shape, axis) for axis in (0, 1)]
        return jnp.where(row_is(*at), 1.0, 0.0).astype(b16)

    @pl.when(step == 0)
    def _():
        barrier = pltpu.get_barrier_semaphore()
        pl.semaphore_signal(barrier, inc=1, device_id=sibling, device_id_type=MESH)
        pl.semaphore_signal(barrier, inc=1, device_id=across, device_id_type=MESH)
        pl.semaphore_wait(barrier, 2)
        for copy in fetches(0, 0):
            copy.start()
        for slot in range(2):
            for kind in range(2):
                windows[slot, kind, WINDOW:] = tail_ref[kind]
        acc1[...] = jnp.zeros_like(acc1)
        acc2[...] = jnp.zeros_like(acc2)
        back_cols[...] = jnp.zeros_like(back_cols)
        front_cols[...] = jnp.zeros_like(front_cols)
        g_gain[...] = jnp.zeros_like(g_gain)
        for ref in (out_ref, grad_in_ref):
            ref[:16] = jnp.zeros((16, model), b16)
        turned = w_ref[:, back_width + front_width - 128 :].astype(f32).T
        gain_row[...] = turned[127:128]

    @pl.when(step < images - 1)
    def _():
        for copy in fetches(step + 1, (step + 1) % 2):
            copy.start()

    def move(source, target, sends, recvs, slot, peer):
        return pltpu.make_async_remote_copy(
            src_ref=source,
            dst_ref=target,
            send_sem=sends.at[slot],
            recv_sem=recvs.at[slot],
            device_id=peer,
            device_id_type=MESH,
        )

    def first(slot):
        return move(partial.at[slot, 1 - core], pair_in.at[slot], s1, r1, slot, sibling)

    def second(slot):
        return move(chip_sum.at[slot], line_in.at[slot], s2, r2, slot, across)

    def third(slot):
        return move(total.at[slot, core], total.at[slot, core], s3, r3, slot, sibling)

    def normalised(values):
        floats = values.astype(f32)
        centred = floats - jnp.mean(floats, axis=1, keepdims=True)
        inv_std = lax.rsqrt(jnp.mean(centred * centred, axis=1, keepdims=True) + norm_eps)
        return floats, centred * inv_std, inv_std

    gain = gain_row[...]

    def place(ref, image, values):
        @pl.when(image < images - 1)
        def _():
            start = pl.multiple_of(image * SEQ // 16 * 16, 16)
            offset = image * SEQ - start
            spread = one_hot(
                (WINDOW, rows), lambda r, j: jnp.logical_and(r == j + offset, j < SEQ)
            )
            placed = jnp.dot(spread, values, preferred_element_type=f32)
            before = lax.broadcasted_iota(jnp.int32, (16, model), 0) < offset
            head = jnp.where(before, ref[pl.ds(start, 16), :].astype(f32), placed[:16])
            ref[pl.ds(start, 16), :] = head.astype(b16)
            ref[pl.ds(start + 16, WINDOW - 16), :] = placed[16:].astype(b16)

        @pl.when(image == images - 1)
        def _():
            ref[(images - 1) * SEQ :] = values[:SEQ]

    @pl.when(step >= 3)
    def _():
        slot = (step - 3) % 2
        third(slot).wait()
        floats, unit, inv_std = normalised(kept[(step - 3) % 4, 0])
        sums = jnp.concatenate([total[slot, 0, 0], total[slot, 1, 0]], axis=1).astype(f32)
        place(out_ref, step - 3, (floats + sums).astype(b16))
        d_normed = jnp.concatenate([total[slot, 0, 1], total[slot, 1, 1]], axis=1).astype(f32)
        weighted = d_normed * unit
        g_gain[...] += jnp.sum(weighted, axis=0, keepdims=True)
        d_unit = d_normed * gain
        d_floats = inv_std * (
            d_unit
            - jnp.mean(d_unit, axis=1, keepdims=True)
            - unit * jnp.mean(weighted * gain, axis=1, keepdims=True)
        )
        floats_back = kept[(step - 3) % 4, 1].astype(f32) + d_floats
        place(grad_in_ref, step - 3, floats_back.astype(b16))

    @pl.when(jnp.logical_and(step >= 2, step < images + 2))
    def _():
        slot = (step - 2) % 2
        second(slot).wait()
        total[slot, core] = (chip_sum[slot].astype(f32) + line_in[slot].astype(f32)).astype(b16)
        third(slot).start()

    @pl.when(jnp.logical_and(step >= 1, step < images + 1))
    def _():
        slot = (step - 1) % 2
        first(slot).wait()
        chip_sum[slot] = (partial[slot, core].astype(f32) + pair_in[slot].astype(f32)).astype(b16)
        second(slot).start()

    @pl.when(step < images)
    def _():
        slot = step % 2
        for copy in fetches(step, slot):
            copy.wait()
        offset = step * SEQ - window_start(step)
        pick = one_hot(
            (rows, windows.shape[2]), lambda r, j: jnp.logical_and(j == r + offset, r < SEQ)
        )
        for kind in range(2):
            kept[step % 4, kind] = jnp.dot(
                pick, windows[slot, kind], preferred_element_type=f32
            ).astype(b16)
        _floats, unit, _inv = normalised(kept[step % 4, 0])
        normed = (unit * gain).astype(b16)
        cot = kept[step % 4, 1]

        def mm(a, b):
            return jnp.dot(a, b, preferred_element_type=f32)

        def mm_nt(a, b):
            return lax.dot_general(a, b, (((1,), (1,)), ((), ())), preferred_element_type=f32)

        def mm_tn(a, b):
            return lax.dot_general(a, b, (((0,), (0,)), ((), ())), preferred_element_type=f32)

        qkv[:, : 3 * head_cols] = mm(normed, w_ref[:, width:back_width])[:, : 3 * head_cols].astype(b16)
        qkv[:, 3 * head_cols :] = mm(cot, w_ref[:, back_width + width :])[:, :head_cols].astype(b16)
        keys_wide = pl.cdiv(rows, 128) * 128
        filler = jnp.zeros((keys_wide - rows, HEAD_DIM), b16)
        real = lax.broadcasted_iota(jnp.int32, (rows, keys_wide), 1) < SEQ
        for head in range(heads):
            def part(kind):
                at = kind * head_cols + head * HEAD_DIM
                return qkv[:, at : at + HEAD_DIM]

            query = part(0) * jnp.asarray(HEAD_DIM ** (-0.5), b16)
            key = jnp.concatenate([part(1), filler], axis=0)
            value = jnp.concatenate([part(2), filler], axis=0)
            d_att = part(3)
            scores = jnp.where(real, mm_nt(query, key), -1e30)
            powers = jnp.exp(scores - jnp.max(scores, axis=1, keepdims=True))
            probs = powers * (1.0 / jnp.sum(powers, axis=1, keepdims=True))
            probs_low = probs.astype(b16)
            spot = head * HEAD_DIM
            front_cols[:, width + spot : width + spot + HEAD_DIM] = mm(probs_low, value).astype(b16)
            d_probs = mm_nt(d_att, value)
            d_value = mm_tn(probs_low, d_att)[:rows].astype(b16)
            inner = jnp.sum(probs * d_probs, axis=1, keepdims=True)
            d_scores = (probs * (d_probs - inner)).astype(b16)
            d_query = (mm(d_scores, key) * (HEAD_DIM ** (-0.5))).astype(b16)
            d_key = mm_tn(d_scores, query)[:rows].astype(b16)
            for kind, value_of in ((0, d_query), (1, d_key), (2, d_value)):
                at = width + kind * head_cols + spot
                back_cols[:, at : at + HEAD_DIM] = value_of

        upper = mm(normed, w_ref[:, :width])
        d_hidden = mm(cot, w_ref[:, back_width : back_width + width])
        scale = (2.0 / 3.141592653589793) ** 0.5
        square = upper * upper
        bend = jnp.tanh(scale * upper * (1.0 + 0.044715 * square))
        step_up = 0.5 * (1.0 + bend)
        front_cols[:, :width] = (upper * step_up).astype(b16)
        slope = step_up + (0.5 * scale) * upper * (1.0 - bend * bend) * (
            1.0 + (3.0 * 0.044715) * square
        )
        back_cols[:, :width] = (d_hidden * slope).astype(b16)

        out_part = mm_nt(front_cols[...], w_ref[:, back_width:]).astype(b16)
        partial[slot, 0, 0] = out_part[:, :half]
        partial[slot, 1, 0] = out_part[:, half:]
        back_part = mm_nt(back_cols[...], w_ref[:, :back_width]).astype(b16)
        partial[slot, 0, 1] = back_part[:, :half]
        partial[slot, 1, 1] = back_part[:, half:]
        first(slot).start()
        acc1[...] += mm_tn(normed, back_cols[...])
        acc2[...] += mm_tn(cot, front_cols[...])

    @pl.when(step == images + 2)
    def _():
        g_ref[:, :back_width] = acc1[...].astype(b16)
        inner = back_width + front_width - 128
        g_ref[:, back_width:inner] = acc2[:, : front_width - 128].astype(b16)
        spare = jnp.broadcast_to(g_gain[...], (128, model)).T
        last = lax.broadcasted_iota(jnp.int32, (model, 128), 1) == 127
        g_ref[:, inner:] = jnp.where(last, spare, acc2[:, front_width - 128 :]).astype(b16)


def image_block(inputs, cotangent, tails, weights, width, head_cols, back_width):
    tokens, model = inputs.shape
    images = tokens // SEQ
    rows = -(-SEQ // 16) * 16
    half = model // 2
    front_width = weights.shape[1] - back_width
    fixed = lambda i: (0, 0)

    def whole(shape):
        return pl.BlockSpec(shape, fixed, pipeline_mode=pl.Buffered(1))

    bf = jnp.bfloat16
    anywhere = pl.BlockSpec(memory_space=pl.ANY)
    return pl.pallas_call(
        functools.partial(image_kernel, images, (width, head_cols)),
        grid=(images + 3,),
        out_shape=(
            jax.ShapeDtypeStruct(inputs.shape, bf),
            jax.ShapeDtypeStruct(inputs.shape, bf),
            jax.ShapeDtypeStruct(weights.shape, bf),
        ),
        in_specs=[
            anywhere,
            anywhere,
            pl.BlockSpec(tails.shape, lambda i: (0, 0, 0), pipeline_mode=pl.Buffered(1)),
            whole(weights.shape),
        ],
        out_specs=[whole(inputs.shape), whole(inputs.shape), whole(weights.shape)],
        scratch_shapes=[
            pltpu.VMEM((model, back_width), jnp.float32),
            pltpu.VMEM((model, front_width), jnp.float32),
            pltpu.VMEM((1, model), jnp.float32),
            pltpu.VMEM((1, model), jnp.float32),
            pltpu.VMEM((2, 2, WINDOW + tails.shape[1], model), bf),
            pltpu.VMEM((4, 2, rows, model), bf),
            pltpu.VMEM((rows, 4 * head_cols), bf),
            pltpu.VMEM((rows, back_width), bf),
            pltpu.VMEM((rows, front_width), bf),
            pltpu.VMEM((2, 2, 2, rows, half), bf),
            pltpu.VMEM((2, 2, rows, half), bf),
            pltpu.VMEM((2, 2, rows, half), bf),
            pltpu.VMEM((2, 2, rows, half), bf),
            pltpu.VMEM((2, 2, 2, rows, half), bf),
            pltpu.SemaphoreType.DMA((2, 2)),
        ]
        + [pltpu.SemaphoreType.DMA((2,))] * 6,
        compiler_params=pltpu.CompilerParams(
            collective_id=4,
            has_side_effects=True,
            vmem_limit_bytes=60 * 2**20,
            dimension_semantics=("arbitrary",),
        ),
        name="image_block",
    )(inputs, cotangent, tails, weights)


def local(
    inputs,
    cotangent,
    master_inward,
    first_inward,
    second_inward,
    master_outward,
    first_outward,
    second_outward,
    master_widening,
    first_widening,
    second_widening,
    master_narrowing,
    first_narrowing,
    second_narrowing,
    master_scaling,
    first_scaling,
    second_scaling,
):
    depth = master_widening.shape[0]
    hidden_here = master_widening.shape[1]
    head_cols = master_inward.shape[2]
    model = inputs.shape[1]
    back_width = hidden_here + 3 * head_cols
    gap = (-back_width) % 128
    back_width += gap
    used = back_width + hidden_here + head_cols
    width = -(-(used + 1) // 128) * 128
    shard = jnp.concatenate(
        [
            master_widening,
            jnp.transpose(master_inward, (1, 0, 2)).reshape(depth, 3 * head_cols),
            jnp.zeros((depth, gap), jnp.float32),
            master_narrowing.T,
            master_outward.T,
            jnp.broadcast_to(master_scaling[:, None], (depth, width - used)),
        ],
        axis=1,
    ).astype(jnp.bfloat16)
    copies = gather_blocks(shard).reshape(model, width)
    rows_here = inputs.shape[0]
    whole_rows = rows_here // 16 * 16
    tails = jnp.stack(
        [
            jnp.pad(rows[whole_rows:], ((0, whole_rows + 16 - rows_here), (0, 0)))
            for rows in (inputs, cotangent)
        ]
    )
    summed_out, input_grad, grads = image_block(
        inputs, cotangent, tails, copies, hidden_here, head_cols, back_width
    )
    share = rows_here // lax.axis_size("tensor")
    start = lax.axis_index("tensor") * share
    output = lax.dynamic_slice_in_dim(summed_out, start, share, 0)
    summed = reduce_blocks(grads.reshape(lax.axis_size("dp"), depth, width))
    grad_widening = summed[:, :hidden_here]
    grad_inward = jnp.transpose(
        summed[:, hidden_here : back_width - gap].reshape(depth, 3, head_cols), (1, 0, 2)
    )
    grad_narrowing = summed[:, back_width : back_width + hidden_here].T
    grad_outward = summed[:, back_width + hidden_here : used].T
    grad_scaling = summed[:, width - 1]
    part_in = lamb_parts(master_inward, first_inward, second_inward, grad_inward)
    part_out = lamb_parts(master_outward, first_outward, second_outward, grad_outward)
    part_wide = lamb_parts(master_widening, first_widening, second_widening, grad_widening)
    part_narrow = lamb_parts(master_narrowing, first_narrowing, second_narrowing, grad_narrowing)
    part_scale = lamb_parts(master_scaling, first_scaling, second_scaling, grad_scaling)
    replicas = 1.0 / lax.axis_size("tensor")
    local_sums = jnp.stack(
        [
            jnp.stack([jnp.sum(master_inward * master_inward), jnp.sum(part_in[2] * part_in[2])]),
            jnp.stack(
                [jnp.sum(master_outward * master_outward), jnp.sum(part_out[2] * part_out[2])]
            ),
            jnp.stack(
                [jnp.sum(master_widening * master_widening), jnp.sum(part_wide[2] * part_wide[2])]
            ),
            jnp.stack(
                [
                    jnp.sum(master_narrowing * master_narrowing),
                    jnp.sum(part_narrow[2] * part_narrow[2]),
                ]
            ),
            jnp.stack(
                [jnp.sum(master_scaling * master_scaling), jnp.sum(part_scale[2] * part_scale[2])]
            )
            * replicas,
        ]
    )
    packed = jnp.zeros((8, 128), jnp.float32).at[:5, :2].set(local_sums)
    trust_norms = jnp.sqrt(total_of(packed, 3)[:5, :2])
    fresh_in = master_inward - learn_rate * (trust_norms[0, 0] / trust_norms[0, 1]) * part_in[2]
    fresh_out = master_outward - learn_rate * (trust_norms[1, 0] / trust_norms[1, 1]) * part_out[2]
    fresh_wide = (
        master_widening - learn_rate * (trust_norms[2, 0] / trust_norms[2, 1]) * part_wide[2]
    )
    fresh_narrow = (
        master_narrowing - learn_rate * (trust_norms[3, 0] / trust_norms[3, 1]) * part_narrow[2]
    )
    fresh_scale = (
        master_scaling - learn_rate * (trust_norms[4, 0] / trust_norms[4, 1]) * part_scale[2]
    )
    return (
        output,
        input_grad,
        part_in[0],
        part_in[1],
        fresh_in,
        fresh_in.astype(jnp.bfloat16),
        part_out[0],
        part_out[1],
        fresh_out,
        fresh_out.astype(jnp.bfloat16),
        part_wide[0],
        part_wide[1],
        fresh_wide,
        fresh_wide.astype(jnp.bfloat16),
        part_narrow[0],
        part_narrow[1],
        fresh_narrow,
        fresh_narrow.astype(jnp.bfloat16),
        part_scale[0],
        part_scale[1],
        fresh_scale,
        fresh_scale.astype(jnp.bfloat16),
        trust_norms,
    )


def solution(mesh):
    in_specs = (
        P("dp", None),
        P("dp", None),
        P(None, "dp", "tensor"),
        P(None, "dp", "tensor"),
        P(None, "dp", "tensor"),
        P("tensor", "dp"),
        P("tensor", "dp"),
        P("tensor", "dp"),
        P("dp", "tensor"),
        P("dp", "tensor"),
        P("dp", "tensor"),
        P("tensor", "dp"),
        P("tensor", "dp"),
        P("tensor", "dp"),
        P("dp"),
        P("dp"),
        P("dp"),
    )
    out_specs = (
        P(("dp", "tensor"), None),
        P("dp", None),
        P(None, "dp", "tensor"),
        P(None, "dp", "tensor"),
        P(None, "dp", "tensor"),
        P(None, "dp", "tensor"),
        P("tensor", "dp"),
        P("tensor", "dp"),
        P("tensor", "dp"),
        P("tensor", "dp"),
        P("dp", "tensor"),
        P("dp", "tensor"),
        P("dp", "tensor"),
        P("dp", "tensor"),
        P("tensor", "dp"),
        P("tensor", "dp"),
        P("tensor", "dp"),
        P("tensor", "dp"),
        P("dp"),
        P("dp"),
        P("dp"),
        P("dp"),
        P(),
    )
    return jax.shard_map(local, mesh=mesh, in_specs=in_specs, out_specs=out_specs, check_vma=False)
```

```python
import functools

import jax
import jax.numpy as jnp
from jax import lax
from jax.experimental import pallas as pl
from jax.experimental.pallas import tpu as pltpu
from jax.sharding import PartitionSpec as P

MESH = pl.DeviceIdType.MESH
PAIR = 2

HEAD_DIM = 64
SEQ = 196
STEP = 5


norm_eps = 1e-06
beta_one = 0.5
beta_two = 0.5
lamb_eps = 1e-06
weight_decay = 0.01
learn_rate = 0.5


def lamb_parts(master, first, second, grad):
    moment = beta_one * first + (1.0 - beta_one) * grad
    square = beta_two * second + (1.0 - beta_two) * grad * grad
    update = (
        moment / (1.0 - beta_one**STEP) / (jnp.sqrt(square / (1.0 - beta_two**STEP)) + lamb_eps)
        + weight_decay * master
    )
    return (moment, square, update)


def greet(place, line, up, down, other):
    barrier = pltpu.get_barrier_semaphore()
    pl.semaphore_signal(barrier, inc=1, device_id=other, device_id_type=MESH)

    @pl.when(place < line - 1)
    def _():
        pl.semaphore_signal(barrier, inc=1, device_id=up, device_id_type=MESH)

    @pl.when(place > 0)
    def _():
        pl.semaphore_signal(barrier, inc=1, device_id=down, device_id_type=MESH)

    pl.semaphore_wait(barrier, 1 + jnp.minimum(place, 1) + jnp.minimum(line - 1 - place, 1))


def gather_kernel(line, own_ref, all_ref, own_sem, up_sem, down_sem, pair_sem, recv_sem):
    me = lax.axis_index("dp")
    place, side = me // PAIR, me % PAIR
    up, down, other = {"dp": me + PAIR}, {"dp": me - PAIR}, {"dp": me + 1 - 2 * side}
    has_up, has_down = place < line - 1, place > 0
    greet(place, line, up, down, other)

    def move(step, source, block, sems, peer):
        return pltpu.make_async_remote_copy(
            src_ref=source,
            dst_ref=all_ref.at[block],
            send_sem=sems.at[step],
            recv_sem=recv_sem.at[block],
            device_id=peer,
            device_id_type=MESH,
        )

    def held(block):
        return all_ref.at[block]

    def arrived(block, peer):
        move(0, held(block), block, pair_sem, peer).wait_recv()

    own = pltpu.make_async_copy(own_ref, all_ref.at[me], own_sem)

    @pl.when(has_up)
    def _():
        move(place, own_ref, me, up_sem, up).start()

    @pl.when(has_down)
    def _():
        move(place, own_ref, me, down_sem, down).start()

    move(place, own_ref, me, pair_sem, other).start()
    own.start()

    @pl.loop(1, line)
    def _(step):
        low, high = place - step, place + step

        @pl.when(low >= 0)
        def _():
            block = low * PAIR + side
            arrived(block, other)

            @pl.when(has_up)
            def _():
                move(low, held(block), block, up_sem, up).start()

            move(low, held(block), block, pair_sem, other).start()

        @pl.when(high < line)
        def _():
            block = high * PAIR + side
            arrived(block, other)

            @pl.when(has_down)
            def _():
                move(high, held(block), block, down_sem, down).start()

            move(high, held(block), block, pair_sem, other).start()

    own.wait()

    @pl.loop(0, line)
    def _(spot):
        block = spot * PAIR + side
        arrived(spot * PAIR + 1 - side, other)
        move(spot, held(block), block, pair_sem, other).wait_send()

        @pl.when(jnp.logical_and(has_up, spot <= place))
        def _():
            move(spot, held(block), block, up_sem, up).wait_send()

        @pl.when(jnp.logical_and(has_down, spot >= place))
        def _():
            move(spot, held(block), block, down_sem, down).wait_send()


def gather_blocks(own):
    rows, width = own.shape
    devices = lax.axis_size("dp")
    line = devices // PAIR
    return pl.pallas_call(
        functools.partial(gather_kernel, line),
        out_shape=jax.ShapeDtypeStruct((devices, rows, width), own.dtype),
        in_specs=[pl.BlockSpec(memory_space=pltpu.VMEM)],
        out_specs=pl.BlockSpec(memory_space=pl.ANY),
        scratch_shapes=[
            pltpu.SemaphoreType.DMA,
            pltpu.SemaphoreType.DMA((line,)),
            pltpu.SemaphoreType.DMA((line,)),
            pltpu.SemaphoreType.DMA((line,)),
            pltpu.SemaphoreType.DMA((devices,)),
        ],
        compiler_params=pltpu.CompilerParams(collective_id=0, has_side_effects=True),
        cost_estimate=pl.CostEstimate(flops=0, bytes_accessed=100_000_000, transcendentals=0),
        name="gather_blocks",
    )(own)


def reduce_kernel(
    line, own_ref, sum_ref, pair_in, up_in, down_in, up_out, down_out,
    pair_send, pair_recv, up_send, up_recv, down_send, down_recv,
):
    me = lax.axis_index("dp")
    place, side = me // PAIR, me % PAIR
    up, down, other = {"dp": me + PAIR}, {"dp": me - PAIR}, {"dp": me + 1 - 2 * side}
    has_up, has_down = place < line - 1, place > 0
    greet(place, line, up, down, other)

    def pair_move(spot):
        return pltpu.make_async_remote_copy(
            src_ref=own_ref.at[spot * PAIR + 1 - side],
            dst_ref=pair_in.at[spot],
            send_sem=pair_send.at[spot],
            recv_sem=pair_recv.at[spot],
            device_id=other,
            device_id_type=MESH,
        )

    def line_move(spot, source, target, sends, recvs, peer):
        return pltpu.make_async_remote_copy(
            src_ref=source.at[spot],
            dst_ref=target.at[spot],
            send_sem=sends.at[spot],
            recv_sem=recvs.at[spot],
            device_id=peer,
            device_id_type=MESH,
        )

    def up_move(spot):
        return line_move(spot, up_out, up_in, up_send, up_recv, up)

    def down_move(spot):
        return line_move(spot, down_out, down_in, down_send, down_recv, down)

    @pl.loop(0, line)
    def _(turn):
        far = line - 1 - turn

        @pl.when(place + far < line)
        def _():
            pair_move(place + far).start()

        @pl.when(jnp.logical_and(place - far >= 0, far > 0))
        def _():
            pair_move(place - far).start()

    def both(spot):
        return own_ref[spot * PAIR + side].astype(jnp.float32) + pair_in[spot].astype(jnp.float32)

    @pl.loop(0, line - 1)
    def _(turn):
        far = line - 1 - turn

        @pl.when(place + far < line)
        def _():
            spot = place + far
            pair_move(spot).wait_recv()

            @pl.when(has_down)
            def _():
                up_move(spot).wait_recv()
                up_out[spot] = (both(spot) + up_in[spot].astype(jnp.float32)).astype(jnp.bfloat16)

            @pl.when(jnp.logical_not(has_down))
            def _():
                up_out[spot] = both(spot).astype(jnp.bfloat16)

            up_move(spot).start()

        @pl.when(place - far >= 0)
        def _():
            spot = place - far
            pair_move(spot).wait_recv()

            @pl.when(has_up)
            def _():
                down_move(spot).wait_recv()
                down_out[spot] = (both(spot) + down_in[spot].astype(jnp.float32)).astype(
                    jnp.bfloat16
                )

            @pl.when(jnp.logical_not(has_up))
            def _():
                down_out[spot] = both(spot).astype(jnp.bfloat16)

            down_move(spot).start()

    pair_move(place).wait_recv()
    sum_ref[...] = both(place)

    @pl.when(has_down)
    def _():
        up_move(place).wait_recv()
        sum_ref[...] += up_in[place].astype(jnp.float32)

    @pl.when(has_up)
    def _():
        down_move(place).wait_recv()
        sum_ref[...] += down_in[place].astype(jnp.float32)

    @pl.loop(0, line)
    def _(spot):
        pair_move(spot).wait_send()

        @pl.when(spot > place)
        def _():
            up_move(spot).wait_send()

        @pl.when(spot < place)
        def _():
            down_move(spot).wait_send()


def reduce_blocks(own):
    devices, rows, width = own.shape
    line = devices // PAIR
    buffer = pltpu.VMEM((line, rows, width), own.dtype)
    return pl.pallas_call(
        functools.partial(reduce_kernel, line),
        out_shape=jax.ShapeDtypeStruct((rows, width), jnp.float32),
        in_specs=[pl.BlockSpec(memory_space=pltpu.VMEM)],
        out_specs=pl.BlockSpec(memory_space=pltpu.VMEM),
        scratch_shapes=[buffer] * 5 + [pltpu.SemaphoreType.DMA((line,))] * 6,
        compiler_params=pltpu.CompilerParams(
            collective_id=1, has_side_effects=True, vmem_limit_bytes=40 * 2**20
        ),
        cost_estimate=pl.CostEstimate(flops=0, bytes_accessed=100_000_000, transcendentals=0),
        name="reduce_blocks",
    )(own)


def total_kernel(
    devices, ranks, own_ref, sum_ref, rank_in, dp_out, dp_in,
    rank_send, rank_recv, dp_send, dp_recv,
):
    me, rank = lax.axis_index("dp"), lax.axis_index("tensor")
    barrier = pltpu.get_barrier_semaphore()
    for shift in range(1, ranks):
        peer = {"tensor": lax.rem(rank + shift, ranks)}
        pl.semaphore_signal(barrier, inc=1, device_id=peer, device_id_type=MESH)
    for shift in range(1, devices):
        peer = {"dp": lax.rem(me + shift, devices)}
        pl.semaphore_signal(barrier, inc=1, device_id=peer, device_id_type=MESH)
    pl.semaphore_wait(barrier, ranks - 1 + devices - 1)

    def rank_move(shift):
        return pltpu.make_async_remote_copy(
            src_ref=own_ref,
            dst_ref=rank_in.at[rank],
            send_sem=rank_send.at[shift],
            recv_sem=rank_recv.at[rank],
            device_id={"tensor": lax.rem(rank + shift, ranks)},
            device_id_type=MESH,
        )

    def rank_arrival(source):
        return pltpu.make_async_remote_copy(
            src_ref=own_ref,
            dst_ref=rank_in.at[source],
            send_sem=rank_send.at[0],
            recv_sem=rank_recv.at[source],
            device_id={"tensor": lax.rem(rank + 1, ranks)},
            device_id_type=MESH,
        )

    def dp_move(shift):
        return pltpu.make_async_remote_copy(
            src_ref=dp_out,
            dst_ref=dp_in.at[me],
            send_sem=dp_send.at[shift],
            recv_sem=dp_recv.at[me],
            device_id={"dp": lax.rem(me + shift, devices)},
            device_id_type=MESH,
        )

    def dp_arrival(source):
        return pltpu.make_async_remote_copy(
            src_ref=dp_out,
            dst_ref=dp_in.at[source],
            send_sem=dp_send.at[0],
            recv_sem=dp_recv.at[source],
            device_id={"dp": lax.rem(me + 1, devices)},
            device_id_type=MESH,
        )

    for shift in range(1, ranks):
        rank_move(shift).start()
    rank_in[rank] = own_ref[...]
    for shift in range(1, ranks):
        rank_arrival(lax.rem(rank + shift, ranks)).wait_recv()
    part = rank_in[0]
    for spot in range(1, ranks):
        part = part + rank_in[spot]
    dp_out[...] = part
    for shift in range(1, devices):
        dp_move(shift).start()
    dp_in[me] = part
    for shift in range(1, devices):
        dp_arrival(lax.rem(me + shift, devices)).wait_recv()
    whole = dp_in[0]
    for spot in range(1, devices):
        whole = whole + dp_in[spot]
    sum_ref[...] = whole
    for shift in range(1, ranks):
        rank_move(shift).wait_send()
    for shift in range(1, devices):
        dp_move(shift).wait_send()


def total_of(own, collective_id):
    devices, ranks = lax.axis_size("dp"), lax.axis_size("tensor")
    return pl.pallas_call(
        functools.partial(total_kernel, devices, ranks),
        out_shape=jax.ShapeDtypeStruct(own.shape, own.dtype),
        in_specs=[pl.BlockSpec(memory_space=pltpu.VMEM)],
        out_specs=pl.BlockSpec(memory_space=pltpu.VMEM),
        scratch_shapes=[
            pltpu.VMEM((ranks,) + own.shape, own.dtype),
            pltpu.VMEM(own.shape, own.dtype),
            pltpu.VMEM((devices,) + own.shape, own.dtype),
            pltpu.SemaphoreType.DMA((ranks,)),
            pltpu.SemaphoreType.DMA((ranks,)),
            pltpu.SemaphoreType.DMA((devices,)),
            pltpu.SemaphoreType.DMA((devices,)),
        ],
        compiler_params=pltpu.CompilerParams(
            collective_id=collective_id, has_side_effects=True
        ),
        cost_estimate=pl.CostEstimate(flops=0, bytes_accessed=20_000_000, transcendentals=0),
        name="total_" + str(collective_id),
    )(own)


WINDOW = 224


def image_kernel(
    images, cuts, x_hbm, c_hbm, tail_ref, w_ref,
    out_ref, grad_in_ref, g_ref,
    acc1, acc2, gain_row, g_gain, windows, kept, qkv, back_cols, front_cols,
    partial, pair_in, chip_sum, line_in, total,
    in_sem, s1, r1, s2, r2, s3, r3,
):
    step = pl.program_id(0)
    rank = lax.axis_index("tensor")
    core = rank % 2
    sibling = {"tensor": rank + 1 - 2 * core}
    across = {"tensor": lax.rem(rank + 2, 4)}
    width, head_cols = cuts
    heads = head_cols // HEAD_DIM
    rows, model = kept.shape[2], kept.shape[3]
    half = model // 2
    f32, b16 = jnp.float32, jnp.bfloat16
    back_width, front_width = back_cols.shape[1], front_cols.shape[1]
    last_window = images * SEQ // 16 * 16 - WINDOW

    def window_start(image):
        return pl.multiple_of(jnp.minimum(image * SEQ // 16 * 16, last_window), 16)

    def fetches(image, slot):
        return [
            pltpu.make_async_copy(
                source.at[pl.ds(window_start(image), WINDOW)],
                windows.at[slot, kind, pl.ds(0, WINDOW)],
                in_sem.at[slot, kind],
            )
            for kind, source in ((0, x_hbm), (1, c_hbm))
        ]

    def one_hot(shape, row_is):
        at = [lax.broadcasted_iota(jnp.int32, shape, axis) for axis in (0, 1)]
        return jnp.where(row_is(*at), 1.0, 0.0).astype(b16)

    @pl.when(step == 0)
    def _():
        barrier = pltpu.get_barrier_semaphore()
        pl.semaphore_signal(barrier, inc=1, device_id=sibling, device_id_type=MESH)
        pl.semaphore_signal(barrier, inc=1, device_id=across, device_id_type=MESH)
        pl.semaphore_wait(barrier, 2)
        for copy in fetches(0, 0):
            copy.start()
        for slot in range(2):
            for kind in range(2):
                windows[slot, kind, WINDOW:] = tail_ref[kind]
        acc1[...] = jnp.zeros_like(acc1)
        acc2[...] = jnp.zeros_like(acc2)
        back_cols[...] = jnp.zeros_like(back_cols)
        front_cols[...] = jnp.zeros_like(front_cols)
        g_gain[...] = jnp.zeros_like(g_gain)
        for ref in (out_ref, grad_in_ref):
            ref[:16] = jnp.zeros((16, model), b16)
        turned = w_ref[:, back_width + front_width - 128 :].astype(f32).T
        gain_row[...] = turned[127:128]

    @pl.when(step < images - 1)
    def _():
        for copy in fetches(step + 1, (step + 1) % 2):
            copy.start()

    def move(source, target, sends, recvs, slot, peer):
        return pltpu.make_async_remote_copy(
            src_ref=source,
            dst_ref=target,
            send_sem=sends.at[slot],
            recv_sem=recvs.at[slot],
            device_id=peer,
            device_id_type=MESH,
        )

    def first(slot):
        return move(partial.at[slot, 1 - core], pair_in.at[slot], s1, r1, slot, sibling)

    def second(slot):
        return move(chip_sum.at[slot], line_in.at[slot], s2, r2, slot, across)

    def third(slot):
        return move(total.at[slot, core], total.at[slot, core], s3, r3, slot, sibling)

    def normalised(values):
        floats = values.astype(f32)
        centred = floats - jnp.mean(floats, axis=1, keepdims=True)
        inv_std = lax.rsqrt(jnp.mean(centred * centred, axis=1, keepdims=True) + norm_eps)
        return floats, centred * inv_std, inv_std

    gain = gain_row[...]

    def place(ref, image, values):
        @pl.when(image < images - 1)
        def _():
            start = pl.multiple_of(image * SEQ // 16 * 16, 16)
            offset = image * SEQ - start
            spread = one_hot(
                (WINDOW, rows), lambda r, j: jnp.logical_and(r == j + offset, j < SEQ)
            )
            placed = jnp.dot(spread, values, preferred_element_type=f32)
            before = lax.broadcasted_iota(jnp.int32, (16, model), 0) < offset
            head = jnp.where(before, ref[pl.ds(start, 16), :].astype(f32), placed[:16])
            ref[pl.ds(start, 16), :] = head.astype(b16)
            ref[pl.ds(start + 16, WINDOW - 16), :] = placed[16:].astype(b16)

        @pl.when(image == images - 1)
        def _():
            ref[(images - 1) * SEQ :] = values[:SEQ]

    @pl.when(step >= 3)
    def _():
        slot = (step - 3) % 2
        third(slot).wait()
        floats, unit, inv_std = normalised(kept[(step - 3) % 4, 0])
        sums = jnp.concatenate([total[slot, 0, 0], total[slot, 1, 0]], axis=1).astype(f32)
        place(out_ref, step - 3, (floats + sums).astype(b16))
        d_normed = jnp.concatenate([total[slot, 0, 1], total[slot, 1, 1]], axis=1).astype(f32)
        weighted = d_normed * unit
        g_gain[...] += jnp.sum(weighted, axis=0, keepdims=True)
        d_unit = d_normed * gain
        d_floats = inv_std * (
            d_unit
            - jnp.mean(d_unit, axis=1, keepdims=True)
            - unit * jnp.mean(weighted * gain, axis=1, keepdims=True)
        )
        floats_back = kept[(step - 3) % 4, 1].astype(f32) + d_floats
        place(grad_in_ref, step - 3, floats_back.astype(b16))

    @pl.when(jnp.logical_and(step >= 2, step < images + 2))
    def _():
        slot = (step - 2) % 2
        second(slot).wait()
        total[slot, core] = (chip_sum[slot].astype(f32) + line_in[slot].astype(f32)).astype(b16)
        third(slot).start()

    @pl.when(jnp.logical_and(step >= 1, step < images + 1))
    def _():
        slot = (step - 1) % 2
        first(slot).wait()
        chip_sum[slot] = (partial[slot, core].astype(f32) + pair_in[slot].astype(f32)).astype(b16)
        second(slot).start()

    @pl.when(step < images)
    def _():
        slot = step % 2
        for copy in fetches(step, slot):
            copy.wait()
        offset = step * SEQ - window_start(step)
        pick = one_hot(
            (rows, windows.shape[2]), lambda r, j: jnp.logical_and(j == r + offset, r < SEQ)
        )
        for kind in range(2):
            kept[step % 4, kind] = jnp.dot(
                pick, windows[slot, kind], preferred_element_type=f32
            ).astype(b16)
        _floats, unit, _inv = normalised(kept[step % 4, 0])
        normed = (unit * gain).astype(b16)
        cot = kept[step % 4, 1]

        def mm(a, b):
            return jnp.dot(a, b, preferred_element_type=f32)

        def mm_nt(a, b):
            return lax.dot_general(a, b, (((1,), (1,)), ((), ())), preferred_element_type=f32)

        def mm_tn(a, b):
            return lax.dot_general(a, b, (((0,), (0,)), ((), ())), preferred_element_type=f32)

        qkv[:, : 3 * head_cols] = mm(normed, w_ref[:, width:back_width])[:, : 3 * head_cols].astype(b16)
        qkv[:, 3 * head_cols :] = mm(cot, w_ref[:, back_width + width :])[:, :head_cols].astype(b16)
        keys_wide = pl.cdiv(rows, 128) * 128
        filler = jnp.zeros((keys_wide - rows, HEAD_DIM), b16)
        real = lax.broadcasted_iota(jnp.int32, (rows, keys_wide), 1) < SEQ
        for head in range(heads):
            def part(kind):
                at = kind * head_cols + head * HEAD_DIM
                return qkv[:, at : at + HEAD_DIM]

            query = part(0) * jnp.asarray(HEAD_DIM ** (-0.5), b16)
            key = jnp.concatenate([part(1), filler], axis=0)
            value = jnp.concatenate([part(2), filler], axis=0)
            d_att = part(3)
            scores = jnp.where(real, mm_nt(query, key), -1e30)
            powers = jnp.exp(scores - jnp.max(scores, axis=1, keepdims=True))
            probs = powers * (1.0 / jnp.sum(powers, axis=1, keepdims=True))
            probs_low = probs.astype(b16)
            spot = head * HEAD_DIM
            front_cols[:, width + spot : width + spot + HEAD_DIM] = mm(probs_low, value).astype(b16)
            d_probs = mm_nt(d_att, value)
            d_value = mm_tn(probs_low, d_att)[:rows].astype(b16)
            inner = jnp.sum(probs * d_probs, axis=1, keepdims=True)
            d_scores = (probs * (d_probs - inner)).astype(b16)
            d_query = (mm(d_scores, key) * (HEAD_DIM ** (-0.5))).astype(b16)
            d_key = mm_tn(d_scores, query)[:rows].astype(b16)
            for kind, value_of in ((0, d_query), (1, d_key), (2, d_value)):
                at = width + kind * head_cols + spot
                back_cols[:, at : at + HEAD_DIM] = value_of

        upper = mm(normed, w_ref[:, :width])
        d_hidden = mm(cot, w_ref[:, back_width : back_width + width])
        scale = (2.0 / 3.141592653589793) ** 0.5
        square = upper * upper
        bend = jnp.tanh(scale * upper * (1.0 + 0.044715 * square))
        step_up = 0.5 * (1.0 + bend)
        front_cols[:, :width] = (upper * step_up).astype(b16)
        slope = step_up + (0.5 * scale) * upper * (1.0 - bend * bend) * (
            1.0 + (3.0 * 0.044715) * square
        )
        back_cols[:, :width] = (d_hidden * slope).astype(b16)

        out_part = mm_nt(front_cols[...], w_ref[:, back_width:]).astype(b16)
        partial[slot, 0, 0] = out_part[:, :half]
        partial[slot, 1, 0] = out_part[:, half:]
        back_part = mm_nt(back_cols[...], w_ref[:, :back_width]).astype(b16)
        partial[slot, 0, 1] = back_part[:, :half]
        partial[slot, 1, 1] = back_part[:, half:]
        first(slot).start()
        acc1[...] += mm_tn(normed, back_cols[...])
        acc2[...] += mm_tn(cot, front_cols[...])

    @pl.when(step == images + 2)
    def _():
        g_ref[:, :back_width] = acc1[...].astype(b16)
        inner = back_width + front_width - 128
        g_ref[:, back_width:inner] = acc2[:, : front_width - 128].astype(b16)
        spare = jnp.broadcast_to(g_gain[...], (128, model)).T
        last = lax.broadcasted_iota(jnp.int32, (model, 128), 1) == 127
        g_ref[:, inner:] = jnp.where(last, spare, acc2[:, front_width - 128 :]).astype(b16)


def image_block(inputs, cotangent, tails, weights, width, head_cols, back_width):
    tokens, model = inputs.shape
    images = tokens // SEQ
    rows = -(-SEQ // 16) * 16
    half = model // 2
    front_width = weights.shape[1] - back_width
    fixed = lambda i: (0, 0)

    def whole(shape):
        return pl.BlockSpec(shape, fixed, pipeline_mode=pl.Buffered(1))

    bf = jnp.bfloat16
    anywhere = pl.BlockSpec(memory_space=pl.ANY)
    return pl.pallas_call(
        functools.partial(image_kernel, images, (width, head_cols)),
        grid=(images + 3,),
        out_shape=(
            jax.ShapeDtypeStruct(inputs.shape, bf),
            jax.ShapeDtypeStruct(inputs.shape, bf),
            jax.ShapeDtypeStruct(weights.shape, bf),
        ),
        in_specs=[
            anywhere,
            anywhere,
            pl.BlockSpec(tails.shape, lambda i: (0, 0, 0), pipeline_mode=pl.Buffered(1)),
            whole(weights.shape),
        ],
        out_specs=[whole(inputs.shape), whole(inputs.shape), whole(weights.shape)],
        scratch_shapes=[
            pltpu.VMEM((model, back_width), jnp.float32),
            pltpu.VMEM((model, front_width), jnp.float32),
            pltpu.VMEM((1, model), jnp.float32),
            pltpu.VMEM((1, model), jnp.float32),
            pltpu.VMEM((2, 2, WINDOW + tails.shape[1], model), bf),
            pltpu.VMEM((4, 2, rows, model), bf),
            pltpu.VMEM((rows, 4 * head_cols), bf),
            pltpu.VMEM((rows, back_width), bf),
            pltpu.VMEM((rows, front_width), bf),
            pltpu.VMEM((2, 2, 2, rows, half), bf),
            pltpu.VMEM((2, 2, rows, half), bf),
            pltpu.VMEM((2, 2, rows, half), bf),
            pltpu.VMEM((2, 2, rows, half), bf),
            pltpu.VMEM((2, 2, 2, rows, half), bf),
            pltpu.SemaphoreType.DMA((2, 2)),
        ]
        + [pltpu.SemaphoreType.DMA((2,))] * 6,
        compiler_params=pltpu.CompilerParams(
            collective_id=4,
            has_side_effects=True,
            vmem_limit_bytes=60 * 2**20,
            dimension_semantics=("arbitrary",),
        ),
        name="image_block",
    )(inputs, cotangent, tails, weights)


def parts_kernel(cuts, replicas, summed_ref, *refs):
    states, outs, sums_ref = refs[:15], refs[15:30], refs[30]
    hidden_here, head_cols, back_width, used = cuts
    width = summed_ref.shape[1]
    row = lax.broadcasted_iota(jnp.int32, sums_ref.shape, 0)
    lane = lax.broadcasted_iota(jnp.int32, sums_ref.shape, 1)
    sums = jnp.zeros(sums_ref.shape, jnp.float32)

    def square_sum(values):
        return jnp.sum(jnp.sum(values * values, axis=1, keepdims=True), axis=0, keepdims=True)

    def one(index, grad, at=None):
        master, first, second = (
            ref[...] if at is None else ref[at] for ref in states[3 * index : 3 * index + 3]
        )
        results = lamb_parts(master, first, second, grad)
        for ref, value in zip(outs[3 * index : 3 * index + 3], results):
            if at is None:
                ref[...] = value
            else:
                ref[at] = value
        return square_sum(master), square_sum(results[2])

    def add(total, index, pair, scale=1.0):
        for column in range(2):
            here = jnp.logical_and(row == index, lane == column)
            total = total + jnp.where(here, pair[column] * scale, 0.0)
        return total

    for kind in range(3):
        at = hidden_here + kind * head_cols
        sums = add(sums, 0, one(0, summed_ref[:, at : at + head_cols], kind))
    outward_at = back_width + hidden_here
    sums = add(sums, 1, one(1, summed_ref[:, outward_at:used].T))
    sums = add(sums, 2, one(2, summed_ref[:, :hidden_here]))
    sums = add(sums, 3, one(3, summed_ref[:, back_width:outward_at].T))
    gain = summed_ref[:, width - 128 :].T
    sums = add(sums, 4, one(4, gain[127:128]), replicas)
    sums_ref[...] = sums


def fresh_kernel(sums_ref, *refs):
    masters, updates, fresh, low = refs[:5], refs[5:10], refs[10:15], refs[15:20]
    for index in range(5):
        norms = jnp.sqrt(sums_ref[index : index + 1, :])
        rate = learn_rate * (norms[:, 0:1] / norms[:, 1:2])
        if len(masters[index].shape) == 3:
            rate = rate.reshape(1, 1, 1)
        value = masters[index][...] - rate * updates[index][...]
        fresh[index][...] = value
        low[index][...] = value.astype(jnp.bfloat16)


def lamb_step(summed, states, cuts):
    vmem = pl.BlockSpec(memory_space=pltpu.VMEM)
    flat = [array for group in states for array in group]
    like = [jax.ShapeDtypeStruct(array.shape, jnp.float32) for array in flat]
    *parts, sums = pl.pallas_call(
        functools.partial(parts_kernel, cuts, 1.0 / lax.axis_size("tensor")),
        out_shape=like + [jax.ShapeDtypeStruct((8, 128), jnp.float32)],
        in_specs=[vmem] * 16,
        out_specs=[vmem] * 16,
        compiler_params=pltpu.CompilerParams(vmem_limit_bytes=40 * 2**20),
        name="lamb_parts",
    )(summed, *flat)
    sums = total_of(sums, 3)
    masters = [group[0] for group in states]
    fresh = pl.pallas_call(
        fresh_kernel,
        out_shape=[jax.ShapeDtypeStruct(m.shape, jnp.float32) for m in masters]
        + [jax.ShapeDtypeStruct(m.shape, jnp.bfloat16) for m in masters],
        in_specs=[vmem] * 11,
        out_specs=[vmem] * 10,
        compiler_params=pltpu.CompilerParams(vmem_limit_bytes=40 * 2**20),
        name="lamb_fresh",
    )(sums, *masters, *parts[2::3])
    return parts, fresh, jnp.sqrt(sums[:5, :2])


def local(
    inputs,
    cotangent,
    master_inward,
    first_inward,
    second_inward,
    master_outward,
    first_outward,
    second_outward,
    master_widening,
    first_widening,
    second_widening,
    master_narrowing,
    first_narrowing,
    second_narrowing,
    master_scaling,
    first_scaling,
    second_scaling,
):
    depth = master_widening.shape[0]
    hidden_here = master_widening.shape[1]
    head_cols = master_inward.shape[2]
    model = inputs.shape[1]
    back_width = hidden_here + 3 * head_cols
    gap = (-back_width) % 128
    back_width += gap
    used = back_width + hidden_here + head_cols
    width = -(-(used + 1) // 128) * 128
    shard = jnp.concatenate(
        [
            master_widening,
            jnp.transpose(master_inward, (1, 0, 2)).reshape(depth, 3 * head_cols),
            jnp.zeros((depth, gap), jnp.float32),
            master_narrowing.T,
            master_outward.T,
            jnp.broadcast_to(master_scaling[:, None], (depth, width - used)),
        ],
        axis=1,
    ).astype(jnp.bfloat16)
    copies = gather_blocks(shard).reshape(model, width)
    rows_here = inputs.shape[0]
    whole_rows = rows_here // 16 * 16
    tails = jnp.stack(
        [
            jnp.pad(rows[whole_rows:], ((0, whole_rows + 16 - rows_here), (0, 0)))
            for rows in (inputs, cotangent)
        ]
    )
    summed_out, input_grad, grads = image_block(
        inputs, cotangent, tails, copies, hidden_here, head_cols, back_width
    )
    share = rows_here // lax.axis_size("tensor")
    start = lax.axis_index("tensor") * share
    output = lax.dynamic_slice_in_dim(summed_out, start, share, 0)
    summed = reduce_blocks(grads.reshape(lax.axis_size("dp"), depth, width))
    states = (
        (master_inward, first_inward, second_inward),
        (master_outward, first_outward, second_outward),
        (master_widening, first_widening, second_widening),
        (master_narrowing, first_narrowing, second_narrowing),
        tuple(v.reshape(1, depth) for v in (master_scaling, first_scaling, second_scaling)),
    )
    parts, fresh, trust_norms = lamb_step(
        summed, states, (hidden_here, head_cols, back_width, used)
    )
    results = []
    for index in range(5):
        group = (parts[3 * index], parts[3 * index + 1], fresh[index], fresh[5 + index])
        results += [v.reshape(depth) for v in group] if index == 4 else group
    return (output, input_grad, *results, trust_norms)


def solution(mesh):
    in_specs = (
        P("dp", None),
        P("dp", None),
        P(None, "dp", "tensor"),
        P(None, "dp", "tensor"),
        P(None, "dp", "tensor"),
        P("tensor", "dp"),
        P("tensor", "dp"),
        P("tensor", "dp"),
        P("dp", "tensor"),
        P("dp", "tensor"),
        P("dp", "tensor"),
        P("tensor", "dp"),
        P("tensor", "dp"),
        P("tensor", "dp"),
        P("dp"),
        P("dp"),
        P("dp"),
    )
    out_specs = (
        P(("dp", "tensor"), None),
        P("dp", None),
        P(None, "dp", "tensor"),
        P(None, "dp", "tensor"),
        P(None, "dp", "tensor"),
        P(None, "dp", "tensor"),
        P("tensor", "dp"),
        P("tensor", "dp"),
        P("tensor", "dp"),
        P("tensor", "dp"),
        P("dp", "tensor"),
        P("dp", "tensor"),
        P("dp", "tensor"),
        P("dp", "tensor"),
        P("tensor", "dp"),
        P("tensor", "dp"),
        P("tensor", "dp"),
        P("tensor", "dp"),
        P("dp"),
        P("dp"),
        P("dp"),
        P("dp"),
        P(),
    )
    return jax.shard_map(local, mesh=mesh, in_specs=in_specs, out_specs=out_specs, check_vma=False)
```

```python
import functools

import jax
import jax.numpy as jnp
from jax import lax
from jax.experimental import pallas as pl
from jax.experimental.pallas import tpu as pltpu
from jax.sharding import PartitionSpec as P

MESH = pl.DeviceIdType.MESH
PAIR = 2

HEAD_DIM = 64
SEQ = 196
STEP = 5


norm_eps = 1e-06
beta_one = 0.5
beta_two = 0.5
lamb_eps = 1e-06
weight_decay = 0.01
learn_rate = 0.5


def lamb_parts(master, first, second, grad):
    moment = beta_one * first + (1.0 - beta_one) * grad
    square = beta_two * second + (1.0 - beta_two) * grad * grad
    update = (
        moment / (1.0 - beta_one**STEP) / (jnp.sqrt(square / (1.0 - beta_two**STEP)) + lamb_eps)
        + weight_decay * master
    )
    return (moment, square, update)


def greet(place, line, up, down, other):
    barrier = pltpu.get_barrier_semaphore()
    pl.semaphore_signal(barrier, inc=1, device_id=other, device_id_type=MESH)

    @pl.when(place < line - 1)
    def _():
        pl.semaphore_signal(barrier, inc=1, device_id=up, device_id_type=MESH)

    @pl.when(place > 0)
    def _():
        pl.semaphore_signal(barrier, inc=1, device_id=down, device_id_type=MESH)

    pl.semaphore_wait(barrier, 1 + jnp.minimum(place, 1) + jnp.minimum(line - 1 - place, 1))


def gather_kernel(line, own_ref, all_ref, own_sem, up_sem, down_sem, pair_sem, recv_sem):
    me = lax.axis_index("dp")
    place, side = me // PAIR, me % PAIR
    up, down, other = {"dp": me + PAIR}, {"dp": me - PAIR}, {"dp": me + 1 - 2 * side}
    has_up, has_down = place < line - 1, place > 0
    greet(place, line, up, down, other)

    def move(step, source, block, sems, peer):
        return pltpu.make_async_remote_copy(
            src_ref=source,
            dst_ref=all_ref.at[block],
            send_sem=sems.at[step],
            recv_sem=recv_sem.at[block],
            device_id=peer,
            device_id_type=MESH,
        )

    def held(block):
        return all_ref.at[block]

    def arrived(block, peer):
        move(0, held(block), block, pair_sem, peer).wait_recv()

    own = pltpu.make_async_copy(own_ref, all_ref.at[me], own_sem)

    @pl.when(has_up)
    def _():
        move(place, own_ref, me, up_sem, up).start()

    @pl.when(has_down)
    def _():
        move(place, own_ref, me, down_sem, down).start()

    move(place, own_ref, me, pair_sem, other).start()
    own.start()

    @pl.loop(1, line)
    def _(step):
        low, high = place - step, place + step

        @pl.when(low >= 0)
        def _():
            block = low * PAIR + side
            arrived(block, other)

            @pl.when(has_up)
            def _():
                move(low, held(block), block, up_sem, up).start()

            move(low, held(block), block, pair_sem, other).start()

        @pl.when(high < line)
        def _():
            block = high * PAIR + side
            arrived(block, other)

            @pl.when(has_down)
            def _():
                move(high, held(block), block, down_sem, down).start()

            move(high, held(block), block, pair_sem, other).start()

    own.wait()

    @pl.loop(0, line)
    def _(spot):
        block = spot * PAIR + side
        arrived(spot * PAIR + 1 - side, other)
        move(spot, held(block), block, pair_sem, other).wait_send()

        @pl.when(jnp.logical_and(has_up, spot <= place))
        def _():
            move(spot, held(block), block, up_sem, up).wait_send()

        @pl.when(jnp.logical_and(has_down, spot >= place))
        def _():
            move(spot, held(block), block, down_sem, down).wait_send()


def gather_blocks(own):
    rows, width = own.shape
    devices = lax.axis_size("dp")
    line = devices // PAIR
    return pl.pallas_call(
        functools.partial(gather_kernel, line),
        out_shape=jax.ShapeDtypeStruct((devices, rows, width), own.dtype),
        in_specs=[pl.BlockSpec(memory_space=pltpu.VMEM)],
        out_specs=pl.BlockSpec(memory_space=pl.ANY),
        scratch_shapes=[
            pltpu.SemaphoreType.DMA,
            pltpu.SemaphoreType.DMA((line,)),
            pltpu.SemaphoreType.DMA((line,)),
            pltpu.SemaphoreType.DMA((line,)),
            pltpu.SemaphoreType.DMA((devices,)),
        ],
        compiler_params=pltpu.CompilerParams(collective_id=0, has_side_effects=True),
        cost_estimate=pl.CostEstimate(flops=0, bytes_accessed=100_000_000, transcendentals=0),
        name="gather_blocks",
    )(own)


def reduce_kernel(
    line, own_ref, sum_ref, pair_in, up_in, down_in, up_out, down_out,
    pair_send, pair_recv, up_send, up_recv, down_send, down_recv,
):
    me = lax.axis_index("dp")
    place, side = me // PAIR, me % PAIR
    up, down, other = {"dp": me + PAIR}, {"dp": me - PAIR}, {"dp": me + 1 - 2 * side}
    has_up, has_down = place < line - 1, place > 0
    greet(place, line, up, down, other)

    def pair_move(spot):
        return pltpu.make_async_remote_copy(
            src_ref=own_ref.at[spot * PAIR + 1 - side],
            dst_ref=pair_in.at[spot],
            send_sem=pair_send.at[spot],
            recv_sem=pair_recv.at[spot],
            device_id=other,
            device_id_type=MESH,
        )

    def line_move(spot, source, target, sends, recvs, peer):
        return pltpu.make_async_remote_copy(
            src_ref=source.at[spot],
            dst_ref=target.at[spot],
            send_sem=sends.at[spot],
            recv_sem=recvs.at[spot],
            device_id=peer,
            device_id_type=MESH,
        )

    def up_move(spot):
        return line_move(spot, up_out, up_in, up_send, up_recv, up)

    def down_move(spot):
        return line_move(spot, down_out, down_in, down_send, down_recv, down)

    @pl.loop(0, line)
    def _(turn):
        far = line - 1 - turn

        @pl.when(place + far < line)
        def _():
            pair_move(place + far).start()

        @pl.when(jnp.logical_and(place - far >= 0, far > 0))
        def _():
            pair_move(place - far).start()

    def both(spot):
        return own_ref[spot * PAIR + side].astype(jnp.float32) + pair_in[spot].astype(jnp.float32)

    @pl.loop(0, line - 1)
    def _(turn):
        far = line - 1 - turn

        @pl.when(place + far < line)
        def _():
            spot = place + far
            pair_move(spot).wait_recv()

            @pl.when(has_down)
            def _():
                up_move(spot).wait_recv()
                up_out[spot] = (both(spot) + up_in[spot].astype(jnp.float32)).astype(jnp.bfloat16)

            @pl.when(jnp.logical_not(has_down))
            def _():
                up_out[spot] = both(spot).astype(jnp.bfloat16)

            up_move(spot).start()

        @pl.when(place - far >= 0)
        def _():
            spot = place - far
            pair_move(spot).wait_recv()

            @pl.when(has_up)
            def _():
                down_move(spot).wait_recv()
                down_out[spot] = (both(spot) + down_in[spot].astype(jnp.float32)).astype(
                    jnp.bfloat16
                )

            @pl.when(jnp.logical_not(has_up))
            def _():
                down_out[spot] = both(spot).astype(jnp.bfloat16)

            down_move(spot).start()

    pair_move(place).wait_recv()
    sum_ref[...] = both(place)

    @pl.when(has_down)
    def _():
        up_move(place).wait_recv()
        sum_ref[...] += up_in[place].astype(jnp.float32)

    @pl.when(has_up)
    def _():
        down_move(place).wait_recv()
        sum_ref[...] += down_in[place].astype(jnp.float32)

    @pl.loop(0, line)
    def _(spot):
        pair_move(spot).wait_send()

        @pl.when(spot > place)
        def _():
            up_move(spot).wait_send()

        @pl.when(spot < place)
        def _():
            down_move(spot).wait_send()


def reduce_blocks(own):
    devices, rows, width = own.shape
    line = devices // PAIR
    buffer = pltpu.VMEM((line, rows, width), own.dtype)
    return pl.pallas_call(
        functools.partial(reduce_kernel, line),
        out_shape=jax.ShapeDtypeStruct((rows, width), jnp.float32),
        in_specs=[pl.BlockSpec(memory_space=pltpu.VMEM)],
        out_specs=pl.BlockSpec(memory_space=pltpu.VMEM),
        scratch_shapes=[buffer] * 5 + [pltpu.SemaphoreType.DMA((line,))] * 6,
        compiler_params=pltpu.CompilerParams(
            collective_id=1, has_side_effects=True, vmem_limit_bytes=40 * 2**20
        ),
        cost_estimate=pl.CostEstimate(flops=0, bytes_accessed=100_000_000, transcendentals=0),
        name="reduce_blocks",
    )(own)


def total_kernel(
    devices, ranks, own_ref, sum_ref, rank_in, dp_out, dp_in,
    rank_send, rank_recv, dp_send, dp_recv,
):
    me, rank = lax.axis_index("dp"), lax.axis_index("tensor")
    barrier = pltpu.get_barrier_semaphore()
    for shift in range(1, ranks):
        peer = {"tensor": lax.rem(rank + shift, ranks)}
        pl.semaphore_signal(barrier, inc=1, device_id=peer, device_id_type=MESH)
    for shift in range(1, devices):
        peer = {"dp": lax.rem(me + shift, devices)}
        pl.semaphore_signal(barrier, inc=1, device_id=peer, device_id_type=MESH)
    pl.semaphore_wait(barrier, ranks - 1 + devices - 1)

    def rank_move(shift):
        return pltpu.make_async_remote_copy(
            src_ref=own_ref,
            dst_ref=rank_in.at[rank],
            send_sem=rank_send.at[shift],
            recv_sem=rank_recv.at[rank],
            device_id={"tensor": lax.rem(rank + shift, ranks)},
            device_id_type=MESH,
        )

    def rank_arrival(source):
        return pltpu.make_async_remote_copy(
            src_ref=own_ref,
            dst_ref=rank_in.at[source],
            send_sem=rank_send.at[0],
            recv_sem=rank_recv.at[source],
            device_id={"tensor": lax.rem(rank + 1, ranks)},
            device_id_type=MESH,
        )

    def dp_move(shift):
        return pltpu.make_async_remote_copy(
            src_ref=dp_out,
            dst_ref=dp_in.at[me],
            send_sem=dp_send.at[shift],
            recv_sem=dp_recv.at[me],
            device_id={"dp": lax.rem(me + shift, devices)},
            device_id_type=MESH,
        )

    def dp_arrival(source):
        return pltpu.make_async_remote_copy(
            src_ref=dp_out,
            dst_ref=dp_in.at[source],
            send_sem=dp_send.at[0],
            recv_sem=dp_recv.at[source],
            device_id={"dp": lax.rem(me + 1, devices)},
            device_id_type=MESH,
        )

    for shift in range(1, ranks):
        rank_move(shift).start()
    rank_in[rank] = own_ref[...]
    for shift in range(1, ranks):
        rank_arrival(lax.rem(rank + shift, ranks)).wait_recv()
    part = rank_in[0]
    for spot in range(1, ranks):
        part = part + rank_in[spot]
    dp_out[...] = part
    for shift in range(1, devices):
        dp_move(shift).start()
    dp_in[me] = part
    for shift in range(1, devices):
        dp_arrival(lax.rem(me + shift, devices)).wait_recv()
    whole = dp_in[0]
    for spot in range(1, devices):
        whole = whole + dp_in[spot]
    sum_ref[...] = whole
    for shift in range(1, ranks):
        rank_move(shift).wait_send()
    for shift in range(1, devices):
        dp_move(shift).wait_send()


def total_of(own, collective_id):
    devices, ranks = lax.axis_size("dp"), lax.axis_size("tensor")
    return pl.pallas_call(
        functools.partial(total_kernel, devices, ranks),
        out_shape=jax.ShapeDtypeStruct(own.shape, own.dtype),
        in_specs=[pl.BlockSpec(memory_space=pltpu.VMEM)],
        out_specs=pl.BlockSpec(memory_space=pltpu.VMEM),
        scratch_shapes=[
            pltpu.VMEM((ranks,) + own.shape, own.dtype),
            pltpu.VMEM(own.shape, own.dtype),
            pltpu.VMEM((devices,) + own.shape, own.dtype),
            pltpu.SemaphoreType.DMA((ranks,)),
            pltpu.SemaphoreType.DMA((ranks,)),
            pltpu.SemaphoreType.DMA((devices,)),
            pltpu.SemaphoreType.DMA((devices,)),
        ],
        compiler_params=pltpu.CompilerParams(
            collective_id=collective_id, has_side_effects=True, vmem_limit_bytes=60 * 2**20
        ),
        cost_estimate=pl.CostEstimate(flops=0, bytes_accessed=20_000_000, transcendentals=0),
        name="total_" + str(collective_id),
    )(own)


WINDOW = 224


def image_kernel(
    images, cuts, x_hbm, c_hbm, tail_ref, w_ref,
    out_ref, grad_in_ref, g_ref,
    acc1, acc2, gain_row, g_gain, windows, kept, qkv, back_cols, front_cols,
    partial, pair_in, chip_sum, line_in, total,
    in_sem, s1, r1, s2, r2, s3, r3,
):
    step = pl.program_id(0)
    rank = lax.axis_index("tensor")
    core = rank % 2
    sibling = {"tensor": rank + 1 - 2 * core}
    across = {"tensor": lax.rem(rank + 2, 4)}
    width, head_cols = cuts
    heads = head_cols // HEAD_DIM
    rows, model = kept.shape[2], kept.shape[3]
    half = model // 2
    f32, b16 = jnp.float32, jnp.bfloat16
    back_width, front_width = back_cols.shape[1], front_cols.shape[1]
    last_window = images * SEQ // 16 * 16 - WINDOW

    def window_start(image):
        return pl.multiple_of(jnp.minimum(image * SEQ // 16 * 16, last_window), 16)

    def fetches(image, slot):
        return [
            pltpu.make_async_copy(
                source.at[pl.ds(window_start(image), WINDOW)],
                windows.at[slot, kind, pl.ds(0, WINDOW)],
                in_sem.at[slot, kind],
            )
            for kind, source in ((0, x_hbm), (1, c_hbm))
        ]

    def one_hot(shape, row_is):
        at = [lax.broadcasted_iota(jnp.int32, shape, axis) for axis in (0, 1)]
        return jnp.where(row_is(*at), 1.0, 0.0).astype(b16)

    @pl.when(step == 0)
    def _():
        barrier = pltpu.get_barrier_semaphore()
        pl.semaphore_signal(barrier, inc=1, device_id=sibling, device_id_type=MESH)
        pl.semaphore_signal(barrier, inc=1, device_id=across, device_id_type=MESH)
        pl.semaphore_wait(barrier, 2)
        for copy in fetches(0, 0):
            copy.start()
        for slot in range(2):
            for kind in range(2):
                windows[slot, kind, WINDOW:] = tail_ref[kind]
        total[...] = jnp.zeros_like(total)
        kept[...] = jnp.zeros_like(kept)
        acc1[...] = jnp.zeros_like(acc1)
        acc2[...] = jnp.zeros_like(acc2)
        back_cols[...] = jnp.zeros_like(back_cols)
        front_cols[...] = jnp.zeros_like(front_cols)
        g_gain[...] = jnp.zeros_like(g_gain)
        for ref in (out_ref, grad_in_ref):
            ref[:16] = jnp.zeros((16, model), b16)
        turned = w_ref[:, back_width + front_width - 128 :].astype(f32).T
        gain_row[...] = turned[127:128]

    @pl.when(step < images - 1)
    def _():
        for copy in fetches(step + 1, (step + 1) % 2):
            copy.start()

    def move(source, target, sends, recvs, slot, peer):
        return pltpu.make_async_remote_copy(
            src_ref=source,
            dst_ref=target,
            send_sem=sends.at[slot],
            recv_sem=recvs.at[slot],
            device_id=peer,
            device_id_type=MESH,
        )

    def first(slot):
        return move(partial.at[slot, 1 - core], pair_in.at[slot], s1, r1, slot, sibling)

    def second(slot):
        return move(chip_sum.at[slot], line_in.at[slot], s2, r2, slot, across)

    def third(slot):
        return move(total.at[slot, core], total.at[slot, core], s3, r3, slot, sibling)

    def normalised(values):
        floats = values.astype(f32)
        centred = floats - jnp.mean(floats, axis=1, keepdims=True)
        inv_std = lax.rsqrt(jnp.mean(centred * centred, axis=1, keepdims=True) + norm_eps)
        return floats, centred * inv_std, inv_std

    gain = gain_row[...]

    image = jnp.maximum(step - 3, 0)

    def place(ref, values):
        start = pl.multiple_of(image * SEQ // 16 * 16, 16)
        offset = image * SEQ - start
        spread = one_hot((WINDOW, rows), lambda r, j: jnp.logical_and(r == j + offset, j < SEQ))
        placed = jnp.dot(spread, values, preferred_element_type=f32)
        before = lax.broadcasted_iota(jnp.int32, (16, model), 0) < offset
        head = jnp.where(before, ref[pl.ds(start, 16), :].astype(f32), placed[:16])
        ref[pl.ds(start, 16), :] = head.astype(b16)
        ref[pl.ds(start + 16, WINDOW - 16), :] = placed[16:].astype(b16)

    def place_late(ref, values):
        @pl.when(step < images + 2)
        def _():
            place(ref, values)

        @pl.when(step == images + 2)
        def _():
            ref[(images - 1) * SEQ :] = values[:SEQ]

    @pl.when(step >= 3)
    def _():
        third((step - 3) % 3).wait()

    def finish(put):
        slot, spot = (step + 3) % 3, (step + 1) % 4
        floats, unit, inv_std = normalised(kept[spot, 0])
        sums = jnp.concatenate([total[slot, 0, 0], total[slot, 1, 0]], axis=1).astype(f32)
        put(out_ref, (floats + sums).astype(b16))
        d_normed = jnp.concatenate([total[slot, 0, 1], total[slot, 1, 1]], axis=1).astype(f32)
        weighted = d_normed * unit
        counted = jnp.sum(weighted, axis=0, keepdims=True)
        g_gain[...] += jnp.where(step >= 3, counted, 0.0)
        d_unit = d_normed * gain
        d_floats = inv_std * (
            d_unit
            - jnp.mean(d_unit, axis=1, keepdims=True)
            - unit * jnp.mean(weighted * gain, axis=1, keepdims=True)
        )
        put(grad_in_ref, (kept[spot, 1].astype(f32) + d_floats).astype(b16))

    @pl.when(jnp.logical_and(step >= 2, step < images + 2))
    def _():
        slot, spot = (step - 2) % 2, (step - 2) % 3
        second(slot).wait()
        total[spot, core] = (chip_sum[slot].astype(f32) + line_in[slot].astype(f32)).astype(b16)
        third(spot).start()

    @pl.when(jnp.logical_and(step >= 1, step < images + 1))
    def _():
        slot = (step - 1) % 2
        first(slot).wait()
        chip_sum[slot] = (partial[slot, core].astype(f32) + pair_in[slot].astype(f32)).astype(b16)
        second(slot).start()

    @pl.when(step < images)
    def _():
        slot = step % 2
        for copy in fetches(step, slot):
            copy.wait()
        offset = step * SEQ - window_start(step)
        pick = one_hot(
            (rows, windows.shape[2]), lambda r, j: jnp.logical_and(j == r + offset, r < SEQ)
        )
        for kind in range(2):
            kept[step % 4, kind] = jnp.dot(
                pick, windows[slot, kind], preferred_element_type=f32
            ).astype(b16)
        _floats, unit, _inv = normalised(kept[step % 4, 0])
        normed = (unit * gain).astype(b16)
        cot = kept[step % 4, 1]

        def mm(a, b):
            return jnp.dot(a, b, preferred_element_type=f32)

        def mm_nt(a, b):
            return lax.dot_general(a, b, (((1,), (1,)), ((), ())), preferred_element_type=f32)

        def mm_tn(a, b):
            return lax.dot_general(a, b, (((0,), (0,)), ((), ())), preferred_element_type=f32)

        qkv[:, : 3 * head_cols] = mm(normed, w_ref[:, width:back_width])[:, : 3 * head_cols].astype(b16)
        qkv[:, 3 * head_cols :] = mm(cot, w_ref[:, back_width + width :])[:, :head_cols].astype(b16)
        keys_wide = pl.cdiv(rows, 128) * 128
        filler = jnp.zeros((keys_wide - rows, HEAD_DIM), b16)
        real = lax.broadcasted_iota(jnp.int32, (rows, keys_wide), 1) < SEQ
        for head in range(heads):
            def part(kind):
                at = kind * head_cols + head * HEAD_DIM
                return qkv[:, at : at + HEAD_DIM]

            query = part(0) * jnp.asarray(HEAD_DIM ** (-0.5), b16)
            key = jnp.concatenate([part(1), filler], axis=0)
            value = jnp.concatenate([part(2), filler], axis=0)
            d_att = part(3)
            scores = jnp.where(real, mm_nt(query, key), -1e30)
            powers = jnp.exp(scores - jnp.max(scores, axis=1, keepdims=True))
            probs = powers * (1.0 / jnp.sum(powers, axis=1, keepdims=True))
            probs_low = probs.astype(b16)
            spot = head * HEAD_DIM
            front_cols[:, width + spot : width + spot + HEAD_DIM] = mm(probs_low, value).astype(b16)
            d_probs = mm_nt(d_att, value)
            d_value = mm_tn(probs_low, d_att)[:rows].astype(b16)
            inner = jnp.sum(probs * d_probs, axis=1, keepdims=True)
            d_scores = (probs * (d_probs - inner)).astype(b16)
            d_query = (mm(d_scores, key) * (HEAD_DIM ** (-0.5))).astype(b16)
            d_key = mm_tn(d_scores, query)[:rows].astype(b16)
            for kind, value_of in ((0, d_query), (1, d_key), (2, d_value)):
                at = width + kind * head_cols + spot
                back_cols[:, at : at + HEAD_DIM] = value_of

        upper = mm(normed, w_ref[:, :width])
        d_hidden = mm(cot, w_ref[:, back_width : back_width + width])
        scale = (2.0 / 3.141592653589793) ** 0.5
        square = upper * upper
        bend = jnp.tanh(scale * upper * (1.0 + 0.044715 * square))
        step_up = 0.5 * (1.0 + bend)
        front_cols[:, :width] = (upper * step_up).astype(b16)
        slope = step_up + (0.5 * scale) * upper * (1.0 - bend * bend) * (
            1.0 + (3.0 * 0.044715) * square
        )
        back_cols[:, :width] = (d_hidden * slope).astype(b16)

        finish(place)
        out_part = mm_nt(front_cols[...], w_ref[:, back_width:]).astype(b16)
        partial[slot, 0, 0] = out_part[:, :half]
        partial[slot, 1, 0] = out_part[:, half:]
        back_part = mm_nt(back_cols[...], w_ref[:, :back_width]).astype(b16)
        partial[slot, 0, 1] = back_part[:, :half]
        partial[slot, 1, 1] = back_part[:, half:]
        first(slot).start()
        acc1[...] += mm_tn(normed, back_cols[...])
        acc2[...] += mm_tn(cot, front_cols[...])

    @pl.when(step >= images)
    def _():
        finish(place_late)

    @pl.when(step == images + 2)
    def _():
        g_ref[:, :back_width] = acc1[...].astype(b16)
        inner = back_width + front_width - 128
        g_ref[:, back_width:inner] = acc2[:, : front_width - 128].astype(b16)
        spare = jnp.broadcast_to(g_gain[...], (128, model)).T
        last = lax.broadcasted_iota(jnp.int32, (model, 128), 1) == 127
        g_ref[:, inner:] = jnp.where(last, spare, acc2[:, front_width - 128 :]).astype(b16)


def image_block(inputs, cotangent, tails, weights, width, head_cols, back_width):
    tokens, model = inputs.shape
    images = tokens // SEQ
    rows = -(-SEQ // 16) * 16
    half = model // 2
    front_width = weights.shape[1] - back_width
    fixed = lambda i: (0, 0)

    def whole(shape):
        return pl.BlockSpec(shape, fixed, pipeline_mode=pl.Buffered(1))

    bf = jnp.bfloat16
    anywhere = pl.BlockSpec(memory_space=pl.ANY)
    return pl.pallas_call(
        functools.partial(image_kernel, images, (width, head_cols)),
        grid=(images + 3,),
        out_shape=(
            jax.ShapeDtypeStruct(inputs.shape, bf),
            jax.ShapeDtypeStruct(inputs.shape, bf),
            jax.ShapeDtypeStruct(weights.shape, bf),
        ),
        in_specs=[
            anywhere,
            anywhere,
            pl.BlockSpec(tails.shape, lambda i: (0, 0, 0), pipeline_mode=pl.Buffered(1)),
            whole(weights.shape),
        ],
        out_specs=[whole(inputs.shape), whole(inputs.shape), whole(weights.shape)],
        scratch_shapes=[
            pltpu.VMEM((model, back_width), jnp.float32),
            pltpu.VMEM((model, front_width), jnp.float32),
            pltpu.VMEM((1, model), jnp.float32),
            pltpu.VMEM((1, model), jnp.float32),
            pltpu.VMEM((2, 2, WINDOW + tails.shape[1], model), bf),
            pltpu.VMEM((4, 2, rows, model), bf),
            pltpu.VMEM((rows, 4 * head_cols), bf),
            pltpu.VMEM((rows, back_width), bf),
            pltpu.VMEM((rows, front_width), bf),
            pltpu.VMEM((2, 2, 2, rows, half), bf),
            pltpu.VMEM((2, 2, rows, half), bf),
            pltpu.VMEM((2, 2, rows, half), bf),
            pltpu.VMEM((2, 2, rows, half), bf),
            pltpu.VMEM((3, 2, 2, rows, half), bf),
            pltpu.SemaphoreType.DMA((2, 2)),
        ]
        + [pltpu.SemaphoreType.DMA((2,))] * 4
        + [pltpu.SemaphoreType.DMA((3,))] * 2,
        compiler_params=pltpu.CompilerParams(
            collective_id=4,
            has_side_effects=True,
            vmem_limit_bytes=60 * 2**20,
            dimension_semantics=("arbitrary",),
        ),
        name="image_block",
    )(inputs, cotangent, tails, weights)


def parts_kernel(cuts, replicas, summed_ref, *refs):
    states, outs, sums_ref = refs[:15], refs[15:30], refs[30]
    hidden_here, head_cols, back_width, used = cuts
    width = summed_ref.shape[1]
    row = lax.broadcasted_iota(jnp.int32, sums_ref.shape, 0)
    lane = lax.broadcasted_iota(jnp.int32, sums_ref.shape, 1)
    sums = jnp.zeros(sums_ref.shape, jnp.float32)

    def square_sum(values):
        return jnp.sum(jnp.sum(values * values, axis=1, keepdims=True), axis=0, keepdims=True)

    def one(index, grad, at=None):
        master, first, second = (
            ref[...] if at is None else ref[at] for ref in states[3 * index : 3 * index + 3]
        )
        results = lamb_parts(master, first, second, grad)
        for ref, value in zip(outs[3 * index : 3 * index + 3], results):
            if at is None:
                ref[...] = value
            else:
                ref[at] = value
        return square_sum(master), square_sum(results[2])

    def add(total, index, pair, scale=1.0):
        for column in range(2):
            here = jnp.logical_and(row == index, lane == column)
            total = total + jnp.where(here, pair[column] * scale, 0.0)
        return total

    for kind in range(3):
        at = hidden_here + kind * head_cols
        sums = add(sums, 0, one(0, summed_ref[:, at : at + head_cols], kind))
    outward_at = back_width + hidden_here
    sums = add(sums, 1, one(1, summed_ref[:, outward_at:used].T))
    sums = add(sums, 2, one(2, summed_ref[:, :hidden_here]))
    sums = add(sums, 3, one(3, summed_ref[:, back_width:outward_at]))
    gain = summed_ref[:, width - 128 :].T
    sums = add(sums, 4, one(4, gain[127:128]), replicas)
    sums_ref[...] = sums


def fresh_kernel(sums_ref, *refs):
    masters, updates, fresh, low = refs[:5], refs[5:10], refs[10:15], refs[15:20]
    for index in range(5):
        norms = jnp.sqrt(sums_ref[index : index + 1, :])
        rate = learn_rate * (norms[:, 0:1] / norms[:, 1:2])
        if len(masters[index].shape) == 3:
            rate = rate.reshape(1, 1, 1)
        value = masters[index][...] - rate * updates[index][...]
        fresh[index][...] = value
        low[index][...] = value.astype(jnp.bfloat16)


def lamb_step(summed, states, cuts):
    def blocks(arrays):
        return [pl.BlockSpec(a.shape, lambda i, n=a.ndim: (0,) * n) for a in arrays]

    one_step = {"grid": (1,), "compiler_params": pltpu.CompilerParams(vmem_limit_bytes=60 * 2**20)}
    flat = [array for group in states for array in group]
    like = [jax.ShapeDtypeStruct(array.shape, jnp.float32) for array in flat]
    like.append(jax.ShapeDtypeStruct((8, 128), jnp.float32))
    *parts, sums = pl.pallas_call(
        functools.partial(parts_kernel, cuts, 1.0 / lax.axis_size("tensor")),
        out_shape=like,
        in_specs=blocks([summed, *flat]),
        out_specs=blocks(like),
        name="lamb_parts",
        **one_step,
    )(summed, *flat)
    sums = total_of(sums, 3)
    masters = [group[0] for group in states]
    made = [jax.ShapeDtypeStruct(m.shape, t) for t in (jnp.float32, jnp.bfloat16) for m in masters]
    fresh = pl.pallas_call(
        fresh_kernel,
        out_shape=made,
        in_specs=blocks([sums, *masters, *masters]),
        out_specs=blocks(made),
        name="lamb_fresh",
        **one_step,
    )(sums, *masters, *parts[2::3])
    return parts, fresh, jnp.sqrt(sums[:5, :2])


def local(
    inputs,
    cotangent,
    master_inward,
    first_inward,
    second_inward,
    master_outward,
    first_outward,
    second_outward,
    master_widening,
    first_widening,
    second_widening,
    master_narrowing,
    first_narrowing,
    second_narrowing,
    master_scaling,
    first_scaling,
    second_scaling,
):
    depth = master_widening.shape[0]
    hidden_here = master_widening.shape[1]
    head_cols = master_inward.shape[2]
    model = inputs.shape[1]
    back_width = hidden_here + 3 * head_cols
    gap = (-back_width) % 128
    back_width += gap
    used = back_width + hidden_here + head_cols
    width = -(-(used + 1) // 128) * 128
    shard = jnp.concatenate(
        [
            master_widening,
            jnp.transpose(master_inward, (1, 0, 2)).reshape(depth, 3 * head_cols),
            jnp.zeros((depth, gap), jnp.float32),
            master_narrowing.T,
            master_outward.T,
            jnp.broadcast_to(master_scaling[:, None], (depth, width - used)),
        ],
        axis=1,
    ).astype(jnp.bfloat16)
    copies = gather_blocks(shard).reshape(model, width)
    rows_here = inputs.shape[0]
    whole_rows = rows_here // 16 * 16
    tails = jnp.stack(
        [
            jnp.pad(rows[whole_rows:], ((0, whole_rows + 16 - rows_here), (0, 0)))
            for rows in (inputs, cotangent)
        ]
    )
    summed_out, input_grad, grads = image_block(
        inputs, cotangent, tails, copies, hidden_here, head_cols, back_width
    )
    share = rows_here // lax.axis_size("tensor")
    start = lax.axis_index("tensor") * share
    output = lax.dynamic_slice_in_dim(summed_out, start, share, 0)
    summed = reduce_blocks(grads.reshape(lax.axis_size("dp"), depth, width))
    states = (
        (master_inward, first_inward, second_inward),
        (master_outward, first_outward, second_outward),
        (master_widening, first_widening, second_widening),
        (master_narrowing.T, first_narrowing.T, second_narrowing.T),
        tuple(v.reshape(1, depth) for v in (master_scaling, first_scaling, second_scaling)),
    )
    parts, fresh, trust_norms = lamb_step(
        summed, states, (hidden_here, head_cols, back_width, used)
    )
    results = []
    for index in range(5):
        group = (parts[3 * index], parts[3 * index + 1], fresh[index], fresh[5 + index])
        if index == 3:
            group = [v.T for v in group]
        if index == 4:
            group = [v.reshape(depth) for v in group]
        results += group
    return (output, input_grad, *results, trust_norms)


def solution(mesh):
    in_specs = (
        P("dp", None),
        P("dp", None),
        P(None, "dp", "tensor"),
        P(None, "dp", "tensor"),
        P(None, "dp", "tensor"),
        P("tensor", "dp"),
        P("tensor", "dp"),
        P("tensor", "dp"),
        P("dp", "tensor"),
        P("dp", "tensor"),
        P("dp", "tensor"),
        P("tensor", "dp"),
        P("tensor", "dp"),
        P("tensor", "dp"),
        P("dp"),
        P("dp"),
        P("dp"),
    )
    out_specs = (
        P(("dp", "tensor"), None),
        P("dp", None),
        P(None, "dp", "tensor"),
        P(None, "dp", "tensor"),
        P(None, "dp", "tensor"),
        P(None, "dp", "tensor"),
        P("tensor", "dp"),
        P("tensor", "dp"),
        P("tensor", "dp"),
        P("tensor", "dp"),
        P("dp", "tensor"),
        P("dp", "tensor"),
        P("dp", "tensor"),
        P("dp", "tensor"),
        P("tensor", "dp"),
        P("tensor", "dp"),
        P("tensor", "dp"),
        P("tensor", "dp"),
        P("dp"),
        P("dp"),
        P("dp"),
        P("dp"),
        P(),
    )
    return jax.shard_map(local, mesh=mesh, in_specs=in_specs, out_specs=out_specs, check_vma=False)
```

```python
import functools

import jax
import jax.numpy as jnp
from jax import lax
from jax.experimental import pallas as pl
from jax.experimental.pallas import tpu as pltpu
from jax.sharding import PartitionSpec as P

MESH = pl.DeviceIdType.MESH
PAIR = 2

HEAD_DIM = 64
SEQ = 196
STEP = 5


norm_eps = 1e-06
beta_one = 0.5
beta_two = 0.5
lamb_eps = 1e-06
weight_decay = 0.01
learn_rate = 0.5


def lamb_parts(master, first, second, grad):
    moment = beta_one * first + (1.0 - beta_one) * grad
    square = beta_two * second + (1.0 - beta_two) * grad * grad
    update = (
        moment / (1.0 - beta_one**STEP) / (jnp.sqrt(square / (1.0 - beta_two**STEP)) + lamb_eps)
        + weight_decay * master
    )
    return (moment, square, update)


def greet(place, line, up, down, other):
    barrier = pltpu.get_barrier_semaphore()
    pl.semaphore_signal(barrier, inc=1, device_id=other, device_id_type=MESH)

    @pl.when(place < line - 1)
    def _():
        pl.semaphore_signal(barrier, inc=1, device_id=up, device_id_type=MESH)

    @pl.when(place > 0)
    def _():
        pl.semaphore_signal(barrier, inc=1, device_id=down, device_id_type=MESH)

    pl.semaphore_wait(barrier, 1 + jnp.minimum(place, 1) + jnp.minimum(line - 1 - place, 1))


def gather_kernel(line, own_ref, all_ref, own_sem, up_sem, down_sem, pair_sem, recv_sem):
    me = lax.axis_index("dp")
    place, side = me // PAIR, me % PAIR
    up, down, other = {"dp": me + PAIR}, {"dp": me - PAIR}, {"dp": me + 1 - 2 * side}
    has_up, has_down = place < line - 1, place > 0
    greet(place, line, up, down, other)

    def move(step, source, block, sems, peer):
        return pltpu.make_async_remote_copy(
            src_ref=source,
            dst_ref=all_ref.at[block],
            send_sem=sems.at[step],
            recv_sem=recv_sem.at[block],
            device_id=peer,
            device_id_type=MESH,
        )

    def held(block):
        return all_ref.at[block]

    def arrived(block, peer):
        move(0, held(block), block, pair_sem, peer).wait_recv()

    own = pltpu.make_async_copy(own_ref, all_ref.at[me], own_sem)

    @pl.when(has_up)
    def _():
        move(place, own_ref, me, up_sem, up).start()

    @pl.when(has_down)
    def _():
        move(place, own_ref, me, down_sem, down).start()

    move(place, own_ref, me, pair_sem, other).start()
    own.start()

    @pl.loop(1, line)
    def _(step):
        low, high = place - step, place + step

        @pl.when(low >= 0)
        def _():
            block = low * PAIR + side
            arrived(block, other)

            @pl.when(has_up)
            def _():
                move(low, held(block), block, up_sem, up).start()

            move(low, held(block), block, pair_sem, other).start()

        @pl.when(high < line)
        def _():
            block = high * PAIR + side
            arrived(block, other)

            @pl.when(has_down)
            def _():
                move(high, held(block), block, down_sem, down).start()

            move(high, held(block), block, pair_sem, other).start()

    own.wait()

    @pl.loop(0, line)
    def _(spot):
        block = spot * PAIR + side
        arrived(spot * PAIR + 1 - side, other)
        move(spot, held(block), block, pair_sem, other).wait_send()

        @pl.when(jnp.logical_and(has_up, spot <= place))
        def _():
            move(spot, held(block), block, up_sem, up).wait_send()

        @pl.when(jnp.logical_and(has_down, spot >= place))
        def _():
            move(spot, held(block), block, down_sem, down).wait_send()


def gather_blocks(own):
    rows, width = own.shape
    devices = lax.axis_size("dp")
    line = devices // PAIR
    return pl.pallas_call(
        functools.partial(gather_kernel, line),
        out_shape=jax.ShapeDtypeStruct((devices, rows, width), own.dtype),
        in_specs=[pl.BlockSpec(memory_space=pltpu.VMEM)],
        out_specs=pl.BlockSpec(memory_space=pl.ANY),
        scratch_shapes=[
            pltpu.SemaphoreType.DMA,
            pltpu.SemaphoreType.DMA((line,)),
            pltpu.SemaphoreType.DMA((line,)),
            pltpu.SemaphoreType.DMA((line,)),
            pltpu.SemaphoreType.DMA((devices,)),
        ],
        compiler_params=pltpu.CompilerParams(collective_id=0, has_side_effects=True),
        cost_estimate=pl.CostEstimate(flops=0, bytes_accessed=100_000_000, transcendentals=0),
        name="gather_blocks",
    )(own)


def reduce_kernel(
    line, own_ref, sum_ref, pair_in, up_in, down_in, up_out, down_out,
    pair_send, pair_recv, up_send, up_recv, down_send, down_recv,
):
    me = lax.axis_index("dp")
    place, side = me // PAIR, me % PAIR
    up, down, other = {"dp": me + PAIR}, {"dp": me - PAIR}, {"dp": me + 1 - 2 * side}
    has_up, has_down = place < line - 1, place > 0
    greet(place, line, up, down, other)

    def pair_move(spot):
        return pltpu.make_async_remote_copy(
            src_ref=own_ref.at[spot * PAIR + 1 - side],
            dst_ref=pair_in.at[spot],
            send_sem=pair_send.at[spot],
            recv_sem=pair_recv.at[spot],
            device_id=other,
            device_id_type=MESH,
        )

    def line_move(spot, source, target, sends, recvs, peer):
        return pltpu.make_async_remote_copy(
            src_ref=source.at[spot],
            dst_ref=target.at[spot],
            send_sem=sends.at[spot],
            recv_sem=recvs.at[spot],
            device_id=peer,
            device_id_type=MESH,
        )

    def up_move(spot):
        return line_move(spot, up_out, up_in, up_send, up_recv, up)

    def down_move(spot):
        return line_move(spot, down_out, down_in, down_send, down_recv, down)

    @pl.loop(0, line)
    def _(turn):
        far = line - 1 - turn

        @pl.when(place + far < line)
        def _():
            pair_move(place + far).start()

        @pl.when(jnp.logical_and(place - far >= 0, far > 0))
        def _():
            pair_move(place - far).start()

    def both(spot):
        return own_ref[spot * PAIR + side].astype(jnp.float32) + pair_in[spot].astype(jnp.float32)

    @pl.loop(0, line - 1)
    def _(turn):
        far = line - 1 - turn

        @pl.when(place + far < line)
        def _():
            spot = place + far
            pair_move(spot).wait_recv()

            @pl.when(has_down)
            def _():
                up_move(spot).wait_recv()
                up_out[spot] = (both(spot) + up_in[spot].astype(jnp.float32)).astype(jnp.bfloat16)

            @pl.when(jnp.logical_not(has_down))
            def _():
                up_out[spot] = both(spot).astype(jnp.bfloat16)

            up_move(spot).start()

        @pl.when(place - far >= 0)
        def _():
            spot = place - far
            pair_move(spot).wait_recv()

            @pl.when(has_up)
            def _():
                down_move(spot).wait_recv()
                down_out[spot] = (both(spot) + down_in[spot].astype(jnp.float32)).astype(
                    jnp.bfloat16
                )

            @pl.when(jnp.logical_not(has_up))
            def _():
                down_out[spot] = both(spot).astype(jnp.bfloat16)

            down_move(spot).start()

    pair_move(place).wait_recv()
    sum_ref[...] = both(place)

    @pl.when(has_down)
    def _():
        up_move(place).wait_recv()
        sum_ref[...] += up_in[place].astype(jnp.float32)

    @pl.when(has_up)
    def _():
        down_move(place).wait_recv()
        sum_ref[...] += down_in[place].astype(jnp.float32)

    @pl.loop(0, line)
    def _(spot):
        pair_move(spot).wait_send()

        @pl.when(spot > place)
        def _():
            up_move(spot).wait_send()

        @pl.when(spot < place)
        def _():
            down_move(spot).wait_send()


def reduce_blocks(own):
    devices, rows, width = own.shape
    line = devices // PAIR
    buffer = pltpu.VMEM((line, rows, width), own.dtype)
    return pl.pallas_call(
        functools.partial(reduce_kernel, line),
        out_shape=jax.ShapeDtypeStruct((rows, width), jnp.float32),
        in_specs=[pl.BlockSpec(memory_space=pltpu.VMEM)],
        out_specs=pl.BlockSpec(memory_space=pltpu.VMEM),
        scratch_shapes=[buffer] * 5 + [pltpu.SemaphoreType.DMA((line,))] * 6,
        compiler_params=pltpu.CompilerParams(
            collective_id=1, has_side_effects=True, vmem_limit_bytes=40 * 2**20
        ),
        cost_estimate=pl.CostEstimate(flops=0, bytes_accessed=100_000_000, transcendentals=0),
        name="reduce_blocks",
    )(own)


def total_kernel(
    devices, ranks, own_ref, sum_ref, rank_in, dp_out, dp_in,
    rank_send, rank_recv, dp_send, dp_recv,
):
    me, rank = lax.axis_index("dp"), lax.axis_index("tensor")
    barrier = pltpu.get_barrier_semaphore()
    for shift in range(1, ranks):
        peer = {"tensor": lax.rem(rank + shift, ranks)}
        pl.semaphore_signal(barrier, inc=1, device_id=peer, device_id_type=MESH)
    for shift in range(1, devices):
        peer = {"dp": lax.rem(me + shift, devices)}
        pl.semaphore_signal(barrier, inc=1, device_id=peer, device_id_type=MESH)
    pl.semaphore_wait(barrier, ranks - 1 + devices - 1)

    def rank_move(shift):
        return pltpu.make_async_remote_copy(
            src_ref=own_ref,
            dst_ref=rank_in.at[rank],
            send_sem=rank_send.at[shift],
            recv_sem=rank_recv.at[rank],
            device_id={"tensor": lax.rem(rank + shift, ranks)},
            device_id_type=MESH,
        )

    def rank_arrival(source):
        return pltpu.make_async_remote_copy(
            src_ref=own_ref,
            dst_ref=rank_in.at[source],
            send_sem=rank_send.at[0],
            recv_sem=rank_recv.at[source],
            device_id={"tensor": lax.rem(rank + 1, ranks)},
            device_id_type=MESH,
        )

    def dp_move(shift):
        return pltpu.make_async_remote_copy(
            src_ref=dp_out,
            dst_ref=dp_in.at[me],
            send_sem=dp_send.at[shift],
            recv_sem=dp_recv.at[me],
            device_id={"dp": lax.rem(me + shift, devices)},
            device_id_type=MESH,
        )

    def dp_arrival(source):
        return pltpu.make_async_remote_copy(
            src_ref=dp_out,
            dst_ref=dp_in.at[source],
            send_sem=dp_send.at[0],
            recv_sem=dp_recv.at[source],
            device_id={"dp": lax.rem(me + 1, devices)},
            device_id_type=MESH,
        )

    for shift in range(1, ranks):
        rank_move(shift).start()
    rank_in[rank] = own_ref[...]
    for shift in range(1, ranks):
        rank_arrival(lax.rem(rank + shift, ranks)).wait_recv()
    part = rank_in[0]
    for spot in range(1, ranks):
        part = part + rank_in[spot]
    dp_out[...] = part
    for shift in range(1, devices):
        dp_move(shift).start()
    dp_in[me] = part
    for shift in range(1, devices):
        dp_arrival(lax.rem(me + shift, devices)).wait_recv()
    whole = dp_in[0]
    for spot in range(1, devices):
        whole = whole + dp_in[spot]
    sum_ref[...] = whole
    for shift in range(1, ranks):
        rank_move(shift).wait_send()
    for shift in range(1, devices):
        dp_move(shift).wait_send()


def total_of(own, collective_id):
    devices, ranks = lax.axis_size("dp"), lax.axis_size("tensor")
    return pl.pallas_call(
        functools.partial(total_kernel, devices, ranks),
        out_shape=jax.ShapeDtypeStruct(own.shape, own.dtype),
        in_specs=[pl.BlockSpec(memory_space=pltpu.VMEM)],
        out_specs=pl.BlockSpec(memory_space=pltpu.VMEM),
        scratch_shapes=[
            pltpu.VMEM((ranks,) + own.shape, own.dtype),
            pltpu.VMEM(own.shape, own.dtype),
            pltpu.VMEM((devices,) + own.shape, own.dtype),
            pltpu.SemaphoreType.DMA((ranks,)),
            pltpu.SemaphoreType.DMA((ranks,)),
            pltpu.SemaphoreType.DMA((devices,)),
            pltpu.SemaphoreType.DMA((devices,)),
        ],
        compiler_params=pltpu.CompilerParams(
            collective_id=collective_id, has_side_effects=True, vmem_limit_bytes=60 * 2**20
        ),
        cost_estimate=pl.CostEstimate(flops=0, bytes_accessed=20_000_000, transcendentals=0),
        name="total_" + str(collective_id),
    )(own)


WINDOW = 224


def image_kernel(
    images, cuts, x_hbm, c_hbm, tail_ref, w_ref,
    out_ref, grad_in_ref, g_ref,
    acc1, acc2, gain_row, g_gain, windows, kept, qkv, back_cols, front_cols,
    partial, pair_in, chip_sum, line_in, total,
    in_sem, s1, r1, s2, r2, s3, r3,
):
    step = pl.program_id(0)
    rank = lax.axis_index("tensor")
    core, half_of_images = rank % 2, rank // 2
    sibling = {"tensor": rank + 1 - 2 * core}
    across = {"tensor": lax.rem(rank + 2, 4)}
    width, head_cols = cuts
    heads = head_cols // HEAD_DIM
    rows, model = kept.shape[2], kept.shape[3]
    half = model // 2
    f32, b16 = jnp.float32, jnp.bfloat16
    back_width, front_width = back_cols.shape[1], front_cols.shape[1]
    last_window = images * SEQ // 16 * 16 - WINDOW

    def image_at(turn):
        return turn // 2 + (turn % 2) * (images // 2 + 1)

    def window_start(image):
        return pl.multiple_of(jnp.minimum(image * SEQ // 16 * 16, last_window), 16)

    def fetches(image, slot):
        return [
            pltpu.make_async_copy(
                source.at[pl.ds(window_start(image), WINDOW)],
                windows.at[slot, kind, pl.ds(0, WINDOW)],
                in_sem.at[slot, kind],
            )
            for kind, source in ((0, x_hbm), (1, c_hbm))
        ]

    def one_hot(shape, row_is):
        at = [lax.broadcasted_iota(jnp.int32, shape, axis) for axis in (0, 1)]
        return jnp.where(row_is(*at), 1.0, 0.0).astype(b16)

    @pl.when(step == 0)
    def _():
        line_in[...] = jnp.zeros_like(line_in)
        barrier = pltpu.get_barrier_semaphore()
        pl.semaphore_signal(barrier, inc=1, device_id=sibling, device_id_type=MESH)
        pl.semaphore_signal(barrier, inc=1, device_id=across, device_id_type=MESH)
        pl.semaphore_wait(barrier, 2)
        for copy in fetches(0, 0):
            copy.start()
        for slot in range(2):
            for kind in range(2):
                windows[slot, kind, WINDOW:] = tail_ref[kind]
        total[...] = jnp.zeros_like(total)
        kept[...] = jnp.zeros_like(kept)
        acc1[...] = jnp.zeros_like(acc1)
        acc2[...] = jnp.zeros_like(acc2)
        back_cols[...] = jnp.zeros_like(back_cols)
        front_cols[...] = jnp.zeros_like(front_cols)
        g_gain[...] = jnp.zeros_like(g_gain)
        for ref in (out_ref, grad_in_ref):
            ref[:16] = jnp.zeros((16, model), b16)
        turned = w_ref[:, back_width + front_width - 128 :].astype(f32).T
        gain_row[...] = turned[127:128]

    @pl.when(step < images - 1)
    def _():
        for copy in fetches(image_at(step + 1), (step + 1) % 2):
            copy.start()

    def move(source, target, sends, recvs, slot, peer):
        return pltpu.make_async_remote_copy(
            src_ref=source,
            dst_ref=target,
            send_sem=sends.at[slot],
            recv_sem=recvs.at[slot],
            device_id=peer,
            device_id_type=MESH,
        )

    def first(slot):
        return move(partial.at[slot, 1 - core], pair_in.at[slot], s1, r1, slot, sibling)

    def second(slot, kind):
        return pltpu.make_async_remote_copy(
            src_ref=chip_sum.at[slot, kind],
            dst_ref=line_in.at[slot, kind],
            send_sem=s2.at[slot, kind],
            recv_sem=r2.at[slot, kind],
            device_id=across,
            device_id_type=MESH,
        )

    def gives_output(turn):
        return jnp.logical_or(turn % 2 != half_of_images, turn == images - 1)

    def takes_output(turn):
        return jnp.logical_or(turn % 2 == half_of_images, turn == images - 1)

    def third(slot):
        return move(total.at[slot, core], total.at[slot, core], s3, r3, slot, sibling)

    def normalised(values):
        floats = values.astype(f32)
        centred = floats - jnp.mean(floats, axis=1, keepdims=True)
        inv_std = lax.rsqrt(jnp.mean(centred * centred, axis=1, keepdims=True) + norm_eps)
        return floats, centred * inv_std, inv_std

    gain = gain_row[...]

    image = image_at(jnp.maximum(step - 3, 0))

    def place(ref, values):
        start = pl.multiple_of(image * SEQ // 16 * 16, 16)
        offset = image * SEQ - start
        spread = one_hot((WINDOW, rows), lambda r, j: jnp.logical_and(r == j + offset, j < SEQ))
        placed = jnp.dot(spread, values, preferred_element_type=f32)
        before = lax.broadcasted_iota(jnp.int32, (16, model), 0) < offset
        head = jnp.where(before, ref[pl.ds(start, 16), :].astype(f32), placed[:16])
        ref[pl.ds(start, 16), :] = head.astype(b16)
        ref[pl.ds(start + 16, WINDOW - 16), :] = placed[16:].astype(b16)

    def place_late(ref, values):
        @pl.when(step < images + 1)
        def _():
            place(ref, values)

        for turn in (images - 2, images - 1):

            @pl.when(step == turn + 3)
            def _(at=image_at(turn) * SEQ):
                ref[at : at + SEQ] = values[:SEQ]

    @pl.when(step >= 3)
    def _():
        third((step - 3) % 3).wait()

    def finish(put):
        slot, spot = (step + 3) % 3, (step + 1) % 4
        floats, unit, inv_std = normalised(kept[spot, 0])
        sums = jnp.concatenate([total[slot, 0, 0], total[slot, 1, 0]], axis=1).astype(f32)
        put(out_ref, (floats + sums).astype(b16))
        d_normed = jnp.concatenate([total[slot, 0, 1], total[slot, 1, 1]], axis=1).astype(f32)
        weighted = d_normed * unit
        counted = jnp.sum(weighted, axis=0, keepdims=True)
        g_gain[...] += jnp.where(step >= 3, counted, 0.0)
        d_unit = d_normed * gain
        d_floats = inv_std * (
            d_unit
            - jnp.mean(d_unit, axis=1, keepdims=True)
            - unit * jnp.mean(weighted * gain, axis=1, keepdims=True)
        )
        put(grad_in_ref, (kept[spot, 1].astype(f32) + d_floats).astype(b16))

    @pl.when(jnp.logical_and(step >= 2, step < images + 2))
    def _():
        slot, spot = (step - 2) % 2, (step - 2) % 3
        second(slot, 1).wait()

        @pl.when(gives_output(step - 2))
        def _():
            second(slot, 0).wait_send()

        @pl.when(takes_output(step - 2))
        def _():
            second(slot, 0).wait_recv()

        total[spot, core] = (chip_sum[slot].astype(f32) + line_in[slot].astype(f32)).astype(b16)
        third(spot).start()

    @pl.when(jnp.logical_and(step >= 1, step < images + 1))
    def _():
        slot = (step - 1) % 2
        first(slot).wait()
        chip_sum[slot] = (partial[slot, core].astype(f32) + pair_in[slot].astype(f32)).astype(b16)
        second(slot, 1).start()

        @pl.when(gives_output(step - 1))
        def _():
            second(slot, 0).start()

    @pl.when(step < images)
    def _():
        slot = step % 2
        for copy in fetches(image_at(step), slot):
            copy.wait()
        offset = image_at(step) * SEQ - window_start(image_at(step))
        pick = one_hot(
            (rows, windows.shape[2]), lambda r, j: jnp.logical_and(j == r + offset, r < SEQ)
        )
        for kind in range(2):
            kept[step % 4, kind] = jnp.dot(
                pick, windows[slot, kind], preferred_element_type=f32
            ).astype(b16)
        _floats, unit, _inv = normalised(kept[step % 4, 0])
        normed = (unit * gain).astype(b16)
        cot = kept[step % 4, 1]

        def mm(a, b):
            return jnp.dot(a, b, preferred_element_type=f32)

        def mm_nt(a, b):
            return lax.dot_general(a, b, (((1,), (1,)), ((), ())), preferred_element_type=f32)

        def mm_tn(a, b):
            return lax.dot_general(a, b, (((0,), (0,)), ((), ())), preferred_element_type=f32)

        qkv[:, : 3 * head_cols] = mm(normed, w_ref[:, width:back_width])[:, : 3 * head_cols].astype(b16)
        qkv[:, 3 * head_cols :] = mm(cot, w_ref[:, back_width + width :])[:, :head_cols].astype(b16)
        keys_wide = pl.cdiv(rows, 128) * 128
        filler = jnp.zeros((keys_wide - rows, HEAD_DIM), b16)
        real = lax.broadcasted_iota(jnp.int32, (rows, keys_wide), 1) < SEQ
        for head in range(heads):
            def part(kind):
                at = kind * head_cols + head * HEAD_DIM
                return qkv[:, at : at + HEAD_DIM]

            query = part(0) * jnp.asarray(HEAD_DIM ** (-0.5), b16)
            key = jnp.concatenate([part(1), filler], axis=0)
            value = jnp.concatenate([part(2), filler], axis=0)
            d_att = part(3)
            scores = jnp.where(real, mm_nt(query, key), -1e30)
            powers = jnp.exp(scores - jnp.max(scores, axis=1, keepdims=True))
            probs = powers * (1.0 / jnp.sum(powers, axis=1, keepdims=True))
            probs_low = probs.astype(b16)
            spot = head * HEAD_DIM
            front_cols[:, width + spot : width + spot + HEAD_DIM] = mm(probs_low, value).astype(b16)
            d_probs = mm_nt(d_att, value)
            d_value = mm_tn(probs_low, d_att)[:rows].astype(b16)
            inner = jnp.sum(probs * d_probs, axis=1, keepdims=True)
            d_scores = (probs * (d_probs - inner)).astype(b16)
            d_query = (mm(d_scores, key) * (HEAD_DIM ** (-0.5))).astype(b16)
            d_key = mm_tn(d_scores, query)[:rows].astype(b16)
            for kind, value_of in ((0, d_query), (1, d_key), (2, d_value)):
                at = width + kind * head_cols + spot
                back_cols[:, at : at + HEAD_DIM] = value_of

        upper = mm(normed, w_ref[:, :width])
        d_hidden = mm(cot, w_ref[:, back_width : back_width + width])
        scale = (2.0 / 3.141592653589793) ** 0.5
        square = upper * upper
        bend = jnp.tanh(scale * upper * (1.0 + 0.044715 * square))
        step_up = 0.5 * (1.0 + bend)
        front_cols[:, :width] = (upper * step_up).astype(b16)
        slope = step_up + (0.5 * scale) * upper * (1.0 - bend * bend) * (
            1.0 + (3.0 * 0.044715) * square
        )
        back_cols[:, :width] = (d_hidden * slope).astype(b16)

        finish(place)
        out_part = mm_nt(front_cols[...], w_ref[:, back_width:]).astype(b16)
        partial[slot, 0, 0] = out_part[:, :half]
        partial[slot, 1, 0] = out_part[:, half:]
        back_part = mm_nt(back_cols[...], w_ref[:, :back_width]).astype(b16)
        partial[slot, 0, 1] = back_part[:, :half]
        partial[slot, 1, 1] = back_part[:, half:]
        first(slot).start()
        acc1[...] += mm_tn(normed, back_cols[...])
        acc2[...] += mm_tn(cot, front_cols[...])

    @pl.when(step >= images)
    def _():
        finish(place_late)

    @pl.when(step == images + 2)
    def _():
        g_ref[:, :back_width] = acc1[...].astype(b16)
        inner = back_width + front_width - 128
        g_ref[:, back_width:inner] = acc2[:, : front_width - 128].astype(b16)
        spare = jnp.broadcast_to(g_gain[...], (128, model)).T
        last = lax.broadcasted_iota(jnp.int32, (model, 128), 1) == 127
        g_ref[:, inner:] = jnp.where(last, spare, acc2[:, front_width - 128 :]).astype(b16)


def image_block(inputs, cotangent, tails, weights, width, head_cols, back_width):
    tokens, model = inputs.shape
    images = tokens // SEQ
    rows = -(-SEQ // 16) * 16
    half = model // 2
    front_width = weights.shape[1] - back_width
    fixed = lambda i: (0, 0)

    def whole(shape):
        return pl.BlockSpec(shape, fixed, pipeline_mode=pl.Buffered(1))

    bf = jnp.bfloat16
    anywhere = pl.BlockSpec(memory_space=pl.ANY)
    return pl.pallas_call(
        functools.partial(image_kernel, images, (width, head_cols)),
        grid=(images + 3,),
        out_shape=(
            jax.ShapeDtypeStruct(inputs.shape, bf),
            jax.ShapeDtypeStruct(inputs.shape, bf),
            jax.ShapeDtypeStruct(weights.shape, bf),
        ),
        in_specs=[
            anywhere,
            anywhere,
            pl.BlockSpec(tails.shape, lambda i: (0, 0, 0), pipeline_mode=pl.Buffered(1)),
            whole(weights.shape),
        ],
        out_specs=[whole(inputs.shape), whole(inputs.shape), whole(weights.shape)],
        scratch_shapes=[
            pltpu.VMEM((model, back_width), jnp.float32),
            pltpu.VMEM((model, front_width), jnp.float32),
            pltpu.VMEM((1, model), jnp.float32),
            pltpu.VMEM((1, model), jnp.float32),
            pltpu.VMEM((2, 2, WINDOW + tails.shape[1], model), bf),
            pltpu.VMEM((4, 2, rows, model), bf),
            pltpu.VMEM((rows, 4 * head_cols), bf),
            pltpu.VMEM((rows, back_width), bf),
            pltpu.VMEM((rows, front_width), bf),
            pltpu.VMEM((2, 2, 2, rows, half), bf),
            pltpu.VMEM((2, 2, rows, half), bf),
            pltpu.VMEM((2, 2, rows, half), bf),
            pltpu.VMEM((2, 2, rows, half), bf),
            pltpu.VMEM((3, 2, 2, rows, half), bf),
            pltpu.SemaphoreType.DMA((2, 2)),
        ]
        + [pltpu.SemaphoreType.DMA((2,))] * 2
        + [pltpu.SemaphoreType.DMA((2, 2))] * 2
        + [pltpu.SemaphoreType.DMA((3,))] * 2,
        compiler_params=pltpu.CompilerParams(
            collective_id=4,
            has_side_effects=True,
            vmem_limit_bytes=60 * 2**20,
            dimension_semantics=("arbitrary",),
        ),
        name="image_block",
    )(inputs, cotangent, tails, weights)


def parts_kernel(cuts, replicas, summed_ref, *refs):
    states, outs, sums_ref = refs[:15], refs[15:30], refs[30]
    hidden_here, head_cols, back_width, used = cuts
    width = summed_ref.shape[1]
    row = lax.broadcasted_iota(jnp.int32, sums_ref.shape, 0)
    lane = lax.broadcasted_iota(jnp.int32, sums_ref.shape, 1)
    sums = jnp.zeros(sums_ref.shape, jnp.float32)

    def square_sum(values):
        return jnp.sum(jnp.sum(values * values, axis=1, keepdims=True), axis=0, keepdims=True)

    def one(index, grad, at=None):
        master, first, second = (
            ref[...] if at is None else ref[at] for ref in states[3 * index : 3 * index + 3]
        )
        results = lamb_parts(master, first, second, grad)
        for ref, value in zip(outs[3 * index : 3 * index + 3], results):
            if at is None:
                ref[...] = value
            else:
                ref[at] = value
        return square_sum(master), square_sum(results[2])

    def add(total, index, pair, scale=1.0):
        for column in range(2):
            here = jnp.logical_and(row == index, lane == column)
            total = total + jnp.where(here, pair[column] * scale, 0.0)
        return total

    for kind in range(3):
        at = hidden_here + kind * head_cols
        sums = add(sums, 0, one(0, summed_ref[:, at : at + head_cols], kind))
    outward_at = back_width + hidden_here
    sums = add(sums, 1, one(1, summed_ref[:, outward_at:used].T))
    sums = add(sums, 2, one(2, summed_ref[:, :hidden_here]))
    sums = add(sums, 3, one(3, summed_ref[:, back_width:outward_at]))
    gain = summed_ref[:, width - 128 :].T
    sums = add(sums, 4, one(4, gain[127:128]), replicas)
    sums_ref[...] = sums


def fresh_kernel(sums_ref, *refs):
    masters, updates, fresh, low = refs[:5], refs[5:10], refs[10:15], refs[15:20]
    for index in range(5):
        norms = jnp.sqrt(sums_ref[index : index + 1, :])
        rate = learn_rate * (norms[:, 0:1] / norms[:, 1:2])
        if len(masters[index].shape) == 3:
            rate = rate.reshape(1, 1, 1)
        value = masters[index][...] - rate * updates[index][...]
        fresh[index][...] = value
        low[index][...] = value.astype(jnp.bfloat16)


def lamb_step(summed, states, cuts):
    def blocks(arrays):
        return [pl.BlockSpec(a.shape, lambda i, n=a.ndim: (0,) * n) for a in arrays]

    one_step = {"grid": (1,), "compiler_params": pltpu.CompilerParams(vmem_limit_bytes=60 * 2**20)}
    flat = [array for group in states for array in group]
    like = [jax.ShapeDtypeStruct(array.shape, jnp.float32) for array in flat]
    like.append(jax.ShapeDtypeStruct((8, 128), jnp.float32))
    *parts, sums = pl.pallas_call(
        functools.partial(parts_kernel, cuts, 1.0 / lax.axis_size("tensor")),
        out_shape=like,
        in_specs=blocks([summed, *flat]),
        out_specs=blocks(like),
        name="lamb_parts",
        **one_step,
    )(summed, *flat)
    sums = total_of(sums, 3)
    masters = [group[0] for group in states]
    made = [jax.ShapeDtypeStruct(m.shape, t) for t in (jnp.float32, jnp.bfloat16) for m in masters]
    fresh = pl.pallas_call(
        fresh_kernel,
        out_shape=made,
        in_specs=blocks([sums, *masters, *masters]),
        out_specs=blocks(made),
        name="lamb_fresh",
        **one_step,
    )(sums, *masters, *parts[2::3])
    return parts, fresh, jnp.sqrt(sums[:5, :2])


def local(
    inputs,
    cotangent,
    master_inward,
    first_inward,
    second_inward,
    master_outward,
    first_outward,
    second_outward,
    master_widening,
    first_widening,
    second_widening,
    master_narrowing,
    first_narrowing,
    second_narrowing,
    master_scaling,
    first_scaling,
    second_scaling,
):
    depth = master_widening.shape[0]
    hidden_here = master_widening.shape[1]
    head_cols = master_inward.shape[2]
    model = inputs.shape[1]
    back_width = hidden_here + 3 * head_cols
    gap = (-back_width) % 128
    back_width += gap
    used = back_width + hidden_here + head_cols
    width = -(-(used + 1) // 128) * 128
    shard = jnp.concatenate(
        [
            master_widening,
            jnp.transpose(master_inward, (1, 0, 2)).reshape(depth, 3 * head_cols),
            jnp.zeros((depth, gap), jnp.float32),
            master_narrowing.T,
            master_outward.T,
            jnp.broadcast_to(master_scaling[:, None], (depth, width - used)),
        ],
        axis=1,
    ).astype(jnp.bfloat16)
    copies = gather_blocks(shard).reshape(model, width)
    rows_here = inputs.shape[0]
    whole_rows = rows_here // 16 * 16
    tails = jnp.stack(
        [
            jnp.pad(rows[whole_rows:], ((0, whole_rows + 16 - rows_here), (0, 0)))
            for rows in (inputs, cotangent)
        ]
    )
    summed_out, input_grad, grads = image_block(
        inputs, cotangent, tails, copies, hidden_here, head_cols, back_width
    )
    share = rows_here // lax.axis_size("tensor")
    start = lax.axis_index("tensor") * share
    output = lax.dynamic_slice_in_dim(summed_out, start, share, 0)
    summed = reduce_blocks(grads.reshape(lax.axis_size("dp"), depth, width))
    states = (
        (master_inward, first_inward, second_inward),
        (master_outward, first_outward, second_outward),
        (master_widening, first_widening, second_widening),
        (master_narrowing.T, first_narrowing.T, second_narrowing.T),
        tuple(v.reshape(1, depth) for v in (master_scaling, first_scaling, second_scaling)),
    )
    parts, fresh, trust_norms = lamb_step(
        summed, states, (hidden_here, head_cols, back_width, used)
    )
    results = []
    for index in range(5):
        group = (parts[3 * index], parts[3 * index + 1], fresh[index], fresh[5 + index])
        if index == 3:
            group = [v.T for v in group]
        if index == 4:
            group = [v.reshape(depth) for v in group]
        results += group
    return (output, input_grad, *results, trust_norms)


def solution(mesh):
    in_specs = (
        P("dp", None),
        P("dp", None),
        P(None, "dp", "tensor"),
        P(None, "dp", "tensor"),
        P(None, "dp", "tensor"),
        P("tensor", "dp"),
        P("tensor", "dp"),
        P("tensor", "dp"),
        P("dp", "tensor"),
        P("dp", "tensor"),
        P("dp", "tensor"),
        P("tensor", "dp"),
        P("tensor", "dp"),
        P("tensor", "dp"),
        P("dp"),
        P("dp"),
        P("dp"),
    )
    out_specs = (
        P(("dp", "tensor"), None),
        P("dp", None),
        P(None, "dp", "tensor"),
        P(None, "dp", "tensor"),
        P(None, "dp", "tensor"),
        P(None, "dp", "tensor"),
        P("tensor", "dp"),
        P("tensor", "dp"),
        P("tensor", "dp"),
        P("tensor", "dp"),
        P("dp", "tensor"),
        P("dp", "tensor"),
        P("dp", "tensor"),
        P("dp", "tensor"),
        P("tensor", "dp"),
        P("tensor", "dp"),
        P("tensor", "dp"),
        P("tensor", "dp"),
        P("dp"),
        P("dp"),
        P("dp"),
        P("dp"),
        P(),
    )
    return jax.shard_map(local, mesh=mesh, in_specs=in_specs, out_specs=out_specs, check_vma=False)
```

```python
import functools

import jax
import jax.numpy as jnp
from jax import lax
from jax.experimental import pallas as pl
from jax.experimental.pallas import tpu as pltpu
from jax.sharding import PartitionSpec as P

MESH = pl.DeviceIdType.MESH
PAIR = 2

HEAD_DIM = 64
SEQ = 196
STEP = 5


norm_eps = 1e-06
beta_one = 0.5
beta_two = 0.5
lamb_eps = 1e-06
weight_decay = 0.01
learn_rate = 0.5


def lamb_parts(master, first, second, grad):
    moment = beta_one * first + (1.0 - beta_one) * grad
    square = beta_two * second + (1.0 - beta_two) * grad * grad
    update = (
        moment / (1.0 - beta_one**STEP) / (jnp.sqrt(square / (1.0 - beta_two**STEP)) + lamb_eps)
        + weight_decay * master
    )
    return (moment, square, update)


def greet(place, line, up, down, other):
    barrier = pltpu.get_barrier_semaphore()
    pl.semaphore_signal(barrier, inc=1, device_id=other, device_id_type=MESH)

    @pl.when(place < line - 1)
    def _():
        pl.semaphore_signal(barrier, inc=1, device_id=up, device_id_type=MESH)

    @pl.when(place > 0)
    def _():
        pl.semaphore_signal(barrier, inc=1, device_id=down, device_id_type=MESH)

    pl.semaphore_wait(barrier, 1 + jnp.minimum(place, 1) + jnp.minimum(line - 1 - place, 1))


def gather_kernel(
    line, cuts, wide_ref, inward_ref, narrow_ref, outward_ref, scaling_ref, all_ref,
    own_ref, own_sem, up_sem, down_sem, pair_sem, recv_sem,
):
    hidden_here, head_cols, back_width, used = cuts
    depth, width = own_ref.shape
    b16 = jnp.bfloat16
    own_ref[:, :hidden_here] = wide_ref[...].astype(b16)
    for kind in range(3):
        at = hidden_here + kind * head_cols
        own_ref[:, at : at + head_cols] = inward_ref[kind].astype(b16)
    at = hidden_here + 3 * head_cols
    own_ref[:, at:back_width] = jnp.zeros((depth, back_width - at), b16)
    own_ref[:, back_width : back_width + hidden_here] = narrow_ref[...].astype(b16)
    own_ref[:, back_width + hidden_here : used] = outward_ref[...].T.astype(b16)
    gain = jnp.broadcast_to(scaling_ref[...], (128, depth)).T
    own_ref[:, used:] = gain[:, : width - used].astype(b16)
    me = lax.axis_index("dp")
    place, side = me // PAIR, me % PAIR
    up, down, other = {"dp": me + PAIR}, {"dp": me - PAIR}, {"dp": me + 1 - 2 * side}
    has_up, has_down = place < line - 1, place > 0
    greet(place, line, up, down, other)

    def move(step, source, block, sems, peer):
        return pltpu.make_async_remote_copy(
            src_ref=source,
            dst_ref=all_ref.at[block],
            send_sem=sems.at[step],
            recv_sem=recv_sem.at[block],
            device_id=peer,
            device_id_type=MESH,
        )

    def held(block):
        return all_ref.at[block]

    def arrived(block, peer):
        move(0, held(block), block, pair_sem, peer).wait_recv()

    own = pltpu.make_async_copy(own_ref, all_ref.at[me], own_sem)

    @pl.when(has_up)
    def _():
        move(place, own_ref, me, up_sem, up).start()

    @pl.when(has_down)
    def _():
        move(place, own_ref, me, down_sem, down).start()

    move(place, own_ref, me, pair_sem, other).start()
    own.start()

    @pl.loop(1, line)
    def _(step):
        low, high = place - step, place + step

        @pl.when(low >= 0)
        def _():
            block = low * PAIR + side
            arrived(block, other)

            @pl.when(has_up)
            def _():
                move(low, held(block), block, up_sem, up).start()

            move(low, held(block), block, pair_sem, other).start()

        @pl.when(high < line)
        def _():
            block = high * PAIR + side
            arrived(block, other)

            @pl.when(has_down)
            def _():
                move(high, held(block), block, down_sem, down).start()

            move(high, held(block), block, pair_sem, other).start()

    own.wait()

    @pl.loop(0, line)
    def _(spot):
        block = spot * PAIR + side
        arrived(spot * PAIR + 1 - side, other)
        move(spot, held(block), block, pair_sem, other).wait_send()

        @pl.when(jnp.logical_and(has_up, spot <= place))
        def _():
            move(spot, held(block), block, up_sem, up).wait_send()

        @pl.when(jnp.logical_and(has_down, spot >= place))
        def _():
            move(spot, held(block), block, down_sem, down).wait_send()


def gather_blocks(masters, cuts, width):
    depth = masters[0].shape[0]
    devices = lax.axis_size("dp")
    line = devices // PAIR
    return pl.pallas_call(
        functools.partial(gather_kernel, line, cuts),
        out_shape=jax.ShapeDtypeStruct((devices, depth, width), jnp.bfloat16),
        in_specs=[pl.BlockSpec(memory_space=pltpu.VMEM)] * 5,
        out_specs=pl.BlockSpec(memory_space=pl.ANY),
        scratch_shapes=[
            pltpu.VMEM((depth, width), jnp.bfloat16),
            pltpu.SemaphoreType.DMA,
            pltpu.SemaphoreType.DMA((line,)),
            pltpu.SemaphoreType.DMA((line,)),
            pltpu.SemaphoreType.DMA((line,)),
            pltpu.SemaphoreType.DMA((devices,)),
        ],
        compiler_params=pltpu.CompilerParams(
            collective_id=0, has_side_effects=True, vmem_limit_bytes=60 * 2**20
        ),
        cost_estimate=pl.CostEstimate(flops=0, bytes_accessed=100_000_000, transcendentals=0),
        name="gather_blocks",
    )(*masters)


def reduce_kernel(
    line, own_ref, sum_ref, pair_in, up_in, down_in, up_out, down_out,
    pair_send, pair_recv, up_send, up_recv, down_send, down_recv,
):
    me = lax.axis_index("dp")
    place, side = me // PAIR, me % PAIR
    up, down, other = {"dp": me + PAIR}, {"dp": me - PAIR}, {"dp": me + 1 - 2 * side}
    has_up, has_down = place < line - 1, place > 0
    greet(place, line, up, down, other)

    def pair_move(spot):
        return pltpu.make_async_remote_copy(
            src_ref=own_ref.at[spot * PAIR + 1 - side],
            dst_ref=pair_in.at[spot],
            send_sem=pair_send.at[spot],
            recv_sem=pair_recv.at[spot],
            device_id=other,
            device_id_type=MESH,
        )

    def line_move(spot, source, target, sends, recvs, peer):
        return pltpu.make_async_remote_copy(
            src_ref=source.at[spot],
            dst_ref=target.at[spot],
            send_sem=sends.at[spot],
            recv_sem=recvs.at[spot],
            device_id=peer,
            device_id_type=MESH,
        )

    def up_move(spot):
        return line_move(spot, up_out, up_in, up_send, up_recv, up)

    def down_move(spot):
        return line_move(spot, down_out, down_in, down_send, down_recv, down)

    @pl.loop(0, line)
    def _(turn):
        far = line - 1 - turn

        @pl.when(place + far < line)
        def _():
            pair_move(place + far).start()

        @pl.when(jnp.logical_and(place - far >= 0, far > 0))
        def _():
            pair_move(place - far).start()

    def both(spot):
        return own_ref[spot * PAIR + side].astype(jnp.float32) + pair_in[spot].astype(jnp.float32)

    @pl.loop(0, line - 1)
    def _(turn):
        far = line - 1 - turn

        @pl.when(place + far < line)
        def _():
            spot = place + far
            pair_move(spot).wait_recv()

            @pl.when(has_down)
            def _():
                up_move(spot).wait_recv()
                up_out[spot] = (both(spot) + up_in[spot].astype(jnp.float32)).astype(jnp.bfloat16)

            @pl.when(jnp.logical_not(has_down))
            def _():
                up_out[spot] = both(spot).astype(jnp.bfloat16)

            up_move(spot).start()

        @pl.when(place - far >= 0)
        def _():
            spot = place - far
            pair_move(spot).wait_recv()

            @pl.when(has_up)
            def _():
                down_move(spot).wait_recv()
                down_out[spot] = (both(spot) + down_in[spot].astype(jnp.float32)).astype(
                    jnp.bfloat16
                )

            @pl.when(jnp.logical_not(has_up))
            def _():
                down_out[spot] = both(spot).astype(jnp.bfloat16)

            down_move(spot).start()

    pair_move(place).wait_recv()
    sum_ref[...] = both(place)

    @pl.when(has_down)
    def _():
        up_move(place).wait_recv()
        sum_ref[...] += up_in[place].astype(jnp.float32)

    @pl.when(has_up)
    def _():
        down_move(place).wait_recv()
        sum_ref[...] += down_in[place].astype(jnp.float32)

    @pl.loop(0, line)
    def _(spot):
        pair_move(spot).wait_send()

        @pl.when(spot > place)
        def _():
            up_move(spot).wait_send()

        @pl.when(spot < place)
        def _():
            down_move(spot).wait_send()


def reduce_blocks(own):
    devices, rows, width = own.shape
    line = devices // PAIR
    buffer = pltpu.VMEM((line, rows, width), own.dtype)
    return pl.pallas_call(
        functools.partial(reduce_kernel, line),
        out_shape=jax.ShapeDtypeStruct((rows, width), jnp.float32),
        in_specs=[pl.BlockSpec(memory_space=pltpu.VMEM)],
        out_specs=pl.BlockSpec(memory_space=pltpu.VMEM),
        scratch_shapes=[buffer] * 5 + [pltpu.SemaphoreType.DMA((line,))] * 6,
        compiler_params=pltpu.CompilerParams(
            collective_id=1, has_side_effects=True, vmem_limit_bytes=40 * 2**20
        ),
        cost_estimate=pl.CostEstimate(flops=0, bytes_accessed=100_000_000, transcendentals=0),
        name="reduce_blocks",
    )(own)


def total_kernel(
    devices, ranks, own_ref, sum_ref, rank_in, dp_out, dp_in,
    rank_send, rank_recv, dp_send, dp_recv,
):
    me, rank = lax.axis_index("dp"), lax.axis_index("tensor")
    barrier = pltpu.get_barrier_semaphore()
    for shift in range(1, ranks):
        peer = {"tensor": lax.rem(rank + shift, ranks)}
        pl.semaphore_signal(barrier, inc=1, device_id=peer, device_id_type=MESH)
    for shift in range(1, devices):
        peer = {"dp": lax.rem(me + shift, devices)}
        pl.semaphore_signal(barrier, inc=1, device_id=peer, device_id_type=MESH)
    pl.semaphore_wait(barrier, ranks - 1 + devices - 1)

    def rank_move(shift):
        return pltpu.make_async_remote_copy(
            src_ref=own_ref,
            dst_ref=rank_in.at[rank],
            send_sem=rank_send.at[shift],
            recv_sem=rank_recv.at[rank],
            device_id={"tensor": lax.rem(rank + shift, ranks)},
            device_id_type=MESH,
        )

    def rank_arrival(source):
        return pltpu.make_async_remote_copy(
            src_ref=own_ref,
            dst_ref=rank_in.at[source],
            send_sem=rank_send.at[0],
            recv_sem=rank_recv.at[source],
            device_id={"tensor": lax.rem(rank + 1, ranks)},
            device_id_type=MESH,
        )

    def dp_move(shift):
        return pltpu.make_async_remote_copy(
            src_ref=dp_out,
            dst_ref=dp_in.at[me],
            send_sem=dp_send.at[shift],
            recv_sem=dp_recv.at[me],
            device_id={"dp": lax.rem(me + shift, devices)},
            device_id_type=MESH,
        )

    def dp_arrival(source):
        return pltpu.make_async_remote_copy(
            src_ref=dp_out,
            dst_ref=dp_in.at[source],
            send_sem=dp_send.at[0],
            recv_sem=dp_recv.at[source],
            device_id={"dp": lax.rem(me + 1, devices)},
            device_id_type=MESH,
        )

    for shift in range(1, ranks):
        rank_move(shift).start()
    rank_in[rank] = own_ref[...]
    for shift in range(1, ranks):
        rank_arrival(lax.rem(rank + shift, ranks)).wait_recv()
    part = rank_in[0]
    for spot in range(1, ranks):
        part = part + rank_in[spot]
    dp_out[...] = part
    for shift in range(1, devices):
        dp_move(shift).start()
    dp_in[me] = part
    for shift in range(1, devices):
        dp_arrival(lax.rem(me + shift, devices)).wait_recv()
    whole = dp_in[0]
    for spot in range(1, devices):
        whole = whole + dp_in[spot]
    sum_ref[...] = whole
    for shift in range(1, ranks):
        rank_move(shift).wait_send()
    for shift in range(1, devices):
        dp_move(shift).wait_send()


def total_of(own, collective_id):
    devices, ranks = lax.axis_size("dp"), lax.axis_size("tensor")
    return pl.pallas_call(
        functools.partial(total_kernel, devices, ranks),
        out_shape=jax.ShapeDtypeStruct(own.shape, own.dtype),
        in_specs=[pl.BlockSpec(memory_space=pltpu.VMEM)],
        out_specs=pl.BlockSpec(memory_space=pltpu.VMEM),
        scratch_shapes=[
            pltpu.VMEM((ranks,) + own.shape, own.dtype),
            pltpu.VMEM(own.shape, own.dtype),
            pltpu.VMEM((devices,) + own.shape, own.dtype),
            pltpu.SemaphoreType.DMA((ranks,)),
            pltpu.SemaphoreType.DMA((ranks,)),
            pltpu.SemaphoreType.DMA((devices,)),
            pltpu.SemaphoreType.DMA((devices,)),
        ],
        compiler_params=pltpu.CompilerParams(
            collective_id=collective_id, has_side_effects=True, vmem_limit_bytes=60 * 2**20
        ),
        cost_estimate=pl.CostEstimate(flops=0, bytes_accessed=20_000_000, transcendentals=0),
        name="total_" + str(collective_id),
    )(own)


WINDOW = 224


def image_kernel(
    images, cuts, x_hbm, c_hbm, tail_ref, w_ref,
    out_ref, grad_in_ref, g_ref,
    acc1, acc2, gain_row, g_gain, windows, kept, qkv, back_cols, front_cols,
    normed_pair, cot_pair,
    partial, pair_in, chip_sum, line_in, total,
    in_sem, s1, r1, s2, r2, s3, r3,
):
    step = pl.program_id(0)
    rank = lax.axis_index("tensor")
    core, half_of_images = rank % 2, rank // 2
    sibling = {"tensor": rank + 1 - 2 * core}
    across = {"tensor": lax.rem(rank + 2, 4)}
    width, head_cols = cuts
    heads = head_cols // HEAD_DIM
    rows, model = kept.shape[2], kept.shape[3]
    half = model // 2
    f32, b16 = jnp.float32, jnp.bfloat16
    back_width, front_width = back_cols.shape[1], front_cols.shape[1]
    last_window = images * SEQ // 16 * 16 - WINDOW

    def image_at(turn):
        return turn // 2 + (turn % 2) * (images // 2 + 1)

    def window_start(image):
        return pl.multiple_of(jnp.minimum(image * SEQ // 16 * 16, last_window), 16)

    def fetches(image, slot):
        return [
            pltpu.make_async_copy(
                source.at[pl.ds(window_start(image), WINDOW)],
                windows.at[slot, kind, pl.ds(0, WINDOW)],
                in_sem.at[slot, kind],
            )
            for kind, source in ((0, x_hbm), (1, c_hbm))
        ]

    def one_hot(shape, row_is):
        at = [lax.broadcasted_iota(jnp.int32, shape, axis) for axis in (0, 1)]
        return jnp.where(row_is(*at), 1.0, 0.0).astype(b16)

    @pl.when(step == 0)
    def _():
        line_in[...] = jnp.zeros_like(line_in)
        barrier = pltpu.get_barrier_semaphore()
        pl.semaphore_signal(barrier, inc=1, device_id=sibling, device_id_type=MESH)
        pl.semaphore_signal(barrier, inc=1, device_id=across, device_id_type=MESH)
        pl.semaphore_wait(barrier, 2)
        for copy in fetches(0, 0):
            copy.start()
        for slot in range(2):
            for kind in range(2):
                windows[slot, kind, WINDOW:] = tail_ref[kind]
        total[...] = jnp.zeros_like(total)
        kept[...] = jnp.zeros_like(kept)
        acc1[...] = jnp.zeros_like(acc1)
        acc2[...] = jnp.zeros_like(acc2)
        back_cols[...] = jnp.zeros_like(back_cols)
        front_cols[...] = jnp.zeros_like(front_cols)
        g_gain[...] = jnp.zeros_like(g_gain)
        for ref in (out_ref, grad_in_ref):
            ref[:16] = jnp.zeros((16, model), b16)
        turned = w_ref[:, back_width + front_width - 128 :].astype(f32).T
        gain_row[...] = turned[127:128]

    @pl.when(step < images - 1)
    def _():
        for copy in fetches(image_at(step + 1), (step + 1) % 2):
            copy.start()

    def move(source, target, sends, recvs, slot, peer):
        return pltpu.make_async_remote_copy(
            src_ref=source,
            dst_ref=target,
            send_sem=sends.at[slot],
            recv_sem=recvs.at[slot],
            device_id=peer,
            device_id_type=MESH,
        )

    def first(slot):
        return move(partial.at[slot, 1 - core], pair_in.at[slot], s1, r1, slot, sibling)

    def second(slot, kind):
        return pltpu.make_async_remote_copy(
            src_ref=chip_sum.at[slot, kind],
            dst_ref=line_in.at[slot, kind],
            send_sem=s2.at[slot, kind],
            recv_sem=r2.at[slot, kind],
            device_id=across,
            device_id_type=MESH,
        )

    def gives_output(turn):
        return jnp.logical_or(turn % 2 != half_of_images, turn == images - 1)

    def takes_output(turn):
        return jnp.logical_or(turn % 2 == half_of_images, turn == images - 1)

    def third(slot):
        return move(total.at[slot, core], total.at[slot, core], s3, r3, slot, sibling)

    def normalised(values):
        floats = values.astype(f32)
        centred = floats - jnp.mean(floats, axis=1, keepdims=True)
        inv_std = lax.rsqrt(jnp.mean(centred * centred, axis=1, keepdims=True) + norm_eps)
        return floats, centred * inv_std, inv_std

    gain = gain_row[...]

    image = image_at(jnp.maximum(step - 3, 0))

    def place(ref, values):
        start = pl.multiple_of(image * SEQ // 16 * 16, 16)
        offset = image * SEQ - start
        spread = one_hot((WINDOW, rows), lambda r, j: jnp.logical_and(r == j + offset, j < SEQ))
        placed = jnp.dot(spread, values, preferred_element_type=f32)
        before = lax.broadcasted_iota(jnp.int32, (16, model), 0) < offset
        head = jnp.where(before, ref[pl.ds(start, 16), :].astype(f32), placed[:16])
        ref[pl.ds(start, 16), :] = head.astype(b16)
        ref[pl.ds(start + 16, WINDOW - 16), :] = placed[16:].astype(b16)

    def place_late(ref, values):
        @pl.when(step < images + 1)
        def _():
            place(ref, values)

        for turn in (images - 2, images - 1):

            @pl.when(step == turn + 3)
            def _(at=image_at(turn) * SEQ):
                ref[at : at + SEQ] = values[:SEQ]

    @pl.when(step >= 3)
    def _():
        third((step - 3) % 3).wait()

    def finish(put):
        slot, spot = (step + 3) % 3, (step + 1) % 4
        floats, unit, inv_std = normalised(kept[spot, 0])
        sums = jnp.concatenate([total[slot, 0, 0], total[slot, 1, 0]], axis=1).astype(f32)
        put(out_ref, (floats + sums).astype(b16))
        d_normed = jnp.concatenate([total[slot, 0, 1], total[slot, 1, 1]], axis=1).astype(f32)
        weighted = d_normed * unit
        counted = jnp.sum(weighted, axis=0, keepdims=True)
        g_gain[...] += jnp.where(step >= 3, counted, 0.0)
        d_unit = d_normed * gain
        d_floats = inv_std * (
            d_unit
            - jnp.mean(d_unit, axis=1, keepdims=True)
            - unit * jnp.mean(weighted * gain, axis=1, keepdims=True)
        )
        put(grad_in_ref, (kept[spot, 1].astype(f32) + d_floats).astype(b16))

    @pl.when(jnp.logical_and(step >= 2, step < images + 2))
    def _():
        slot, spot = (step - 2) % 2, (step - 2) % 3
        second(slot, 1).wait()

        @pl.when(gives_output(step - 2))
        def _():
            second(slot, 0).wait_send()

        @pl.when(takes_output(step - 2))
        def _():
            second(slot, 0).wait_recv()

        total[spot, core] = (chip_sum[slot].astype(f32) + line_in[slot].astype(f32)).astype(b16)
        third(spot).start()

    @pl.when(jnp.logical_and(step >= 1, step < images + 1))
    def _():
        slot = (step - 1) % 2
        first(slot).wait()
        chip_sum[slot] = (partial[slot, core].astype(f32) + pair_in[slot].astype(f32)).astype(b16)
        second(slot, 1).start()

        @pl.when(gives_output(step - 1))
        def _():
            second(slot, 0).start()

    @pl.when(step < images)
    def _():
        slot = step % 2
        for copy in fetches(image_at(step), slot):
            copy.wait()
        offset = image_at(step) * SEQ - window_start(image_at(step))
        pick = one_hot(
            (rows, windows.shape[2]), lambda r, j: jnp.logical_and(j == r + offset, r < SEQ)
        )
        for kind in range(2):
            kept[step % 4, kind] = jnp.dot(
                pick, windows[slot, kind], preferred_element_type=f32
            ).astype(b16)
        _floats, unit, _inv = normalised(kept[step % 4, 0])
        normed = (unit * gain).astype(b16)
        cot = kept[step % 4, 1]
        here = pl.ds(pl.multiple_of(slot * rows, 16), rows)
        normed_pair[here, :] = normed
        cot_pair[here, :] = cot

        def mm(a, b):
            return jnp.dot(a, b, preferred_element_type=f32)

        def mm_nt(a, b):
            return lax.dot_general(a, b, (((1,), (1,)), ((), ())), preferred_element_type=f32)

        def mm_tn(a, b):
            return lax.dot_general(a, b, (((0,), (0,)), ((), ())), preferred_element_type=f32)

        qkv[:, : 3 * head_cols] = mm(normed, w_ref[:, width:back_width])[:, : 3 * head_cols].astype(b16)
        qkv[:, 3 * head_cols :] = mm(cot, w_ref[:, back_width + width :])[:, :head_cols].astype(b16)
        keys_wide = pl.cdiv(rows, 128) * 128
        filler = jnp.zeros((keys_wide - rows, HEAD_DIM), b16)
        real = lax.broadcasted_iota(jnp.int32, (rows, keys_wide), 1) < SEQ
        for head in range(heads):
            def part(kind):
                at = kind * head_cols + head * HEAD_DIM
                return qkv[:, at : at + HEAD_DIM]

            query = part(0) * jnp.asarray(HEAD_DIM ** (-0.5), b16)
            key = jnp.concatenate([part(1), filler], axis=0)
            value = jnp.concatenate([part(2), filler], axis=0)
            d_att = part(3)
            scores = jnp.where(real, mm_nt(query, key), -1e30)
            powers = jnp.exp(scores - jnp.max(scores, axis=1, keepdims=True))
            probs = powers * (1.0 / jnp.sum(powers, axis=1, keepdims=True))
            probs_low = probs.astype(b16)
            spot = head * HEAD_DIM
            front_cols[here, width + spot : width + spot + HEAD_DIM] = mm(probs_low, value).astype(b16)
            d_probs = mm_nt(d_att, value)
            d_value = mm_tn(probs_low, d_att)[:rows].astype(b16)
            inner = jnp.sum(probs * d_probs, axis=1, keepdims=True)
            d_scores = (probs * (d_probs - inner)).astype(b16)
            d_query = (mm(d_scores, key) * (HEAD_DIM ** (-0.5))).astype(b16)
            d_key = mm_tn(d_scores, query)[:rows].astype(b16)
            for kind, value_of in ((0, d_query), (1, d_key), (2, d_value)):
                at = width + kind * head_cols + spot
                back_cols[here, at : at + HEAD_DIM] = value_of

        upper = mm(normed, w_ref[:, :width])
        d_hidden = mm(cot, w_ref[:, back_width : back_width + width])
        scale = (2.0 / 3.141592653589793) ** 0.5
        square = upper * upper
        bend = jnp.tanh(scale * upper * (1.0 + 0.044715 * square))
        step_up = 0.5 * (1.0 + bend)
        front_cols[here, :width] = (upper * step_up).astype(b16)
        slope = step_up + (0.5 * scale) * upper * (1.0 - bend * bend) * (
            1.0 + (3.0 * 0.044715) * square
        )
        back_cols[here, :width] = (d_hidden * slope).astype(b16)

        finish(place)
        out_part = mm_nt(front_cols[here, :], w_ref[:, back_width:]).astype(b16)
        partial[slot, 0, 0] = out_part[:, :half]
        partial[slot, 1, 0] = out_part[:, half:]
        back_part = mm_nt(back_cols[here, :], w_ref[:, :back_width]).astype(b16)
        partial[slot, 0, 1] = back_part[:, :half]
        partial[slot, 1, 1] = back_part[:, half:]
        first(slot).start()

        @pl.when(slot == 1)
        def _():
            acc1[...] += mm_tn(normed_pair[...], back_cols[...])
            acc2[...] += mm_tn(cot_pair[...], front_cols[...])

        if images % 2:

            @pl.when(step == images - 1)
            def _():
                acc1[...] += mm_tn(normed_pair[:rows], back_cols[:rows])
                acc2[...] += mm_tn(cot_pair[:rows], front_cols[:rows])

    @pl.when(step >= images)
    def _():
        finish(place_late)

    @pl.when(step == images + 2)
    def _():
        g_ref[:, :back_width] = acc1[...].astype(b16)
        inner = back_width + front_width - 128
        g_ref[:, back_width:inner] = acc2[:, : front_width - 128].astype(b16)
        spare = jnp.broadcast_to(g_gain[...], (128, model)).T
        last = lax.broadcasted_iota(jnp.int32, (model, 128), 1) == 127
        g_ref[:, inner:] = jnp.where(last, spare, acc2[:, front_width - 128 :]).astype(b16)


def image_block(inputs, cotangent, tails, weights, width, head_cols, back_width):
    tokens, model = inputs.shape
    images = tokens // SEQ
    rows = -(-SEQ // 16) * 16
    half = model // 2
    front_width = weights.shape[1] - back_width
    fixed = lambda i: (0, 0)

    def whole(shape):
        return pl.BlockSpec(shape, fixed, pipeline_mode=pl.Buffered(1))

    bf = jnp.bfloat16
    anywhere = pl.BlockSpec(memory_space=pl.ANY)
    return pl.pallas_call(
        functools.partial(image_kernel, images, (width, head_cols)),
        grid=(images + 3,),
        out_shape=(
            jax.ShapeDtypeStruct(inputs.shape, bf),
            jax.ShapeDtypeStruct(inputs.shape, bf),
            jax.ShapeDtypeStruct(weights.shape, bf),
        ),
        in_specs=[
            anywhere,
            anywhere,
            pl.BlockSpec(tails.shape, lambda i: (0, 0, 0), pipeline_mode=pl.Buffered(1)),
            whole(weights.shape),
        ],
        out_specs=[whole(inputs.shape), whole(inputs.shape), whole(weights.shape)],
        scratch_shapes=[
            pltpu.VMEM((model, back_width), jnp.float32),
            pltpu.VMEM((model, front_width), jnp.float32),
            pltpu.VMEM((1, model), jnp.float32),
            pltpu.VMEM((1, model), jnp.float32),
            pltpu.VMEM((2, 2, WINDOW + tails.shape[1], model), bf),
            pltpu.VMEM((4, 2, rows, model), bf),
            pltpu.VMEM((rows, 4 * head_cols), bf),
            pltpu.VMEM((2 * rows, back_width), bf),
            pltpu.VMEM((2 * rows, front_width), bf),
            pltpu.VMEM((2 * rows, model), bf),
            pltpu.VMEM((2 * rows, model), bf),
            pltpu.VMEM((2, 2, 2, rows, half), bf),
            pltpu.VMEM((2, 2, rows, half), bf),
            pltpu.VMEM((2, 2, rows, half), bf),
            pltpu.VMEM((2, 2, rows, half), bf),
            pltpu.VMEM((3, 2, 2, rows, half), bf),
            pltpu.SemaphoreType.DMA((2, 2)),
        ]
        + [pltpu.SemaphoreType.DMA((2,))] * 2
        + [pltpu.SemaphoreType.DMA((2, 2))] * 2
        + [pltpu.SemaphoreType.DMA((3,))] * 2,
        compiler_params=pltpu.CompilerParams(
            collective_id=4,
            has_side_effects=True,
            vmem_limit_bytes=60 * 2**20,
            dimension_semantics=("arbitrary",),
        ),
        name="image_block",
    )(inputs, cotangent, tails, weights)


def parts_kernel(cuts, replicas, summed_ref, *refs):
    states, outs, sums_ref = refs[:15], refs[15:30], refs[30]
    hidden_here, head_cols, back_width, used = cuts
    width = summed_ref.shape[1]
    row = lax.broadcasted_iota(jnp.int32, sums_ref.shape, 0)
    lane = lax.broadcasted_iota(jnp.int32, sums_ref.shape, 1)
    sums = jnp.zeros(sums_ref.shape, jnp.float32)

    def square_sum(values):
        return jnp.sum(jnp.sum(values * values, axis=1, keepdims=True), axis=0, keepdims=True)

    def one(index, grad, at=None):
        master, first, second = (
            ref[...] if at is None else ref[at] for ref in states[3 * index : 3 * index + 3]
        )
        results = lamb_parts(master, first, second, grad)
        for ref, value in zip(outs[3 * index : 3 * index + 3], results):
            if at is None:
                ref[...] = value
            else:
                ref[at] = value
        return square_sum(master), square_sum(results[2])

    def add(total, index, pair, scale=1.0):
        for column in range(2):
            here = jnp.logical_and(row == index, lane == column)
            total = total + jnp.where(here, pair[column] * scale, 0.0)
        return total

    for kind in range(3):
        at = hidden_here + kind * head_cols
        sums = add(sums, 0, one(0, summed_ref[:, at : at + head_cols], kind))
    outward_at = back_width + hidden_here
    sums = add(sums, 1, one(1, summed_ref[:, outward_at:used].T))
    sums = add(sums, 2, one(2, summed_ref[:, :hidden_here]))
    sums = add(sums, 3, one(3, summed_ref[:, back_width:outward_at]))
    gain = summed_ref[:, width - 128 :].T
    sums = add(sums, 4, one(4, gain[127:128]), replicas)
    sums_ref[...] = sums


def fresh_kernel(sums_ref, *refs):
    masters, updates, fresh, low = refs[:5], refs[5:10], refs[10:15], refs[15:20]
    for index in range(5):
        norms = jnp.sqrt(sums_ref[index : index + 1, :])
        rate = learn_rate * (norms[:, 0:1] / norms[:, 1:2])
        if len(masters[index].shape) == 3:
            rate = rate.reshape(1, 1, 1)
        value = masters[index][...] - rate * updates[index][...]
        fresh[index][...] = value
        low[index][...] = value.astype(jnp.bfloat16)


def lamb_step(summed, states, cuts):
    def blocks(arrays):
        return [pl.BlockSpec(a.shape, lambda i, n=a.ndim: (0,) * n) for a in arrays]

    one_step = {"grid": (1,), "compiler_params": pltpu.CompilerParams(vmem_limit_bytes=60 * 2**20)}
    flat = [array for group in states for array in group]
    like = [jax.ShapeDtypeStruct(array.shape, jnp.float32) for array in flat]
    like.append(jax.ShapeDtypeStruct((8, 128), jnp.float32))
    *parts, sums = pl.pallas_call(
        functools.partial(parts_kernel, cuts, 1.0 / lax.axis_size("tensor")),
        out_shape=like,
        in_specs=blocks([summed, *flat]),
        out_specs=blocks(like),
        name="lamb_parts",
        **one_step,
    )(summed, *flat)
    sums = total_of(sums, 3)
    masters = [group[0] for group in states]
    made = [jax.ShapeDtypeStruct(m.shape, t) for t in (jnp.float32, jnp.bfloat16) for m in masters]
    fresh = pl.pallas_call(
        fresh_kernel,
        out_shape=made,
        in_specs=blocks([sums, *masters, *masters]),
        out_specs=blocks(made),
        name="lamb_fresh",
        **one_step,
    )(sums, *masters, *parts[2::3])
    return parts, fresh, jnp.sqrt(sums[:5, :2])


def local(
    inputs,
    cotangent,
    master_inward,
    first_inward,
    second_inward,
    master_outward,
    first_outward,
    second_outward,
    master_widening,
    first_widening,
    second_widening,
    master_narrowing,
    first_narrowing,
    second_narrowing,
    master_scaling,
    first_scaling,
    second_scaling,
):
    depth = master_widening.shape[0]
    hidden_here = master_widening.shape[1]
    head_cols = master_inward.shape[2]
    model = inputs.shape[1]
    back_width = hidden_here + 3 * head_cols
    gap = (-back_width) % 128
    back_width += gap
    used = back_width + hidden_here + head_cols
    width = -(-(used + 1) // 128) * 128
    cuts = (hidden_here, head_cols, back_width, used)
    copies = gather_blocks(
        (
            master_widening,
            master_inward,
            master_narrowing.T,
            master_outward,
            master_scaling.reshape(1, depth),
        ),
        cuts,
        width,
    ).reshape(model, width)
    rows_here = inputs.shape[0]
    whole_rows = rows_here // 16 * 16
    tails = jnp.stack(
        [
            jnp.pad(rows[whole_rows:], ((0, whole_rows + 16 - rows_here), (0, 0)))
            for rows in (inputs, cotangent)
        ]
    )
    summed_out, input_grad, grads = image_block(
        inputs, cotangent, tails, copies, hidden_here, head_cols, back_width
    )
    share = rows_here // lax.axis_size("tensor")
    start = lax.axis_index("tensor") * share
    output = lax.dynamic_slice_in_dim(summed_out, start, share, 0)
    summed = reduce_blocks(grads.reshape(lax.axis_size("dp"), depth, width))
    states = (
        (master_inward, first_inward, second_inward),
        (master_outward, first_outward, second_outward),
        (master_widening, first_widening, second_widening),
        (master_narrowing.T, first_narrowing.T, second_narrowing.T),
        tuple(v.reshape(1, depth) for v in (master_scaling, first_scaling, second_scaling)),
    )
    parts, fresh, trust_norms = lamb_step(summed, states, cuts)
    results = []
    for index in range(5):
        group = (parts[3 * index], parts[3 * index + 1], fresh[index], fresh[5 + index])
        if index == 3:
            group = [v.T for v in group]
        if index == 4:
            group = [v.reshape(depth) for v in group]
        results += group
    return (output, input_grad, *results, trust_norms)


def solution(mesh):
    in_specs = (
        P("dp", None),
        P("dp", None),
        P(None, "dp", "tensor"),
        P(None, "dp", "tensor"),
        P(None, "dp", "tensor"),
        P("tensor", "dp"),
        P("tensor", "dp"),
        P("tensor", "dp"),
        P("dp", "tensor"),
        P("dp", "tensor"),
        P("dp", "tensor"),
        P("tensor", "dp"),
        P("tensor", "dp"),
        P("tensor", "dp"),
        P("dp"),
        P("dp"),
        P("dp"),
    )
    out_specs = (
        P(("dp", "tensor"), None),
        P("dp", None),
        P(None, "dp", "tensor"),
        P(None, "dp", "tensor"),
        P(None, "dp", "tensor"),
        P(None, "dp", "tensor"),
        P("tensor", "dp"),
        P("tensor", "dp"),
        P("tensor", "dp"),
        P("tensor", "dp"),
        P("dp", "tensor"),
        P("dp", "tensor"),
        P("dp", "tensor"),
        P("dp", "tensor"),
        P("tensor", "dp"),
        P("tensor", "dp"),
        P("tensor", "dp"),
        P("tensor", "dp"),
        P("dp"),
        P("dp"),
        P("dp"),
        P("dp"),
        P(),
    )
    return jax.shard_map(local, mesh=mesh, in_specs=in_specs, out_specs=out_specs, check_vma=False)
```

```python
import functools

import jax
import jax.numpy as jnp
from jax import lax
from jax.experimental import pallas as pl
from jax.experimental.pallas import tpu as pltpu
from jax.sharding import PartitionSpec as P

MESH = pl.DeviceIdType.MESH
PAIR = 2

HEAD_DIM = 64
SEQ = 196
STEP = 5


norm_eps = 1e-06
beta_one = 0.5
beta_two = 0.5
lamb_eps = 1e-06
weight_decay = 0.01
learn_rate = 0.5


def lamb_parts(master, first, second, grad):
    moment = beta_one * first + (1.0 - beta_one) * grad
    square = beta_two * second + (1.0 - beta_two) * grad * grad
    update = (
        moment / (1.0 - beta_one**STEP) / (jnp.sqrt(square / (1.0 - beta_two**STEP)) + lamb_eps)
        + weight_decay * master
    )
    return (moment, square, update)


def greet(place, line, up, down, other):
    barrier = pltpu.get_barrier_semaphore()
    pl.semaphore_signal(barrier, inc=1, device_id=other, device_id_type=MESH)

    @pl.when(place < line - 1)
    def _():
        pl.semaphore_signal(barrier, inc=1, device_id=up, device_id_type=MESH)

    @pl.when(place > 0)
    def _():
        pl.semaphore_signal(barrier, inc=1, device_id=down, device_id_type=MESH)

    pl.semaphore_wait(barrier, 1 + jnp.minimum(place, 1) + jnp.minimum(line - 1 - place, 1))


def gather_kernel(
    line, cuts, wide_ref, inward_ref, narrow_ref, outward_ref, scaling_ref, all_ref,
    own_ref, own_sem, up_sem, down_sem, pair_sem, recv_sem,
):
    hidden_here, head_cols, back_width, used = cuts
    depth, width = own_ref.shape
    b16 = jnp.bfloat16
    own_ref[:, :hidden_here] = wide_ref[...].astype(b16)
    for kind in range(3):
        at = hidden_here + kind * head_cols
        own_ref[:, at : at + head_cols] = inward_ref[kind].astype(b16)
    at = hidden_here + 3 * head_cols
    own_ref[:, at:back_width] = jnp.zeros((depth, back_width - at), b16)
    own_ref[:, back_width : back_width + hidden_here] = narrow_ref[...].astype(b16)
    own_ref[:, back_width + hidden_here : used] = outward_ref[...].T.astype(b16)
    gain = jnp.broadcast_to(scaling_ref[...], (128, depth)).T
    own_ref[:, used:] = gain[:, : width - used].astype(b16)
    me = lax.axis_index("dp")
    place, side = me // PAIR, me % PAIR
    up, down, other = {"dp": me + PAIR}, {"dp": me - PAIR}, {"dp": me + 1 - 2 * side}
    has_up, has_down = place < line - 1, place > 0
    greet(place, line, up, down, other)

    def move(step, source, block, sems, peer):
        return pltpu.make_async_remote_copy(
            src_ref=source,
            dst_ref=all_ref.at[block],
            send_sem=sems.at[step],
            recv_sem=recv_sem.at[block],
            device_id=peer,
            device_id_type=MESH,
        )

    def held(block):
        return all_ref.at[block]

    def arrived(block, peer):
        move(0, held(block), block, pair_sem, peer).wait_recv()

    own = pltpu.make_async_copy(own_ref, all_ref.at[me], own_sem)

    @pl.when(has_up)
    def _():
        move(place, own_ref, me, up_sem, up).start()

    @pl.when(has_down)
    def _():
        move(place, own_ref, me, down_sem, down).start()

    move(place, own_ref, me, pair_sem, other).start()
    own.start()

    @pl.loop(1, line)
    def _(step):
        low, high = place - step, place + step

        @pl.when(low >= 0)
        def _():
            block = low * PAIR + side
            arrived(block, other)

            @pl.when(has_up)
            def _():
                move(low, held(block), block, up_sem, up).start()

            move(low, held(block), block, pair_sem, other).start()

        @pl.when(high < line)
        def _():
            block = high * PAIR + side
            arrived(block, other)

            @pl.when(has_down)
            def _():
                move(high, held(block), block, down_sem, down).start()

            move(high, held(block), block, pair_sem, other).start()

    own.wait()

    @pl.loop(0, line)
    def _(spot):
        block = spot * PAIR + side
        arrived(spot * PAIR + 1 - side, other)
        move(spot, held(block), block, pair_sem, other).wait_send()

        @pl.when(jnp.logical_and(has_up, spot <= place))
        def _():
            move(spot, held(block), block, up_sem, up).wait_send()

        @pl.when(jnp.logical_and(has_down, spot >= place))
        def _():
            move(spot, held(block), block, down_sem, down).wait_send()


def gather_blocks(masters, cuts, width):
    depth = masters[0].shape[0]
    devices = lax.axis_size("dp")
    line = devices // PAIR
    return pl.pallas_call(
        functools.partial(gather_kernel, line, cuts),
        out_shape=jax.ShapeDtypeStruct((devices, depth, width), jnp.bfloat16),
        in_specs=[pl.BlockSpec(memory_space=pltpu.VMEM)] * 5,
        out_specs=pl.BlockSpec(memory_space=pl.ANY),
        scratch_shapes=[
            pltpu.VMEM((depth, width), jnp.bfloat16),
            pltpu.SemaphoreType.DMA,
            pltpu.SemaphoreType.DMA((line,)),
            pltpu.SemaphoreType.DMA((line,)),
            pltpu.SemaphoreType.DMA((line,)),
            pltpu.SemaphoreType.DMA((devices,)),
        ],
        compiler_params=pltpu.CompilerParams(
            collective_id=0, has_side_effects=True, vmem_limit_bytes=60 * 2**20
        ),
        cost_estimate=pl.CostEstimate(flops=0, bytes_accessed=100_000_000, transcendentals=0),
        name="gather_blocks",
    )(*masters)


def reduce_kernel(
    line, own_ref, sum_ref, pair_in, up_in, down_in, up_out, down_out,
    pair_send, pair_recv, up_send, up_recv, down_send, down_recv,
):
    me = lax.axis_index("dp")
    place, side = me // PAIR, me % PAIR
    up, down, other = {"dp": me + PAIR}, {"dp": me - PAIR}, {"dp": me + 1 - 2 * side}
    has_up, has_down = place < line - 1, place > 0
    greet(place, line, up, down, other)

    def pair_move(spot):
        return pltpu.make_async_remote_copy(
            src_ref=own_ref.at[spot * PAIR + 1 - side],
            dst_ref=pair_in.at[spot],
            send_sem=pair_send.at[spot],
            recv_sem=pair_recv.at[spot],
            device_id=other,
            device_id_type=MESH,
        )

    def line_move(spot, source, target, sends, recvs, peer):
        return pltpu.make_async_remote_copy(
            src_ref=source.at[spot],
            dst_ref=target.at[spot],
            send_sem=sends.at[spot],
            recv_sem=recvs.at[spot],
            device_id=peer,
            device_id_type=MESH,
        )

    def up_move(spot):
        return line_move(spot, up_out, up_in, up_send, up_recv, up)

    def down_move(spot):
        return line_move(spot, down_out, down_in, down_send, down_recv, down)

    @pl.loop(0, line)
    def _(turn):
        far = line - 1 - turn

        @pl.when(place + far < line)
        def _():
            pair_move(place + far).start()

        @pl.when(jnp.logical_and(place - far >= 0, far > 0))
        def _():
            pair_move(place - far).start()

    def both(spot):
        return own_ref[spot * PAIR + side].astype(jnp.float32) + pair_in[spot].astype(jnp.float32)

    @pl.loop(0, line - 1)
    def _(turn):
        far = line - 1 - turn

        @pl.when(place + far < line)
        def _():
            spot = place + far
            pair_move(spot).wait_recv()

            @pl.when(has_down)
            def _():
                up_move(spot).wait_recv()
                up_out[spot] = (both(spot) + up_in[spot].astype(jnp.float32)).astype(jnp.bfloat16)

            @pl.when(jnp.logical_not(has_down))
            def _():
                up_out[spot] = both(spot).astype(jnp.bfloat16)

            up_move(spot).start()

        @pl.when(place - far >= 0)
        def _():
            spot = place - far
            pair_move(spot).wait_recv()

            @pl.when(has_up)
            def _():
                down_move(spot).wait_recv()
                down_out[spot] = (both(spot) + down_in[spot].astype(jnp.float32)).astype(
                    jnp.bfloat16
                )

            @pl.when(jnp.logical_not(has_up))
            def _():
                down_out[spot] = both(spot).astype(jnp.bfloat16)

            down_move(spot).start()

    pair_move(place).wait_recv()
    sum_ref[...] = both(place)

    @pl.when(has_down)
    def _():
        up_move(place).wait_recv()
        sum_ref[...] += up_in[place].astype(jnp.float32)

    @pl.when(has_up)
    def _():
        down_move(place).wait_recv()
        sum_ref[...] += down_in[place].astype(jnp.float32)

    @pl.loop(0, line)
    def _(spot):
        pair_move(spot).wait_send()

        @pl.when(spot > place)
        def _():
            up_move(spot).wait_send()

        @pl.when(spot < place)
        def _():
            down_move(spot).wait_send()


def reduce_blocks(own):
    devices, rows, width = own.shape
    line = devices // PAIR
    buffer = pltpu.VMEM((line, rows, width), own.dtype)
    return pl.pallas_call(
        functools.partial(reduce_kernel, line),
        out_shape=jax.ShapeDtypeStruct((rows, width), jnp.float32),
        in_specs=[pl.BlockSpec(memory_space=pltpu.VMEM)],
        out_specs=pl.BlockSpec(memory_space=pltpu.VMEM),
        scratch_shapes=[buffer] * 5 + [pltpu.SemaphoreType.DMA((line,))] * 6,
        compiler_params=pltpu.CompilerParams(
            collective_id=1, has_side_effects=True, vmem_limit_bytes=40 * 2**20
        ),
        cost_estimate=pl.CostEstimate(flops=0, bytes_accessed=100_000_000, transcendentals=0),
        name="reduce_blocks",
    )(own)


def total_kernel(
    devices, ranks, own_ref, sum_ref, rank_in, dp_out, dp_in,
    rank_send, rank_recv, dp_send, dp_recv,
):
    me, rank = lax.axis_index("dp"), lax.axis_index("tensor")
    barrier = pltpu.get_barrier_semaphore()
    for shift in range(1, ranks):
        peer = {"tensor": lax.rem(rank + shift, ranks)}
        pl.semaphore_signal(barrier, inc=1, device_id=peer, device_id_type=MESH)
    for shift in range(1, devices):
        peer = {"dp": lax.rem(me + shift, devices)}
        pl.semaphore_signal(barrier, inc=1, device_id=peer, device_id_type=MESH)
    pl.semaphore_wait(barrier, ranks - 1 + devices - 1)

    def rank_move(shift):
        return pltpu.make_async_remote_copy(
            src_ref=own_ref,
            dst_ref=rank_in.at[rank],
            send_sem=rank_send.at[shift],
            recv_sem=rank_recv.at[rank],
            device_id={"tensor": lax.rem(rank + shift, ranks)},
            device_id_type=MESH,
        )

    def rank_arrival(source):
        return pltpu.make_async_remote_copy(
            src_ref=own_ref,
            dst_ref=rank_in.at[source],
            send_sem=rank_send.at[0],
            recv_sem=rank_recv.at[source],
            device_id={"tensor": lax.rem(rank + 1, ranks)},
            device_id_type=MESH,
        )

    def dp_move(shift):
        return pltpu.make_async_remote_copy(
            src_ref=dp_out,
            dst_ref=dp_in.at[me],
            send_sem=dp_send.at[shift],
            recv_sem=dp_recv.at[me],
            device_id={"dp": lax.rem(me + shift, devices)},
            device_id_type=MESH,
        )

    def dp_arrival(source):
        return pltpu.make_async_remote_copy(
            src_ref=dp_out,
            dst_ref=dp_in.at[source],
            send_sem=dp_send.at[0],
            recv_sem=dp_recv.at[source],
            device_id={"dp": lax.rem(me + 1, devices)},
            device_id_type=MESH,
        )

    for shift in range(1, ranks):
        rank_move(shift).start()
    rank_in[rank] = own_ref[...]
    for shift in range(1, ranks):
        rank_arrival(lax.rem(rank + shift, ranks)).wait_recv()
    part = rank_in[0]
    for spot in range(1, ranks):
        part = part + rank_in[spot]
    dp_out[...] = part
    for shift in range(1, devices):
        dp_move(shift).start()
    dp_in[me] = part
    for shift in range(1, devices):
        dp_arrival(lax.rem(me + shift, devices)).wait_recv()
    whole = dp_in[0]
    for spot in range(1, devices):
        whole = whole + dp_in[spot]
    sum_ref[...] = whole
    for shift in range(1, ranks):
        rank_move(shift).wait_send()
    for shift in range(1, devices):
        dp_move(shift).wait_send()


def total_of(own, collective_id):
    devices, ranks = lax.axis_size("dp"), lax.axis_size("tensor")
    return pl.pallas_call(
        functools.partial(total_kernel, devices, ranks),
        out_shape=jax.ShapeDtypeStruct(own.shape, own.dtype),
        in_specs=[pl.BlockSpec(memory_space=pltpu.VMEM)],
        out_specs=pl.BlockSpec(memory_space=pltpu.VMEM),
        scratch_shapes=[
            pltpu.VMEM((ranks,) + own.shape, own.dtype),
            pltpu.VMEM(own.shape, own.dtype),
            pltpu.VMEM((devices,) + own.shape, own.dtype),
            pltpu.SemaphoreType.DMA((ranks,)),
            pltpu.SemaphoreType.DMA((ranks,)),
            pltpu.SemaphoreType.DMA((devices,)),
            pltpu.SemaphoreType.DMA((devices,)),
        ],
        compiler_params=pltpu.CompilerParams(
            collective_id=collective_id, has_side_effects=True, vmem_limit_bytes=60 * 2**20
        ),
        cost_estimate=pl.CostEstimate(flops=0, bytes_accessed=20_000_000, transcendentals=0),
        name="total_" + str(collective_id),
    )(own)


WINDOW = 224


def image_kernel(
    images, cuts, x_hbm, c_hbm, tail_ref, w_ref,
    out_ref, grad_in_ref, g_ref,
    acc1, acc2, gain_row, g_gain, windows, kept, qkv, back_cols, front_cols,
    partial, pair_in, chip_sum, line_in, total,
    in_sem, s1, r1, s2, r2, s3, r3,
):
    step = pl.program_id(0)
    rank = lax.axis_index("tensor")
    core, half_of_images = rank % 2, rank // 2
    sibling = {"tensor": rank + 1 - 2 * core}
    across = {"tensor": lax.rem(rank + 2, 4)}
    width, head_cols = cuts
    heads = head_cols // HEAD_DIM
    rows, model = kept.shape[2], kept.shape[3]
    half = model // 2
    f32, b16 = jnp.float32, jnp.bfloat16
    back_width, front_width = back_cols.shape[1], front_cols.shape[1]
    last_window = images * SEQ // 16 * 16 - WINDOW

    def image_at(turn):
        return turn // 2 + (turn % 2) * (images // 2 + 1)

    def window_start(image):
        return pl.multiple_of(jnp.minimum(image * SEQ // 16 * 16, last_window), 16)

    def fetches(image, slot):
        return [
            pltpu.make_async_copy(
                source.at[pl.ds(window_start(image), WINDOW)],
                windows.at[slot, kind, pl.ds(0, WINDOW)],
                in_sem.at[slot, kind],
            )
            for kind, source in ((0, x_hbm), (1, c_hbm))
        ]

    def one_hot(shape, row_is):
        at = [lax.broadcasted_iota(jnp.int32, shape, axis) for axis in (0, 1)]
        return jnp.where(row_is(*at), 1.0, 0.0).astype(b16)

    @pl.when(step == 0)
    def _():
        line_in[...] = jnp.zeros_like(line_in)
        barrier = pltpu.get_barrier_semaphore()
        pl.semaphore_signal(barrier, inc=1, device_id=sibling, device_id_type=MESH)
        pl.semaphore_signal(barrier, inc=1, device_id=across, device_id_type=MESH)
        pl.semaphore_wait(barrier, 2)
        for copy in fetches(0, 0):
            copy.start()
        for slot in range(2):
            for kind in range(2):
                windows[slot, kind, WINDOW:] = tail_ref[kind]
        total[...] = jnp.zeros_like(total)
        kept[...] = jnp.zeros_like(kept)
        acc1[...] = jnp.zeros_like(acc1)
        acc2[...] = jnp.zeros_like(acc2)
        back_cols[...] = jnp.zeros_like(back_cols)
        front_cols[...] = jnp.zeros_like(front_cols)
        g_gain[...] = jnp.zeros_like(g_gain)
        for ref in (out_ref, grad_in_ref):
            ref[:16] = jnp.zeros((16, model), b16)
        turned = w_ref[:, back_width + front_width - 128 :].astype(f32).T
        gain_row[...] = turned[127:128]

    @pl.when(step < images - 1)
    def _():
        for copy in fetches(image_at(step + 1), (step + 1) % 2):
            copy.start()

    def move(source, target, sends, recvs, slot, peer):
        return pltpu.make_async_remote_copy(
            src_ref=source,
            dst_ref=target,
            send_sem=sends.at[slot],
            recv_sem=recvs.at[slot],
            device_id=peer,
            device_id_type=MESH,
        )

    def first(slot):
        return move(partial.at[slot, 1 - core], pair_in.at[slot], s1, r1, slot, sibling)

    def second(slot, kind):
        return pltpu.make_async_remote_copy(
            src_ref=chip_sum.at[slot, kind],
            dst_ref=line_in.at[slot, kind],
            send_sem=s2.at[slot, kind],
            recv_sem=r2.at[slot, kind],
            device_id=across,
            device_id_type=MESH,
        )

    def gives_output(turn):
        return jnp.logical_or(turn % 2 != half_of_images, turn == images - 1)

    def takes_output(turn):
        return jnp.logical_or(turn % 2 == half_of_images, turn == images - 1)

    def third(slot):
        return move(total.at[slot, core], total.at[slot, core], s3, r3, slot, sibling)

    def normalised(values):
        floats = values.astype(f32)
        centred = floats - jnp.mean(floats, axis=1, keepdims=True)
        inv_std = lax.rsqrt(jnp.mean(centred * centred, axis=1, keepdims=True) + norm_eps)
        return floats, centred * inv_std, inv_std

    gain = gain_row[...]

    image = image_at(jnp.maximum(step - 3, 0))

    def place(ref, values):
        start = pl.multiple_of(image * SEQ // 16 * 16, 16)
        offset = image * SEQ - start
        spread = one_hot((WINDOW, rows), lambda r, j: jnp.logical_and(r == j + offset, j < SEQ))
        placed = jnp.dot(spread, values, preferred_element_type=f32)
        before = lax.broadcasted_iota(jnp.int32, (16, model), 0) < offset
        head = jnp.where(before, ref[pl.ds(start, 16), :].astype(f32), placed[:16])
        ref[pl.ds(start, 16), :] = head.astype(b16)
        ref[pl.ds(start + 16, WINDOW - 16), :] = placed[16:].astype(b16)

    def place_late(ref, values):
        @pl.when(step < images + 1)
        def _():
            place(ref, values)

        for turn in (images - 2, images - 1):

            @pl.when(step == turn + 3)
            def _(at=image_at(turn) * SEQ):
                ref[at : at + SEQ] = values[:SEQ]

    @pl.when(step >= 3)
    def _():
        third((step - 3) % 3).wait()

    def finish(put):
        slot, spot = (step + 3) % 3, (step + 1) % 4
        floats, unit, inv_std = normalised(kept[spot, 0])
        sums = jnp.concatenate([total[slot, 0, 0], total[slot, 1, 0]], axis=1).astype(f32)
        put(out_ref, (floats + sums).astype(b16))
        d_normed = jnp.concatenate([total[slot, 0, 1], total[slot, 1, 1]], axis=1).astype(f32)
        weighted = d_normed * unit
        counted = jnp.sum(weighted, axis=0, keepdims=True)
        g_gain[...] += jnp.where(step >= 3, counted, 0.0)
        d_unit = d_normed * gain
        d_floats = inv_std * (
            d_unit
            - jnp.mean(d_unit, axis=1, keepdims=True)
            - unit * jnp.mean(weighted * gain, axis=1, keepdims=True)
        )
        put(grad_in_ref, (kept[spot, 1].astype(f32) + d_floats).astype(b16))

    @pl.when(step < images)
    def _():
        slot = step % 2
        for copy in fetches(image_at(step), slot):
            copy.wait()
        offset = image_at(step) * SEQ - window_start(image_at(step))
        pick = one_hot(
            (rows, windows.shape[2]), lambda r, j: jnp.logical_and(j == r + offset, r < SEQ)
        )
        for kind in range(2):
            kept[step % 4, kind] = jnp.dot(
                pick, windows[slot, kind], preferred_element_type=f32
            ).astype(b16)
        _floats, unit, _inv = normalised(kept[step % 4, 0])
        normed = (unit * gain).astype(b16)
        cot = kept[step % 4, 1]

        def mm(a, b):
            return jnp.dot(a, b, preferred_element_type=f32)

        def mm_nt(a, b):
            return lax.dot_general(a, b, (((1,), (1,)), ((), ())), preferred_element_type=f32)

        def mm_tn(a, b):
            return lax.dot_general(a, b, (((0,), (0,)), ((), ())), preferred_element_type=f32)

        qkv[:, : 3 * head_cols] = mm(normed, w_ref[:, width:back_width])[:, : 3 * head_cols].astype(b16)
        qkv[:, 3 * head_cols :] = mm(cot, w_ref[:, back_width + width :])[:, :head_cols].astype(b16)
        keys_wide = pl.cdiv(rows, 128) * 128
        filler = jnp.zeros((keys_wide - rows, HEAD_DIM), b16)
        real = lax.broadcasted_iota(jnp.int32, (rows, keys_wide), 1) < SEQ
        for head in range(heads):
            def part(kind):
                at = kind * head_cols + head * HEAD_DIM
                return qkv[:, at : at + HEAD_DIM]

            query = part(0) * jnp.asarray(HEAD_DIM ** (-0.5), b16)
            key = jnp.concatenate([part(1), filler], axis=0)
            value = jnp.concatenate([part(2), filler], axis=0)
            d_att = part(3)
            scores = jnp.where(real, mm_nt(query, key), -1e30)
            powers = jnp.exp(scores - jnp.max(scores, axis=1, keepdims=True))
            probs = powers * (1.0 / jnp.sum(powers, axis=1, keepdims=True))
            probs_low = probs.astype(b16)
            spot = head * HEAD_DIM
            front_cols[:, width + spot : width + spot + HEAD_DIM] = mm(probs_low, value).astype(b16)
            d_probs = mm_nt(d_att, value)
            d_value = mm_tn(probs_low, d_att)[:rows].astype(b16)
            inner = jnp.sum(probs * d_probs, axis=1, keepdims=True)
            d_scores = (probs * (d_probs - inner)).astype(b16)
            d_query = (mm(d_scores, key) * (HEAD_DIM ** (-0.5))).astype(b16)
            d_key = mm_tn(d_scores, query)[:rows].astype(b16)
            for kind, value_of in ((0, d_query), (1, d_key), (2, d_value)):
                at = width + kind * head_cols + spot
                back_cols[:, at : at + HEAD_DIM] = value_of

        upper = mm(normed, w_ref[:, :width])
        d_hidden = mm(cot, w_ref[:, back_width : back_width + width])
        scale = (2.0 / 3.141592653589793) ** 0.5
        square = upper * upper
        bend = jnp.tanh(scale * upper * (1.0 + 0.044715 * square))
        step_up = 0.5 * (1.0 + bend)
        front_cols[:, :width] = (upper * step_up).astype(b16)
        slope = step_up + (0.5 * scale) * upper * (1.0 - bend * bend) * (
            1.0 + (3.0 * 0.044715) * square
        )
        back_cols[:, :width] = (d_hidden * slope).astype(b16)

        finish(place)
        out_part = mm_nt(front_cols[...], w_ref[:, back_width:]).astype(b16)
        partial[slot, 0, 0] = out_part[:, :half]
        partial[slot, 1, 0] = out_part[:, half:]
        back_part = mm_nt(back_cols[...], w_ref[:, :back_width]).astype(b16)
        partial[slot, 0, 1] = back_part[:, :half]
        partial[slot, 1, 1] = back_part[:, half:]
        acc1[...] += mm_tn(normed, back_cols[...])
        acc2[...] += mm_tn(cot, front_cols[...])

    @pl.when(step >= images)
    def _():
        finish(place_late)

    @pl.when(jnp.logical_and(step >= 2, step < images + 2))
    def _():
        slot, spot = (step - 2) % 2, (step - 2) % 3
        second(slot, 1).wait()

        @pl.when(gives_output(step - 2))
        def _():
            second(slot, 0).wait_send()

        @pl.when(takes_output(step - 2))
        def _():
            second(slot, 0).wait_recv()

        total[spot, core] = (chip_sum[slot].astype(f32) + line_in[slot].astype(f32)).astype(b16)
        third(spot).start()

    @pl.when(jnp.logical_and(step >= 1, step < images + 1))
    def _():
        slot = (step - 1) % 2
        first(slot).wait()
        chip_sum[slot] = (partial[slot, core].astype(f32) + pair_in[slot].astype(f32)).astype(b16)
        second(slot, 1).start()

        @pl.when(gives_output(step - 1))
        def _():
            second(slot, 0).start()

    @pl.when(step < images)
    def _():
        first(step % 2).start()

    @pl.when(step == images + 2)
    def _():
        g_ref[:, :back_width] = acc1[...].astype(b16)
        inner = back_width + front_width - 128
        g_ref[:, back_width:inner] = acc2[:, : front_width - 128].astype(b16)
        spare = jnp.broadcast_to(g_gain[...], (128, model)).T
        last = lax.broadcasted_iota(jnp.int32, (model, 128), 1) == 127
        g_ref[:, inner:] = jnp.where(last, spare, acc2[:, front_width - 128 :]).astype(b16)


def image_block(inputs, cotangent, tails, weights, width, head_cols, back_width):
    tokens, model = inputs.shape
    images = tokens // SEQ
    rows = -(-SEQ // 16) * 16
    half = model // 2
    front_width = weights.shape[1] - back_width
    fixed = lambda i: (0, 0)

    def whole(shape):
        return pl.BlockSpec(shape, fixed, pipeline_mode=pl.Buffered(1))

    bf = jnp.bfloat16
    anywhere = pl.BlockSpec(memory_space=pl.ANY)
    return pl.pallas_call(
        functools.partial(image_kernel, images, (width, head_cols)),
        grid=(images + 3,),
        out_shape=(
            jax.ShapeDtypeStruct(inputs.shape, bf),
            jax.ShapeDtypeStruct(inputs.shape, bf),
            jax.ShapeDtypeStruct(weights.shape, bf),
        ),
        in_specs=[
            anywhere,
            anywhere,
            pl.BlockSpec(tails.shape, lambda i: (0, 0, 0), pipeline_mode=pl.Buffered(1)),
            whole(weights.shape),
        ],
        out_specs=[whole(inputs.shape), whole(inputs.shape), whole(weights.shape)],
        scratch_shapes=[
            pltpu.VMEM((model, back_width), jnp.float32),
            pltpu.VMEM((model, front_width), jnp.float32),
            pltpu.VMEM((1, model), jnp.float32),
            pltpu.VMEM((1, model), jnp.float32),
            pltpu.VMEM((2, 2, WINDOW + tails.shape[1], model), bf),
            pltpu.VMEM((4, 2, rows, model), bf),
            pltpu.VMEM((rows, 4 * head_cols), bf),
            pltpu.VMEM((rows, back_width), bf),
            pltpu.VMEM((rows, front_width), bf),
            pltpu.VMEM((2, 2, 2, rows, half), bf),
            pltpu.VMEM((2, 2, rows, half), bf),
            pltpu.VMEM((2, 2, rows, half), bf),
            pltpu.VMEM((2, 2, rows, half), bf),
            pltpu.VMEM((3, 2, 2, rows, half), bf),
            pltpu.SemaphoreType.DMA((2, 2)),
        ]
        + [pltpu.SemaphoreType.DMA((2,))] * 2
        + [pltpu.SemaphoreType.DMA((2, 2))] * 2
        + [pltpu.SemaphoreType.DMA((3,))] * 2,
        compiler_params=pltpu.CompilerParams(
            collective_id=4,
            has_side_effects=True,
            vmem_limit_bytes=60 * 2**20,
            dimension_semantics=("arbitrary",),
        ),
        name="image_block",
    )(inputs, cotangent, tails, weights)


def parts_kernel(cuts, replicas, summed_ref, *refs):
    states, outs, sums_ref = refs[:15], refs[15:30], refs[30]
    hidden_here, head_cols, back_width, used = cuts
    width = summed_ref.shape[1]
    row = lax.broadcasted_iota(jnp.int32, sums_ref.shape, 0)
    lane = lax.broadcasted_iota(jnp.int32, sums_ref.shape, 1)
    sums = jnp.zeros(sums_ref.shape, jnp.float32)

    def square_sum(values):
        return jnp.sum(jnp.sum(values * values, axis=1, keepdims=True), axis=0, keepdims=True)

    def one(index, grad, at=None):
        master, first, second = (
            ref[...] if at is None else ref[at] for ref in states[3 * index : 3 * index + 3]
        )
        results = lamb_parts(master, first, second, grad)
        for ref, value in zip(outs[3 * index : 3 * index + 3], results):
            if at is None:
                ref[...] = value
            else:
                ref[at] = value
        return square_sum(master), square_sum(results[2])

    def add(total, index, pair, scale=1.0):
        for column in range(2):
            here = jnp.logical_and(row == index, lane == column)
            total = total + jnp.where(here, pair[column] * scale, 0.0)
        return total

    for kind in range(3):
        at = hidden_here + kind * head_cols
        sums = add(sums, 0, one(0, summed_ref[:, at : at + head_cols], kind))
    outward_at = back_width + hidden_here
    sums = add(sums, 1, one(1, summed_ref[:, outward_at:used].T))
    sums = add(sums, 2, one(2, summed_ref[:, :hidden_here]))
    sums = add(sums, 3, one(3, summed_ref[:, back_width:outward_at]))
    gain = summed_ref[:, width - 128 :].T
    sums = add(sums, 4, one(4, gain[127:128]), replicas)
    sums_ref[...] = sums


def fresh_kernel(sums_ref, *refs):
    masters, updates, fresh, low = refs[:5], refs[5:10], refs[10:15], refs[15:20]
    for index in range(5):
        norms = jnp.sqrt(sums_ref[index : index + 1, :])
        rate = learn_rate * (norms[:, 0:1] / norms[:, 1:2])
        if len(masters[index].shape) == 3:
            rate = rate.reshape(1, 1, 1)
        value = masters[index][...] - rate * updates[index][...]
        fresh[index][...] = value
        low[index][...] = value.astype(jnp.bfloat16)


def lamb_step(summed, states, cuts):
    def blocks(arrays):
        return [pl.BlockSpec(a.shape, lambda i, n=a.ndim: (0,) * n) for a in arrays]

    one_step = {"grid": (1,), "compiler_params": pltpu.CompilerParams(vmem_limit_bytes=60 * 2**20)}
    flat = [array for group in states for array in group]
    like = [jax.ShapeDtypeStruct(array.shape, jnp.float32) for array in flat]
    like.append(jax.ShapeDtypeStruct((8, 128), jnp.float32))
    *parts, sums = pl.pallas_call(
        functools.partial(parts_kernel, cuts, 1.0 / lax.axis_size("tensor")),
        out_shape=like,
        in_specs=blocks([summed, *flat]),
        out_specs=blocks(like),
        name="lamb_parts",
        **one_step,
    )(summed, *flat)
    sums = total_of(sums, 3)
    masters = [group[0] for group in states]
    made = [jax.ShapeDtypeStruct(m.shape, t) for t in (jnp.float32, jnp.bfloat16) for m in masters]
    fresh = pl.pallas_call(
        fresh_kernel,
        out_shape=made,
        in_specs=blocks([sums, *masters, *masters]),
        out_specs=blocks(made),
        name="lamb_fresh",
        **one_step,
    )(sums, *masters, *parts[2::3])
    return parts, fresh, jnp.sqrt(sums[:5, :2])


def local(
    inputs,
    cotangent,
    master_inward,
    first_inward,
    second_inward,
    master_outward,
    first_outward,
    second_outward,
    master_widening,
    first_widening,
    second_widening,
    master_narrowing,
    first_narrowing,
    second_narrowing,
    master_scaling,
    first_scaling,
    second_scaling,
):
    depth = master_widening.shape[0]
    hidden_here = master_widening.shape[1]
    head_cols = master_inward.shape[2]
    model = inputs.shape[1]
    back_width = hidden_here + 3 * head_cols
    gap = (-back_width) % 128
    back_width += gap
    used = back_width + hidden_here + head_cols
    width = -(-(used + 1) // 128) * 128
    cuts = (hidden_here, head_cols, back_width, used)
    copies = gather_blocks(
        (
            master_widening,
            master_inward,
            master_narrowing.T,
            master_outward,
            master_scaling.reshape(1, depth),
        ),
        cuts,
        width,
    ).reshape(model, width)
    rows_here = inputs.shape[0]
    whole_rows = rows_here // 16 * 16
    tails = jnp.stack(
        [
            jnp.pad(rows[whole_rows:], ((0, whole_rows + 16 - rows_here), (0, 0)))
            for rows in (inputs, cotangent)
        ]
    )
    summed_out, input_grad, grads = image_block(
        inputs, cotangent, tails, copies, hidden_here, head_cols, back_width
    )
    share = rows_here // lax.axis_size("tensor")
    start = lax.axis_index("tensor") * share
    output = lax.dynamic_slice_in_dim(summed_out, start, share, 0)
    summed = reduce_blocks(grads.reshape(lax.axis_size("dp"), depth, width))
    states = (
        (master_inward, first_inward, second_inward),
        (master_outward, first_outward, second_outward),
        (master_widening, first_widening, second_widening),
        (master_narrowing.T, first_narrowing.T, second_narrowing.T),
        tuple(v.reshape(1, depth) for v in (master_scaling, first_scaling, second_scaling)),
    )
    parts, fresh, trust_norms = lamb_step(summed, states, cuts)
    results = []
    for index in range(5):
        group = (parts[3 * index], parts[3 * index + 1], fresh[index], fresh[5 + index])
        if index == 3:
            group = [v.T for v in group]
        if index == 4:
            group = [v.reshape(depth) for v in group]
        results += group
    return (output, input_grad, *results, trust_norms)


def solution(mesh):
    in_specs = (
        P("dp", None),
        P("dp", None),
        P(None, "dp", "tensor"),
        P(None, "dp", "tensor"),
        P(None, "dp", "tensor"),
        P("tensor", "dp"),
        P("tensor", "dp"),
        P("tensor", "dp"),
        P("dp", "tensor"),
        P("dp", "tensor"),
        P("dp", "tensor"),
        P("tensor", "dp"),
        P("tensor", "dp"),
        P("tensor", "dp"),
        P("dp"),
        P("dp"),
        P("dp"),
    )
    out_specs = (
        P(("dp", "tensor"), None),
        P("dp", None),
        P(None, "dp", "tensor"),
        P(None, "dp", "tensor"),
        P(None, "dp", "tensor"),
        P(None, "dp", "tensor"),
        P("tensor", "dp"),
        P("tensor", "dp"),
        P("tensor", "dp"),
        P("tensor", "dp"),
        P("dp", "tensor"),
        P("dp", "tensor"),
        P("dp", "tensor"),
        P("dp", "tensor"),
        P("tensor", "dp"),
        P("tensor", "dp"),
        P("tensor", "dp"),
        P("tensor", "dp"),
        P("dp"),
        P("dp"),
        P("dp"),
        P("dp"),
        P(),
    )
    return jax.shard_map(local, mesh=mesh, in_specs=in_specs, out_specs=out_specs, check_vma=False)
```
